8 devices in a mesh: part: 1 (over z), row: 2 (over y), col: 4 (over x, core).
Axes of the slice: x: 2, y: 2, z: 1, core: 2. Of those that a mesh axis runs over, the one named last changes fastest.
Arguments:
- ratings: float32 [8192, 512], P(('part', 'row'), 'col')
- mask: int32 [8192, 512], P(('part', 'row'), 'col')
- user_init: float32 [8192, 16], P(('part', 'row'))
- item_init: float32 [512, 16], P(('part', 'col'))
Outputs:
- output 1: float32 [8192, 16], P(('part', 'row'))
- output 2: float32 [512, 16], P(('part', 'col'))
All inputs are finite; a program needn't handle non-finite values.
Results may differ from the reference program's by a relative error of at most 0.00939186.
Values are sent between devices in bfloat16 or wider.
A program may use at most 1 GiB of HBM per device.

```python
import jax
import jax.numpy as jnp

RANK_DIM = 16
NUM_USERS = 8192
NUM_ITEMS = 512
CG_STEPS = 4
RIDGE_WEIGHT = 0.0005


def setup_inputs(seed: int = 0, part: int = 0) -> dict:
    root_key = jax.random.fold_in(jax.random.key(seed), part)
    sub_keys = jax.random.split(root_key, 7)
    user_true = jax.random.normal(sub_keys[0], (NUM_USERS, RANK_DIM), jnp.float32)
    item_true = jax.random.normal(sub_keys[1], (NUM_ITEMS, RANK_DIM), jnp.float32)
    rating_noise = jax.random.normal(sub_keys[2], (NUM_USERS, NUM_ITEMS), jnp.float32)
    ratings = jnp.dot(user_true, item_true.T) * RANK_DIM ** -0.5 + 0.5 * rating_noise
    density = jax.random.randint(sub_keys[3], (NUM_USERS, 1), 30, 71)
    mask = (jax.random.randint(sub_keys[4], (NUM_USERS, NUM_ITEMS), 0, 100) < density).astype(jnp.int32)
    col_scale = 8.0 ** (-jnp.arange(RANK_DIM, dtype=jnp.float32) / (RANK_DIM - 1))
    item_noise = jax.random.normal(sub_keys[5], (NUM_ITEMS, RANK_DIM), jnp.float32)
    item_init = (item_true + 0.5 * item_noise) * col_scale * RANK_DIM ** -0.25
    user_init = 2.0 * jax.random.normal(sub_keys[6], (NUM_USERS, RANK_DIM), jnp.float32) * RANK_DIM ** -0.25
    return {"ratings": ratings, "mask": mask, "user_init": user_init, "item_init": item_init}


def cg_solve(mask_on, ratings, fixed_fac, start, ridge):
    fixed_bf = fixed_fac.astype(jnp.bfloat16)
    mask_bf = mask_on.astype(jnp.bfloat16)
    scores = jnp.dot(start.astype(jnp.bfloat16), fixed_bf.T, preferred_element_type=jnp.float32)
    resid_obs = jnp.where(mask_on, ratings - scores, 0.0).astype(jnp.bfloat16)
    residual = jnp.dot(resid_obs, fixed_bf, preferred_element_type=jnp.float32) - ridge * start
    direction = residual
    estimate = start
    res_sq = jnp.sum(residual * residual, axis=1, keepdims=True)
    for cg_step in range(CG_STEPS):
        scores = jnp.dot(direction.astype(jnp.bfloat16), fixed_bf.T, preferred_element_type=jnp.float32)
        masked = mask_bf * scores.astype(jnp.bfloat16)
        gram_dir = jnp.dot(masked, fixed_bf, preferred_element_type=jnp.float32) + ridge * direction
        step_size = res_sq / jnp.sum(direction * gram_dir, axis=1, keepdims=True)
        estimate = estimate + step_size * direction
        if cg_step + 1 < CG_STEPS:
            residual = residual - step_size * gram_dir
            new_sq = jnp.sum(residual * residual, axis=1, keepdims=True)
            direction = residual + (new_sq / res_sq) * direction
            res_sq = new_sq
    return estimate


def reference(ratings, mask, user_init, item_init):
    mask_on = mask > 0
    user_new = cg_solve(mask_on, ratings, item_init, user_init, RIDGE_WEIGHT * NUM_ITEMS)
    item_new = cg_solve(mask_on.T, ratings.T, user_new, item_init, RIDGE_WEIGHT * NUM_USERS)
    return (user_new, item_new)
```

```python
import functools

import jax
import jax.numpy as jnp
from jax import lax
from jax.experimental import pallas as pl
from jax.experimental.pallas import tpu as pltpu
from jax.sharding import PartitionSpec as P

CG_STEPS = 4
RIDGE_WEIGHT = 0.0005
RANK = 16
DIAGS = RANK // 2 + 1
MESH = pl.DeviceIdType.MESH
F32 = jnp.float32
BF16 = jnp.bfloat16
COLS = 4
CHUNKS = 4


def dot_nt(a, b):
    return lax.dot_general(a, b, (((1,), (1,)), ((), ())), preferred_element_type=F32)


def dot_nn(a, b):
    return lax.dot_general(a, b, (((1,), (0,)), ((), ())), preferred_element_type=F32)


def turn(x, shift):
    return x if shift % RANK == 0 else pltpu.roll(x, shift % RANK, 0)


def pair_products(fac):
    prods = jnp.concatenate([fac * turn(fac, -d) for d in range(DIAGS)], axis=0)
    high = prods.astype(BF16)
    low = (prods - high.astype(F32)).astype(BF16)
    return high, low


def apply_gram(diags, vec):
    out = diags[0] * vec
    for d in range(1, DIAGS):
        out = out + diags[d] * turn(vec, -d)
        if d < RANK // 2:
            out = out + turn(diags[d] * vec, d)
    return out


def cg_solve(diags, residual, start, ridge):
    direction = residual
    estimate = start
    res_sq = jnp.sum(residual * residual, axis=0, keepdims=True)
    for cg_step in range(CG_STEPS):
        gram_dir = apply_gram(diags, direction) + ridge * direction
        step_size = res_sq / jnp.sum(direction * gram_dir, axis=0, keepdims=True)
        estimate = estimate + step_size * direction
        if cg_step + 1 < CG_STEPS:
            residual = residual - step_size * gram_dir
            new_sq = jnp.sum(residual * residual, axis=0, keepdims=True)
            direction = residual + (new_sq / res_sq) * direction
            res_sq = new_sq
    return estimate


def sweep_kernel(
    user_ridge, item_ridge,
    ratings_hbm, mask_hbm, user_hbm, item_hbm,
    user_out, item_out,
    rate, mask32, user0, item0,
    mask16, mask16_peer, item16, item16_peer, ffs,
    gram_send, gram_recv, gram_own,
    res_pair, res_pair_recv, res_far, res_far_recv, res_own,
    fac, user1, item_send, item_recv,
    in_sem, out_sem, item_sem, mask_sem, pair_sem, far_sem, gram_sem, fac_sem, user_sem, cross_sem,
):
    part = lax.axis_index("part")
    row = lax.axis_index("row")
    col = lax.axis_index("col")
    chip = col // 2
    core = col % 2
    pair_col = chip * 2 + (1 - core)
    far_col = (1 - chip) * 2 + core
    diag_col = (1 - chip) * 2 + (1 - core)
    pair = (part, row, pair_col)
    far = (part, row, far_col)
    diag = (part, row, diag_col)
    cross = (part, 1 - row, col)

    span = mask16.shape[1]
    width = span // CHUNKS
    items = item0.shape[1]

    def copy_to(src, dst, sems, slot, device):
        return pltpu.make_async_remote_copy(
            src_ref=src, dst_ref=dst, send_sem=sems.at[0, slot], recv_sem=sems.at[1, slot],
            device_id=device, device_id_type=MESH,
        )

    barrier = pltpu.get_barrier_semaphore()
    for device in (pair, far, diag, cross):
        pl.semaphore_signal(barrier, inc=1, device_id=device, device_id_type=MESH)

    order = (diag_col, far_col, pair_col, col)

    def load(src, dst, slot):
        return pltpu.make_async_copy(src, dst, in_sem.at[slot])

    loads = [load(item_hbm, item0, 0)]
    for slot, block in enumerate(order):
        rows = pl.ds(pl.multiple_of(block * span, span), span)
        loads.append(load(mask_hbm.at[rows], mask32.at[slot], 1 + slot))
    loads.append(load(user_hbm, user0, 5))
    for slot, block in enumerate(order):
        rows = pl.ds(pl.multiple_of(block * span, span), span)
        loads.append(load(ratings_hbm.at[rows], rate.at[slot], 6 + slot))
    for copy in loads:
        copy.start()

    loads[0].wait()
    item16[...] = item0[...].astype(BF16)
    high, low = pair_products(item16[...].astype(F32))
    ffs[0, :, :items] = high
    ffs[0, :, items:] = low
    loads[1].wait()
    mask16[0] = mask32[0].astype(F32).astype(BF16)
    pl.semaphore_wait(barrier, 4)
    item_copy = copy_to(item16, item16_peer, item_sem, 0, pair)
    item_copy.start()
    mask_copies = [copy_to(mask16.at[0], mask16_peer.at[0], mask_sem, 0, pair)]
    mask_copies[0].start()
    loads[2].wait()
    mask16[1] = mask32[1].astype(F32).astype(BF16)
    loads[3].wait()
    mask16[2] = mask32[2].astype(F32).astype(BF16)
    mask_copies.append(copy_to(mask16.at[2], mask16_peer.at[1], mask_sem, 1, pair))
    mask_copies[1].start()
    loads[4].wait()
    mask16[3] = mask32[3].astype(F32).astype(BF16)

    item_copy.wait_recv()
    high, low = pair_products(item16_peer[...].astype(F32))
    ffs[1, :, :items] = high
    ffs[1, :, items:] = low

    def gram_part(slot, chunk):
        mine = mask16[slot, pl.ds(chunk * width, width), :]
        peer = mask16_peer[slot // 2, pl.ds(chunk * width, width), :]
        total = dot_nt(ffs[0], jnp.concatenate([mine, mine], axis=1))
        return total + dot_nt(ffs[1], jnp.concatenate([peer, peer], axis=1))

    mask_copies[0].wait_recv()
    gram_copies = []
    for chunk in range(CHUNKS):
        gram_send[chunk] = gram_part(1, chunk).astype(BF16)
        gram_copies.append(copy_to(gram_send.at[chunk], gram_recv.at[chunk], gram_sem, chunk, far))
        gram_copies[-1].start()

    loads[5].wait()

    def user_residual(slot, block):
        start = user0[:, pl.ds(pl.multiple_of(block * span, span), span)]
        scores = dot_nn(start.T.astype(BF16), item16[...])
        resid = jnp.where(mask32[slot] > 0, rate[slot] - scores, 0.0).astype(BF16)
        return dot_nt(item16[...], resid)

    loads[6].wait()
    res_pair[0] = user_residual(0, diag_col)
    pair_copies = [copy_to(res_pair.at[0], res_pair_recv.at[0], pair_sem, 0, pair)]
    pair_copies[0].start()
    loads[8].wait()
    res_pair[1] = user_residual(2, pair_col)
    pair_copies.append(copy_to(res_pair.at[1], res_pair_recv.at[1], pair_sem, 1, pair))
    pair_copies[1].start()
    loads[7].wait()
    far_part = user_residual(1, far_col)
    pair_copies[0].wait_recv()
    res_far[...] = far_part + res_pair_recv[0]
    far_copy = copy_to(res_far, res_far_recv, far_sem, 0, far)
    far_copy.start()
    loads[9].wait()
    own_part = user_residual(3, col)
    mask_copies[1].wait_recv()
    for chunk in range(CHUNKS):
        gram_own[chunk] = gram_part(3, chunk)
    pair_copies[1].wait_recv()
    mine0 = user0[:, pl.ds(pl.multiple_of(col * span, span), span)]
    res_own[...] = own_part + res_pair_recv[1] - user_ridge * mine0

    def item_part(source, slot, chunk, acc):
        factors = fac[source, chunk]
        wide = factors.astype(F32)
        rows = pl.ds(chunk * width, width)
        seen = mask16[slot, rows, :]
        high, low = pair_products(wide)
        gram = dot_nn(high, seen) + dot_nn(low, seen)
        scores = dot_nn(wide.T.astype(BF16), item16[...])
        resid = jnp.where(mask32[slot, rows, :] > 0, rate[slot, rows, :] - scores, 0.0).astype(BF16)
        part_sum = jnp.concatenate([gram, dot_nn(factors, resid)], axis=0)
        return part_sum if acc is None else acc + part_sum

    far_copy.wait_recv()
    sums = None
    fac_copies = []
    user_copies = []
    peers = ((0, pair, pair_col, 2), (1, far, far_col, 1), (2, diag, diag_col, 0))

    def gather(chunk, acc):
        for lane, _, source, slot in peers:
            fac_copies[chunk][lane].wait_recv()
            acc = item_part(source, slot, chunk, acc)
        return acc

    for chunk in range(CHUNKS):
        lanes = pl.ds(chunk * width, width)
        gram_copies[chunk].wait_recv()
        full = gram_own[chunk] + gram_recv[chunk].astype(F32)
        diags = [full[d * RANK:(d + 1) * RANK] for d in range(DIAGS)]
        start = user0[:, pl.ds(pl.multiple_of(col * span + chunk * width, width), width)]
        solved = cg_solve(diags, res_own[:, lanes] + res_far_recv[:, lanes], start, user_ridge)
        fac[col, chunk] = solved.astype(BF16)
        user1[col, chunk] = solved
        sent = []
        for lane, device, _, _ in peers:
            sent.append(copy_to(fac.at[col, chunk], fac.at[col, chunk], fac_sem, chunk * 3 + lane, device))
            sent[-1].start()
        fac_copies.append(sent)
        whole = []
        for lane, device, _, _ in peers:
            whole.append(copy_to(user1.at[col, chunk], user1.at[col, chunk], user_sem, chunk * 3 + lane, device))
            whole[-1].start()
        user_copies.append(whole)
        sums = item_part(col, 3, chunk, sums)
        if chunk:
            sums = gather(chunk - 1, sums)
    sums = gather(CHUNKS - 1, sums)
    item_send[...] = sums
    cross_copy = copy_to(item_send, item_recv, cross_sem, 0, cross)
    cross_copy.start()

    outs = []
    for chunk in range(CHUNKS):
        for lane in range(3):
            user_copies[chunk][lane].wait_recv()
        for source in range(COLS):
            dst = user_out.at[:, pl.ds(source * span + chunk * width, width)]
            outs.append(pltpu.make_async_copy(user1.at[source, chunk], dst, out_sem.at[chunk * COLS + source]))
            outs[-1].start()

    cross_copy.wait_recv()
    full = item_send[...] + item_recv[...]
    diags = [full[d * RANK:(d + 1) * RANK] for d in range(DIAGS)]
    residual = full[DIAGS * RANK:] - item_ridge * item0[...]
    item_out[...] = cg_solve(diags, residual, item0[...], item_ridge)

    for copy in outs:
        copy.wait()
    for copy in [item_copy, far_copy, cross_copy] + mask_copies + pair_copies + gram_copies + sum(fac_copies, []) + sum(user_copies, []):
        copy.wait_send()


def solution(mesh):
    row_size = mesh.shape["row"]
    col_size = mesh.shape["col"]
    grid_spec = P(("part", "row"), "col")
    user_spec = P(("part", "row"), None)
    item_spec = P(("part", "col"), None)

    def local_step(ratings_blk, mask_blk, user_blk, item_blk):
        users, items = ratings_blk.shape
        span = users // COLS
        width = span // CHUNKS
        any_spec = pl.BlockSpec(memory_space=pl.ANY)
        vmem = pltpu.VMEM
        dma = pltpu.SemaphoreType.DMA
        terms = DIAGS * RANK
        user_new, item_new = pl.pallas_call(
            functools.partial(sweep_kernel, RIDGE_WEIGHT * items * col_size, RIDGE_WEIGHT * users * row_size),
            out_shape=(
                jax.ShapeDtypeStruct((RANK, users), F32),
                jax.ShapeDtypeStruct((RANK, items), F32),
            ),
            in_specs=[any_spec] * 4,
            out_specs=(any_spec, pl.BlockSpec(memory_space=pltpu.VMEM)),
            scratch_shapes=[
                vmem((COLS, span, items), F32),
                vmem((COLS, span, items), jnp.int32),
                vmem((RANK, users), F32),
                vmem((RANK, items), F32),
                vmem((COLS, span, items), BF16),
                vmem((2, span, items), BF16),
                vmem((RANK, items), BF16),
                vmem((RANK, items), BF16),
                vmem((2, terms, 2 * items), BF16),
                vmem((CHUNKS, terms, width), BF16),
                vmem((CHUNKS, terms, width), BF16),
                vmem((CHUNKS, terms, width), F32),
                vmem((2, RANK, span), F32),
                vmem((2, RANK, span), F32),
                vmem((RANK, span), F32),
                vmem((RANK, span), F32),
                vmem((RANK, span), F32),
                vmem((COLS, CHUNKS, RANK, width), BF16),
                vmem((COLS, CHUNKS, RANK, width), F32),
                vmem((terms + RANK, items), F32),
                vmem((terms + RANK, items), F32),
                dma((10,)),
                dma((COLS * CHUNKS,)),
                dma((2, 1)),
                dma((2, 2)),
                dma((2, 2)),
                dma((2, 1)),
                dma((2, CHUNKS)),
                dma((2, CHUNKS * 3)),
                dma((2, CHUNKS * 3)),
                dma((2, 1)),
            ],
            compiler_params=pltpu.CompilerParams(collective_id=0, has_side_effects=True),
        )(ratings_blk, mask_blk, user_blk.T, item_blk.T)
        return user_new.T, item_new.T

    return jax.shard_map(local_step, mesh=mesh, in_specs=(grid_spec, grid_spec, user_spec, item_spec), out_specs=(user_spec, item_spec), check_vma=False)
```

```python
import functools

import jax
import jax.numpy as jnp
from jax import lax
from jax.experimental import pallas as pl
from jax.experimental.pallas import tpu as pltpu
from jax.sharding import PartitionSpec as P

CG_STEPS = 4
RIDGE_WEIGHT = 0.0005
RANK = 16
DIAGS = RANK // 2 + 1
MESH = pl.DeviceIdType.MESH
F32 = jnp.float32
BF16 = jnp.bfloat16
COLS = 4
CHUNKS = 4


def dot_nt(a, b):
    return lax.dot_general(a, b, (((1,), (1,)), ((), ())), preferred_element_type=F32)


def dot_nn(a, b):
    return lax.dot_general(a, b, (((1,), (0,)), ((), ())), preferred_element_type=F32)


def turn(x, shift):
    return x if shift % RANK == 0 else pltpu.roll(x, shift % RANK, 0)


def pair_products(fac):
    prods = jnp.concatenate([fac * turn(fac, -d) for d in range(DIAGS)], axis=0)
    high = prods.astype(BF16)
    low = (prods - high.astype(F32)).astype(BF16)
    return high, low


def apply_gram(diags, vec):
    out = diags[0] * vec
    for d in range(1, DIAGS):
        out = out + diags[d] * turn(vec, -d)
        if d < RANK // 2:
            out = out + turn(diags[d] * vec, d)
    return out


def cg_solve(diags, residual, start, ridge):
    direction = residual
    estimate = start
    res_sq = jnp.sum(residual * residual, axis=0, keepdims=True)
    for cg_step in range(CG_STEPS):
        gram_dir = apply_gram(diags, direction) + ridge * direction
        step_size = res_sq / jnp.sum(direction * gram_dir, axis=0, keepdims=True)
        estimate = estimate + step_size * direction
        if cg_step + 1 < CG_STEPS:
            residual = residual - step_size * gram_dir
            new_sq = jnp.sum(residual * residual, axis=0, keepdims=True)
            direction = residual + (new_sq / res_sq) * direction
            res_sq = new_sq
    return estimate


def sweep_kernel(
    user_ridge, item_ridge,
    ratings_hbm, mask_hbm, user_hbm, item_hbm,
    user_out, item_out,
    rate, mask32, user0, item0,
    mask16, mask16_peer, item16, item16_peer, ffs, zrate,
    gram_send, gram_recv, gram_own,
    res_pair, res_pair_recv, res_far, res_far_recv, res_own,
    fac, user1, item_send, item_recv,
    in_sem, item_sem, mask_sem, pair_sem, far_sem, gram_sem, fac_sem, user_sem, cross_sem,
):
    part = lax.axis_index("part")
    row = lax.axis_index("row")
    col = lax.axis_index("col")
    chip = col // 2
    core = col % 2
    pair_col = chip * 2 + (1 - core)
    far_col = (1 - chip) * 2 + core
    diag_col = (1 - chip) * 2 + (1 - core)
    pair = (part, row, pair_col)
    far = (part, row, far_col)
    diag = (part, row, diag_col)
    cross = (part, 1 - row, col)

    span = mask16.shape[1]
    width = span // CHUNKS
    items = item0.shape[1]
    terms = DIAGS * RANK

    def copy_to(src, dst, sems, slot, device):
        return pltpu.make_async_remote_copy(
            src_ref=src, dst_ref=dst, send_sem=sems.at[0, slot], recv_sem=sems.at[1, slot],
            device_id=device, device_id_type=MESH,
        )

    barrier = pltpu.get_barrier_semaphore()
    for device in (pair, far, diag, cross):
        pl.semaphore_signal(barrier, inc=1, device_id=device, device_id_type=MESH)

    order = (diag_col, far_col, pair_col, col)

    def load(src, dst, slot):
        return pltpu.make_async_copy(src, dst, in_sem.at[slot])

    def block_rows(block):
        return pl.ds(pl.multiple_of(block * span, span), span)

    item_load = load(item_hbm, item0, 0)
    mask_loads = [load(mask_hbm.at[block_rows(block)], mask32.at[slot], 1 + slot) for slot, block in enumerate(order)]
    user_load = load(user_hbm, user0, 5)
    rate_loads = [load(ratings_hbm.at[block_rows(block)], rate.at[slot], 6 + slot) for slot, block in enumerate(order)]
    mask_loads[0].start()
    item_load.start()
    for copy in mask_loads[1:]:
        copy.start()
    user_load.start()
    for slot in (0, 1, 2, 3):
        rate_loads[slot].start()

    mask_loads[0].wait()
    mask16[0] = mask32[0].astype(F32).astype(BF16)
    item_load.wait()
    item16[...] = item0[...].astype(BF16)
    pl.semaphore_wait(barrier, 4)
    item_copy = copy_to(item16, item16_peer, item_sem, 0, pair)
    item_copy.start()
    mask_copies = []
    for chunk in range(CHUNKS):
        rows = pl.ds(chunk * width, width)
        mask_copies.append(copy_to(mask16.at[0, rows], mask16_peer.at[0, rows], mask_sem, chunk, pair))
        mask_copies[-1].start()
    high, low = pair_products(item16[...].astype(F32))
    ffs[0, :, :items] = high
    ffs[0, :, items:] = low
    mask_loads[1].wait()
    mask16[1] = mask32[1].astype(F32).astype(BF16)
    mask_loads[2].wait()
    mask16[2] = mask32[2].astype(F32).astype(BF16)
    own_mask_copy = copy_to(mask16.at[2], mask16_peer.at[1], mask_sem, CHUNKS, pair)
    own_mask_copy.start()
    mask_loads[3].wait()
    mask16[3] = mask32[3].astype(F32).astype(BF16)

    item_copy.wait_recv()
    high, low = pair_products(item16_peer[...].astype(F32))
    ffs[1, :, :items] = high
    ffs[1, :, items:] = low

    def gram_part(slot, chunk):
        mine = mask16[slot, pl.ds(chunk * width, width), :]
        peer = mask16_peer[slot // 2, pl.ds(chunk * width, width), :]
        total = dot_nt(ffs[0], jnp.concatenate([mine, mine], axis=1))
        return total + dot_nt(ffs[1], jnp.concatenate([peer, peer], axis=1))

    gram_copies = [copy_to(gram_send.at[chunk], gram_recv.at[chunk], gram_sem, chunk, far) for chunk in range(CHUNKS)]
    for chunk in range(CHUNKS):
        mask_copies[chunk].wait_recv()
        gram_send[chunk] = gram_part(1, chunk).astype(BF16)
        if chunk < 2:
            gram_copies[chunk].start()

    user_load.wait()

    def user_residual(slot, block):
        start = user0[:, block_rows(block)]
        scores = dot_nn(start.T.astype(BF16), item16[...])
        resid = jnp.where(mask32[slot] > 0, rate[slot] - scores, 0.0).astype(BF16)
        return dot_nt(item16[...], resid)

    rate_loads[0].wait()
    res_pair[0] = user_residual(0, diag_col)
    pair_copies = [copy_to(res_pair.at[slot], res_pair_recv.at[slot], pair_sem, slot, pair) for slot in range(2)]
    pair_copies[0].start()
    rate_loads[1].wait()
    far_part = user_residual(1, far_col)
    pair_copies[0].wait_recv()
    res_far[...] = (far_part + res_pair_recv[0]).astype(BF16)
    far_copy = copy_to(res_far, res_far_recv, far_sem, 0, far)
    far_copy.start()
    gram_copies[2].start()
    rate_loads[2].wait()
    res_pair[1] = user_residual(2, pair_col)
    pair_copies[1].start()
    rate_loads[3].wait()
    own_part = user_residual(3, col)
    own_mask_copy.wait_recv()
    for chunk in range(CHUNKS):
        gram_own[chunk] = gram_part(3, chunk)
    pair_copies[1].wait_recv()
    res_own[...] = own_part + res_pair_recv[1] - user_ridge * user0[:, block_rows(col)]

    for slot in range(COLS):
        seen_rate = jnp.where(mask32[slot] > 0, rate[slot], 0.0)
        high = seen_rate.astype(BF16)
        rest = seen_rate - high.astype(F32)
        middle = rest.astype(BF16)
        zrate[slot, :, :items] = high
        zrate[slot, :, items:2 * items] = middle
        zrate[slot, :, 2 * items:] = (rest - middle.astype(F32)).astype(BF16)

    def item_part(entries, acc):
        factors = jnp.concatenate([fac[source, chunk] for source, _, chunk in entries], axis=1)
        rows = [pl.ds(chunk * width, width) for _, _, chunk in entries]
        seen = jnp.concatenate([mask16[slot, r, :] for (_, slot, _), r in zip(entries, rows)], axis=0)
        rated = jnp.concatenate([zrate[slot, r, :] for (_, slot, _), r in zip(entries, rows)], axis=0)
        pairs = jnp.concatenate(pair_products(factors.astype(F32)), axis=0)
        sums = (dot_nn(pairs, seen), dot_nn(factors, rated))
        return sums if acc is None else (acc[0] + sums[0], acc[1] + sums[1])

    peers = ((0, pair, pair_col, 2), (1, far, far_col, 1), (2, diag, diag_col, 0))

    def arrived(chunk):
        for lane in range(3):
            fac_copies[chunk][lane].wait_recv()
        return [(source, slot, chunk) for _, _, source, slot in peers]

    far_copy.wait_recv()
    sums = None
    fac_copies = []
    user_copies = []
    for chunk in range(CHUNKS):
        lanes = pl.ds(chunk * width, width)
        gram_copies[chunk].wait_recv()
        if chunk == 0:
            gram_copies[3].start()
        full = gram_own[chunk] + gram_recv[chunk].astype(F32)
        diags = [full[d * RANK:(d + 1) * RANK] for d in range(DIAGS)]
        start = user0[:, pl.ds(pl.multiple_of(col * span + chunk * width, width), width)]
        residual = res_own[:, lanes] + res_far_recv[:, lanes].astype(F32)
        solved = cg_solve(diags, residual, start, user_ridge)
        fac[col, chunk] = solved.astype(BF16)
        user1[col, chunk] = solved
        sent = []
        for lane, device, _, _ in peers[::-1]:
            sent.append(copy_to(fac.at[col, chunk], fac.at[col, chunk], fac_sem, chunk * 3 + lane, device))
            sent[-1].start()
        fac_copies.append(sent[::-1])
        whole = []
        for lane, device, _, _ in peers[:2]:
            whole.append(copy_to(user1.at[col, chunk], user1.at[col, chunk], user_sem, chunk * 3 + lane, device))
            whole[-1].start()
        user_copies.append(whole)
        sums = item_part([(col, 3, chunk)] + (arrived(chunk - 1) if chunk else []), sums)
    last = arrived(CHUNKS - 1)
    sums = item_part(last, sums)
    gram = sums[0][:terms] + sums[0][terms:]
    diags = [gram[d * RANK:(d + 1) * RANK] for d in range(DIAGS)]
    start = item16[...].astype(F32)
    residual = sums[1][:, :items] + sums[1][:, items:2 * items] + sums[1][:, 2 * items:] - apply_gram(diags, start)
    high = residual.astype(BF16)
    item_send[:terms] = gram.astype(BF16)
    item_send[terms:terms + RANK] = high
    item_send[terms + RANK:] = (residual - high.astype(F32)).astype(BF16)
    cross_copy = copy_to(item_send, item_recv, cross_sem, 0, cross)
    cross_copy.start()

    forwards = []
    for chunk in range(CHUNKS):
        user_copies[chunk][1].wait_recv()
        forwards.append(copy_to(user1.at[far_col, chunk], user1.at[far_col, chunk], user_sem, chunk * 3 + 2, pair))
        forwards[-1].start()
    for chunk in range(CHUNKS):
        user_copies[chunk][0].wait_recv()
        forwards[chunk].wait_recv()
        for source in range(COLS):
            user_out[:, pl.ds(source * span + chunk * width, width)] = user1[source, chunk]

    cross_copy.wait_recv()
    full = item_send[...].astype(F32) + item_recv[...].astype(F32)
    diags = [full[d * RANK:(d + 1) * RANK] for d in range(DIAGS)]
    residual = full[terms:terms + RANK] + full[terms + RANK:] - item_ridge * item0[...]
    item_out[...] = cg_solve(diags, residual, item0[...], item_ridge)

    remote = [item_copy, own_mask_copy, far_copy, cross_copy] + mask_copies + pair_copies + gram_copies + forwards
    for copy in remote + sum(fac_copies, []) + sum(user_copies, []):
        copy.wait_send()


def write_kernel(user_ref, item_ref, user_out, item_out, sems):
    copies = [
        pltpu.make_async_copy(user_ref, user_out, sems.at[0]),
        pltpu.make_async_copy(item_ref, item_out, sems.at[1]),
    ]
    for copy in copies:
        copy.start()
    for copy in copies:
        copy.wait()


def solution(mesh):
    row_size = mesh.shape["row"]
    col_size = mesh.shape["col"]
    grid_spec = P(("part", "row"), "col")
    user_spec = P(("part", "row"), None)
    item_spec = P(("part", "col"), None)

    def local_step(ratings_blk, mask_blk, user_blk, item_blk):
        users, items = ratings_blk.shape
        span = users // COLS
        width = span // CHUNKS
        hbm_spec = pl.BlockSpec(memory_space=pltpu.HBM)
        vmem = pltpu.VMEM
        dma = pltpu.SemaphoreType.DMA
        terms = DIAGS * RANK
        user_new, item_new = pl.pallas_call(
            functools.partial(sweep_kernel, RIDGE_WEIGHT * items * col_size, RIDGE_WEIGHT * users * row_size),
            out_shape=(
                pltpu.VMEM((RANK, users), F32),
                pltpu.VMEM((RANK, items), F32),
            ),
            in_specs=[hbm_spec] * 4,
            out_specs=(pl.BlockSpec(memory_space=pltpu.VMEM),) * 2,
            scratch_shapes=[
                vmem((COLS, span, items), F32),
                vmem((COLS, span, items), jnp.int32),
                vmem((RANK, users), F32),
                vmem((RANK, items), F32),
                vmem((COLS, span, items), BF16),
                vmem((2, span, items), BF16),
                vmem((RANK, items), BF16),
                vmem((RANK, items), BF16),
                vmem((2, terms, 2 * items), BF16),
                vmem((COLS, span, 3 * items), BF16),
                vmem((CHUNKS, terms, width), BF16),
                vmem((CHUNKS, terms, width), BF16),
                vmem((CHUNKS, terms, width), F32),
                vmem((2, RANK, span), F32),
                vmem((2, RANK, span), F32),
                vmem((RANK, span), BF16),
                vmem((RANK, span), BF16),
                vmem((RANK, span), F32),
                vmem((COLS, CHUNKS, RANK, width), BF16),
                vmem((COLS, CHUNKS, RANK, width), F32),
                vmem((terms + 2 * RANK, items), BF16),
                vmem((terms + 2 * RANK, items), BF16),
                dma((10,)),
                dma((2, 1)),
                dma((2, CHUNKS + 1)),
                dma((2, 2)),
                dma((2, 1)),
                dma((2, CHUNKS)),
                dma((2, CHUNKS * 3)),
                dma((2, CHUNKS * 3)),
                dma((2, 1)),
            ],
            compiler_params=pltpu.CompilerParams(collective_id=0, has_side_effects=True, vmem_limit_bytes=60000 * 1024),
        )(ratings_blk, mask_blk, user_blk.T, item_blk.T)
        user_new, item_new = pl.pallas_call(
            write_kernel,
            out_shape=(
                jax.ShapeDtypeStruct((RANK, users), F32),
                jax.ShapeDtypeStruct((RANK, items), F32),
            ),
            in_specs=[pl.BlockSpec(memory_space=pltpu.VMEM)] * 2,
            out_specs=(hbm_spec, hbm_spec),
            scratch_shapes=[dma((2,))],
            compiler_params=pltpu.CompilerParams(vmem_limit_bytes=2**20),
        )(user_new, item_new)
        return user_new.T, item_new.T

    return jax.shard_map(local_step, mesh=mesh, in_specs=(grid_spec, grid_spec, user_spec, item_spec), out_specs=(user_spec, item_spec), check_vma=False)
```

```python
import functools

import jax
import jax.numpy as jnp
from jax import lax
from jax.experimental import pallas as pl
from jax.experimental.pallas import tpu as pltpu
from jax.sharding import PartitionSpec as P

CG_STEPS = 4
RIDGE_WEIGHT = 0.0005
RANK = 16
DIAGS = RANK // 2 + 1
MESH = pl.DeviceIdType.MESH
F32 = jnp.float32
BF16 = jnp.bfloat16
COLS = 4
CHUNKS = 4
EARLY = 2


def dot_nt(a, b):
    return lax.dot_general(a, b, (((1,), (1,)), ((), ())), preferred_element_type=F32)


def dot_nn(a, b):
    return lax.dot_general(a, b, (((1,), (0,)), ((), ())), preferred_element_type=F32)


def turn(x, shift):
    return x if shift % RANK == 0 else pltpu.roll(x, shift % RANK, 0)


def pair_products(fac):
    prods = jnp.concatenate([fac * turn(fac, -d) for d in range(DIAGS)], axis=0)
    high = prods.astype(BF16)
    low = (prods - high.astype(F32)).astype(BF16)
    return high, low


def apply_gram(diags, vec):
    out = diags[0] * vec
    for d in range(1, DIAGS):
        out = out + diags[d] * turn(vec, -d)
        if d < RANK // 2:
            out = out + turn(diags[d] * vec, d)
    return out


def cg_solve(diags, residual, start, ridge):
    direction = residual
    estimate = start
    res_sq = jnp.sum(residual * residual, axis=0, keepdims=True)
    for cg_step in range(CG_STEPS):
        gram_dir = apply_gram(diags, direction) + ridge * direction
        step_size = res_sq / jnp.sum(direction * gram_dir, axis=0, keepdims=True)
        estimate = estimate + step_size * direction
        if cg_step + 1 < CG_STEPS:
            residual = residual - step_size * gram_dir
            new_sq = jnp.sum(residual * residual, axis=0, keepdims=True)
            direction = residual + (new_sq / res_sq) * direction
            res_sq = new_sq
    return estimate


def sweep_kernel(
    user_ridge, item_ridge,
    ratings_hbm, mask_hbm, user_hbm, item_hbm,
    user_out, item_out,
    rate, mask32, user0, item0,
    mask16, mask16_peer, item16, item16_peer, ffs, zrate,
    gram_send, gram_recv, gram_own,
    res_pair, res_pair_recv, res_far, res_far_recv, res_own,
    fac, user1, item_send, item_recv,
    in_sem, item_sem, mask_sem, pair_sem, far_sem, gram_sem, fac_sem, user_sem, cross_sem,
):
    part = lax.axis_index("part")
    row = lax.axis_index("row")
    col = lax.axis_index("col")
    chip = col // 2
    core = col % 2
    pair_col = chip * 2 + (1 - core)
    far_col = (1 - chip) * 2 + core
    diag_col = (1 - chip) * 2 + (1 - core)
    pair = (part, row, pair_col)
    far = (part, row, far_col)
    diag = (part, row, diag_col)
    cross = (part, 1 - row, col)

    span = mask16.shape[1]
    width = span // CHUNKS
    items = item0.shape[1]
    terms = DIAGS * RANK

    def copy_to(src, dst, sems, slot, device):
        return pltpu.make_async_remote_copy(
            src_ref=src, dst_ref=dst, send_sem=sems.at[0, slot], recv_sem=sems.at[1, slot],
            device_id=device, device_id_type=MESH,
        )

    barrier = pltpu.get_barrier_semaphore()
    for device in (pair, far, diag, cross):
        pl.semaphore_signal(barrier, inc=1, device_id=device, device_id_type=MESH)

    order = (diag_col, far_col, pair_col, col)

    def load(src, dst, slot):
        return pltpu.make_async_copy(src, dst, in_sem.at[slot])

    def block_rows(block):
        return pl.ds(pl.multiple_of(block * span, span), span)

    item_load = load(item_hbm, item0, 0)
    user_load = load(user_hbm, user0, 1)
    rate_loads = [load(ratings_hbm.at[block_rows(block)], rate.at[slot], 2 + slot) for slot, block in enumerate(order)]
    mask_loads = []
    for slot, block in enumerate(order):
        pieces = []
        for chunk in range(CHUNKS):
            rows = pl.ds(pl.multiple_of(block * span + chunk * width, width), width)
            dst = mask32.at[slot, pl.ds(chunk * width, width)]
            pieces.append(load(mask_hbm.at[rows], dst, 6 + slot * CHUNKS + chunk))
        mask_loads.append(pieces)

    def convert(slot, chunk):
        mask_loads[slot][chunk].wait()
        rows = pl.ds(chunk * width, width)
        mask16[slot, rows] = mask32[slot, rows].astype(F32).astype(BF16)

    item_load.start()
    for pieces in mask_loads[:2]:
        for copy in pieces:
            copy.start()

    item_load.wait()
    item16[...] = item0[...].astype(BF16)
    pl.semaphore_wait(barrier, 4)
    item_copy = copy_to(item16, item16_peer, item_sem, 0, pair)
    item_copy.start()
    mask_copies = []
    for chunk in range(CHUNKS):
        rows = pl.ds(chunk * width, width)
        convert(0, chunk)
        mask_copies.append(copy_to(mask16.at[0, rows], mask16_peer.at[0, rows], mask_sem, chunk, pair))
        mask_copies[-1].start()
    for pieces in mask_loads[2:]:
        for copy in pieces:
            copy.start()
    user_load.start()
    for copy in rate_loads:
        copy.start()
    high, low = pair_products(item16[...].astype(F32))
    ffs[0, :, :items] = high
    ffs[0, :, items:] = low
    for chunk in range(CHUNKS):
        convert(1, chunk)
    item_copy.wait_recv()
    high, low = pair_products(item16_peer[...].astype(F32))
    ffs[1, :, :items] = high
    ffs[1, :, items:] = low

    def gram_part(slot, chunk):
        mine = mask16[slot, pl.ds(chunk * width, width), :]
        peer = mask16_peer[slot // 2, pl.ds(chunk * width, width), :]
        total = dot_nt(ffs[0], jnp.concatenate([mine, mine], axis=1))
        return total + dot_nt(ffs[1], jnp.concatenate([peer, peer], axis=1))

    gram_copies = [copy_to(gram_send.at[chunk], gram_recv.at[chunk], gram_sem, chunk, far) for chunk in range(CHUNKS)]
    for chunk in range(CHUNKS):
        mask_copies[chunk].wait_recv()
        gram_send[chunk] = gram_part(1, chunk).astype(BF16)
        if chunk < EARLY:
            gram_copies[chunk].start()

    user_load.wait()

    def user_residual(slot, block):
        start = user0[:, block_rows(block)]
        scores = dot_nn(start.T.astype(BF16), item16[...])
        resid = jnp.where(mask32[slot] > 0, rate[slot] - scores, 0.0).astype(BF16)
        return dot_nt(item16[...], resid)

    rate_loads[0].wait()
    res_pair[0] = user_residual(0, diag_col)
    pair_copies = [copy_to(res_pair.at[slot], res_pair_recv.at[slot], pair_sem, slot, pair) for slot in range(2)]
    pair_copies[0].start()
    rate_loads[1].wait()
    far_part = user_residual(1, far_col)
    pair_copies[0].wait_recv()
    res_far[...] = (far_part + res_pair_recv[0]).astype(BF16)
    far_copy = copy_to(res_far, res_far_recv, far_sem, 0, far)
    far_copy.start()
    for copy in gram_copies[EARLY:]:
        copy.start()
    for chunk in range(CHUNKS):
        convert(2, chunk)
    own_mask_copy = copy_to(mask16.at[2], mask16_peer.at[1], mask_sem, CHUNKS, pair)
    own_mask_copy.start()
    for chunk in range(CHUNKS):
        convert(3, chunk)
    rate_loads[2].wait()
    res_pair[1] = user_residual(2, pair_col)
    pair_copies[1].start()
    rate_loads[3].wait()
    own_part = user_residual(3, col)
    own_mask_copy.wait_recv()
    for chunk in range(CHUNKS):
        gram_own[chunk] = gram_part(3, chunk)
    pair_copies[1].wait_recv()
    res_own[...] = own_part + res_pair_recv[1] - user_ridge * user0[:, block_rows(col)]

    for slot in range(COLS):
        seen_rate = jnp.where(mask32[slot] > 0, rate[slot], 0.0)
        high = seen_rate.astype(BF16)
        rest = seen_rate - high.astype(F32)
        middle = rest.astype(BF16)
        zrate[slot, :, :items] = high
        zrate[slot, :, items:2 * items] = middle
        zrate[slot, :, 2 * items:] = (rest - middle.astype(F32)).astype(BF16)

    def item_part(entries, acc):
        factors = jnp.concatenate([fac[source, chunk] for source, _, chunk in entries], axis=1)
        rows = [pl.ds(chunk * width, width) for _, _, chunk in entries]
        seen = jnp.concatenate([mask16[slot, r, :] for (_, slot, _), r in zip(entries, rows)], axis=0)
        rated = jnp.concatenate([zrate[slot, r, :] for (_, slot, _), r in zip(entries, rows)], axis=0)
        pairs = jnp.concatenate(pair_products(factors.astype(F32)), axis=0)
        sums = (dot_nn(pairs, seen), dot_nn(factors, rated))
        return sums if acc is None else (acc[0] + sums[0], acc[1] + sums[1])

    peers = ((0, pair, pair_col, 2), (1, far, far_col, 1), (2, diag, diag_col, 0))

    def arrived(chunk):
        for lane in range(3):
            fac_copies[chunk][lane].wait_recv()
        return [(source, slot, chunk) for _, _, source, slot in peers]

    far_copy.wait_recv()
    sums = None
    fac_copies = []
    user_copies = []
    for chunk in range(CHUNKS):
        lanes = pl.ds(chunk * width, width)
        gram_copies[chunk].wait_recv()
        full = gram_own[chunk] + gram_recv[chunk].astype(F32)
        diags = [full[d * RANK:(d + 1) * RANK] for d in range(DIAGS)]
        start = user0[:, pl.ds(pl.multiple_of(col * span + chunk * width, width), width)]
        residual = res_own[:, lanes] + res_far_recv[:, lanes].astype(F32)
        solved = cg_solve(diags, residual, start, user_ridge)
        fac[col, chunk] = solved.astype(BF16)
        user1[col, chunk] = solved
        sent = []
        for lane, device, _, _ in peers[::-1]:
            sent.append(copy_to(fac.at[col, chunk], fac.at[col, chunk], fac_sem, chunk * 3 + lane, device))
            sent[-1].start()
        fac_copies.append(sent[::-1])
        whole = []
        for lane, device, _, _ in peers[:2]:
            whole.append(copy_to(user1.at[col, chunk], user1.at[col, chunk], user_sem, chunk * 3 + lane, device))
            whole[-1].start()
        user_copies.append(whole)
        sums = item_part([(col, 3, chunk)], sums)
    for chunk in range(CHUNKS - 1):
        entries = arrived(chunk)
        sums = item_part(entries, sums)
    last = arrived(CHUNKS - 1)
    sums = item_part(last, sums)
    gram = sums[0][:terms] + sums[0][terms:]
    diags = [gram[d * RANK:(d + 1) * RANK] for d in range(DIAGS)]
    start = item16[...].astype(F32)
    residual = sums[1][:, :items] + sums[1][:, items:2 * items] + sums[1][:, 2 * items:] - apply_gram(diags, start)
    high = residual.astype(BF16)
    item_send[:terms] = gram.astype(BF16)
    item_send[terms:terms + RANK] = high
    item_send[terms + RANK:] = (residual - high.astype(F32)).astype(BF16)
    cross_copy = copy_to(item_send, item_recv, cross_sem, 0, cross)
    cross_copy.start()

    forwards = []
    for chunk in range(CHUNKS):
        user_copies[chunk][1].wait_recv()
        forwards.append(copy_to(user1.at[far_col, chunk], user1.at[far_col, chunk], user_sem, chunk * 3 + 2, pair))
        forwards[-1].start()
    for chunk in range(CHUNKS):
        user_copies[chunk][0].wait_recv()
        forwards[chunk].wait_recv()
        for source in range(COLS):
            user_out[:, pl.ds(source * span + chunk * width, width)] = user1[source, chunk]

    cross_copy.wait_recv()
    full = item_send[...].astype(F32) + item_recv[...].astype(F32)
    diags = [full[d * RANK:(d + 1) * RANK] for d in range(DIAGS)]
    residual = full[terms:terms + RANK] + full[terms + RANK:] - item_ridge * item0[...]
    item_out[...] = cg_solve(diags, residual, item0[...], item_ridge)

    remote = [item_copy, own_mask_copy, far_copy, cross_copy] + mask_copies + pair_copies + gram_copies + forwards
    for copy in remote + sum(fac_copies, []) + sum(user_copies, []):
        copy.wait_send()


def write_kernel(user_ref, item_ref, user_out, item_out, sems):
    copies = [
        pltpu.make_async_copy(user_ref, user_out, sems.at[0]),
        pltpu.make_async_copy(item_ref, item_out, sems.at[1]),
    ]
    for copy in copies:
        copy.start()
    for copy in copies:
        copy.wait()


def solution(mesh):
    row_size = mesh.shape["row"]
    col_size = mesh.shape["col"]
    grid_spec = P(("part", "row"), "col")
    user_spec = P(("part", "row"), None)
    item_spec = P(("part", "col"), None)

    def local_step(ratings_blk, mask_blk, user_blk, item_blk):
        users, items = ratings_blk.shape
        span = users // COLS
        width = span // CHUNKS
        hbm_spec = pl.BlockSpec(memory_space=pltpu.HBM)
        vmem = pltpu.VMEM
        dma = pltpu.SemaphoreType.DMA
        terms = DIAGS * RANK
        user_new, item_new = pl.pallas_call(
            functools.partial(sweep_kernel, RIDGE_WEIGHT * items * col_size, RIDGE_WEIGHT * users * row_size),
            out_shape=(
                pltpu.VMEM((RANK, users), F32),
                pltpu.VMEM((RANK, items), F32),
            ),
            in_specs=[hbm_spec] * 4,
            out_specs=(pl.BlockSpec(memory_space=pltpu.VMEM),) * 2,
            scratch_shapes=[
                vmem((COLS, span, items), F32),
                vmem((COLS, span, items), jnp.int32),
                vmem((RANK, users), F32),
                vmem((RANK, items), F32),
                vmem((COLS, span, items), BF16),
                vmem((2, span, items), BF16),
                vmem((RANK, items), BF16),
                vmem((RANK, items), BF16),
                vmem((2, terms, 2 * items), BF16),
                vmem((COLS, span, 3 * items), BF16),
                vmem((CHUNKS, terms, width), BF16),
                vmem((CHUNKS, terms, width), BF16),
                vmem((CHUNKS, terms, width), F32),
                vmem((2, RANK, span), F32),
                vmem((2, RANK, span), F32),
                vmem((RANK, span), BF16),
                vmem((RANK, span), BF16),
                vmem((RANK, span), F32),
                vmem((COLS, CHUNKS, RANK, width), BF16),
                vmem((COLS, CHUNKS, RANK, width), F32),
                vmem((terms + 2 * RANK, items), BF16),
                vmem((terms + 2 * RANK, items), BF16),
                dma((6 + COLS * CHUNKS,)),
                dma((2, 1)),
                dma((2, CHUNKS + 1)),
                dma((2, 2)),
                dma((2, 1)),
                dma((2, CHUNKS)),
                dma((2, CHUNKS * 3)),
                dma((2, CHUNKS * 3)),
                dma((2, 1)),
            ],
            compiler_params=pltpu.CompilerParams(collective_id=0, has_side_effects=True, vmem_limit_bytes=60000 * 1024),
        )(ratings_blk, mask_blk, user_blk.T, item_blk.T)
        user_new, item_new = pl.pallas_call(
            write_kernel,
            out_shape=(
                jax.ShapeDtypeStruct((RANK, users), F32),
                jax.ShapeDtypeStruct((RANK, items), F32),
            ),
            in_specs=[pl.BlockSpec(memory_space=pltpu.VMEM)] * 2,
            out_specs=(hbm_spec, hbm_spec),
            scratch_shapes=[dma((2,))],
            compiler_params=pltpu.CompilerParams(vmem_limit_bytes=2**20),
        )(user_new, item_new)
        return user_new.T, item_new.T

    return jax.shard_map(local_step, mesh=mesh, in_specs=(grid_spec, grid_spec, user_spec, item_spec), out_specs=(user_spec, item_spec), check_vma=False)
```

```python
import functools

import jax
import jax.numpy as jnp
from jax import lax
from jax.experimental import pallas as pl
from jax.experimental.pallas import tpu as pltpu
from jax.sharding import PartitionSpec as P

CG_STEPS = 4
RIDGE_WEIGHT = 0.0005
RANK = 16
DIAGS = RANK // 2 + 1
MESH = pl.DeviceIdType.MESH
F32 = jnp.float32
BF16 = jnp.bfloat16
COLS = 4
CHUNKS = 4
EARLY = 2
DELAY = 2
LAST = CHUNKS - 1
LANES = 128


def dot_nt(a, b):
    return lax.dot_general(a, b, (((1,), (1,)), ((), ())), preferred_element_type=F32)


def dot_nn(a, b):
    return lax.dot_general(a, b, (((1,), (0,)), ((), ())), preferred_element_type=F32)


def turn(x, shift):
    return x if shift % RANK == 0 else pltpu.roll(x, shift % RANK, 0)


def pair_products(fac):
    prods = jnp.concatenate([fac * turn(fac, -d) for d in range(DIAGS)], axis=0)
    high = prods.astype(BF16)
    low = (prods - high.astype(F32)).astype(BF16)
    return high, low


def apply_gram(diags, vec):
    out = diags[0] * vec
    for d in range(1, DIAGS):
        out = out + diags[d] * turn(vec, -d)
        if d < RANK // 2:
            out = out + turn(diags[d] * vec, d)
    return out


def cg_solve(diags, residual, start, ridge):
    direction = residual
    estimate = start
    res_sq = jnp.sum(residual * residual, axis=0, keepdims=True)
    for cg_step in range(CG_STEPS):
        gram_dir = apply_gram(diags, direction) + ridge * direction
        step_size = res_sq / jnp.sum(direction * gram_dir, axis=0, keepdims=True)
        estimate = estimate + step_size * direction
        if cg_step + 1 < CG_STEPS:
            residual = residual - step_size * gram_dir
            new_sq = jnp.sum(residual * residual, axis=0, keepdims=True)
            direction = residual + (new_sq / res_sq) * direction
            res_sq = new_sq
    return estimate


def sweep_kernel(
    user_ridge, item_ridge,
    ratings_hbm, mask_hbm, user_hbm, item_hbm,
    user_out, item_out,
    rate, mask32, user0, item0,
    mask16, mask16_peer, item16, item16_peer, ffs, zrate,
    gram_send, gram_recv, gram_own,
    res_pair, res_pair_recv, res_far, res_far_recv, res_own,
    fac, user1, item_send, item_recv,
    late_send, late_recv, late_seen, late_rated, late_fac, late_sums,
    in_sem, item_sem, mask_sem, pair_sem, far_sem, gram_sem, fac_sem, user_sem, cross_sem, late_sem, late_fac_sem,
):
    part = lax.axis_index("part")
    row = lax.axis_index("row")
    col = lax.axis_index("col")
    chip = col // 2
    core = col % 2
    pair_col = chip * 2 + (1 - core)
    far_col = (1 - chip) * 2 + core
    diag_col = (1 - chip) * 2 + (1 - core)
    pair = (part, row, pair_col)
    far = (part, row, far_col)
    diag = (part, row, diag_col)
    cross = (part, 1 - row, col)
    peers = ((pair, pair_col, 2), (far, far_col, 1), (diag, diag_col, 0))
    others = [device for device, _, _ in peers] + [cross] + [(part, 1 - row, source) for _, source, _ in peers]

    span = mask16.shape[1]
    width = span // CHUNKS
    items = item0.shape[1]
    terms = DIAGS * RANK

    def copy_to(src, dst, sems, slot, device):
        return pltpu.make_async_remote_copy(
            src_ref=src, dst_ref=dst, send_sem=sems.at[0, slot], recv_sem=sems.at[1, slot],
            device_id=device, device_id_type=MESH,
        )

    barrier = pltpu.get_barrier_semaphore()
    for device in (pair, far, diag, cross):
        pl.semaphore_signal(barrier, inc=1, device_id=device, device_id_type=MESH)

    order = (diag_col, far_col, pair_col, col)

    def load(src, dst, slot):
        return pltpu.make_async_copy(src, dst, in_sem.at[slot])

    def block_rows(block):
        return pl.ds(pl.multiple_of(block * span, span), span)

    item_load = load(item_hbm, item0, 0)
    user_load = load(user_hbm, user0, 1)
    early = LAST * width
    rate_loads = []
    rate_late_loads = []
    for slot, block in enumerate(order):
        rows = pl.ds(pl.multiple_of(block * span, span), early)
        rate_loads.append(load(ratings_hbm.at[rows], rate.at[slot, pl.ds(0, early)], 2 + slot))
        rows = pl.ds(pl.multiple_of(block * span + early, width), width)
        rate_late_loads.append(load(ratings_hbm.at[rows], rate.at[slot, pl.ds(early, width)], 6 + slot))
    mask_loads = []
    for slot, block in enumerate(order):
        pieces = []
        for chunk in range(CHUNKS):
            rows = pl.ds(pl.multiple_of(block * span + chunk * width, width), width)
            dst = mask32.at[slot, pl.ds(chunk * width, width)]
            pieces.append(load(mask_hbm.at[rows], dst, 10 + slot * CHUNKS + chunk))
        mask_loads.append(pieces)

    def convert(slot, chunk):
        mask_loads[slot][chunk].wait()
        rows = pl.ds(chunk * width, width)
        seen = mask32[slot, rows].astype(F32).astype(BF16)
        mask16[slot, rows] = seen
        if chunk == LAST:
            late_seen[row * COLS + order[slot]] = seen

    item_load.start()
    for pieces in mask_loads[:2]:
        for copy in pieces:
            copy.start()
    for slot in range(COLS):
        if slot >= 2:
            mask_loads[slot][LAST].start()
        rate_late_loads[slot].start()

    item_load.wait()
    item16[...] = item0[...].astype(BF16)
    pl.semaphore_wait(barrier, 4)
    item_copy = copy_to(item16, item16_peer, item_sem, 0, pair)
    item_copy.start()
    mask_copies = []
    for chunk in range(CHUNKS):
        rows = pl.ds(chunk * width, width)
        convert(0, chunk)
        mask_copies.append(copy_to(mask16.at[0, rows], mask16_peer.at[0, rows], mask_sem, chunk, pair))
        mask_copies[-1].start()
    user_load.start()
    for pieces in mask_loads[2:]:
        for copy in pieces[:LAST]:
            copy.start()
    for copy in rate_loads:
        copy.start()
    late_copies = []
    for slot in range(COLS):
        if slot:
            convert(slot, LAST)
        rate_late_loads[slot].wait()
        rows = pl.ds(early, width)
        late_send[order[slot]] = jnp.where(mask32[slot, rows] > 0, rate[slot, rows], jnp.inf)
        late_copies.append(
            copy_to(late_send.at[order[slot]], late_recv.at[order[slot]], late_sem, slot, cross)
        )
        late_copies[-1].start()
    high, low = pair_products(item16[...].astype(F32))
    ffs[0, :, :items] = high
    ffs[0, :, items:] = low
    for chunk in range(LAST):
        convert(1, chunk)
    item_copy.wait_recv()
    high, low = pair_products(item16_peer[...].astype(F32))
    ffs[1, :, :items] = high
    ffs[1, :, items:] = low

    def gram_part(slot, chunk):
        mine = mask16[slot, pl.ds(chunk * width, width), :]
        peer = mask16_peer[slot // 2, pl.ds(chunk * width, width), :]
        total = dot_nt(ffs[0], jnp.concatenate([mine, mine], axis=1))
        return total + dot_nt(ffs[1], jnp.concatenate([peer, peer], axis=1))

    tiles = width // LANES
    whole_diags = RANK // 2

    def pack(gram, chunk):
        for d in range(whole_diags):
            for t in range(tiles):
                piece = gram[d * RANK:(d + 1) * RANK, t * LANES:(t + 1) * LANES]
                gram_send[chunk, d * tiles + t] = piece.astype(BF16)
        half = gram[whole_diags * RANK:whole_diags * RANK + RANK // 2]
        for t in range(0, tiles, 2):
            both = [half[:, u * LANES:(u + 1) * LANES] for u in (t, t + 1)]
            gram_send[chunk, whole_diags * tiles + t // 2] = jnp.concatenate(both, axis=0).astype(BF16)

    def unpack(chunk):
        diags = []
        for d in range(whole_diags):
            diags.append(jnp.concatenate([gram_recv[chunk, d * tiles + t].astype(F32) for t in range(tiles)], axis=1))
        pieces = []
        for t in range(0, tiles, 2):
            both = gram_recv[chunk, whole_diags * tiles + t // 2].astype(F32)
            for half in (both[:RANK // 2], both[RANK // 2:]):
                pieces.append(jnp.concatenate([half, half], axis=0))
        return diags + [jnp.concatenate(pieces, axis=1)]

    gram_copies = [copy_to(gram_send.at[chunk], gram_recv.at[chunk], gram_sem, chunk, far) for chunk in range(CHUNKS)]
    for chunk in range(CHUNKS):
        mask_copies[chunk].wait_recv()
        pack(gram_part(1, chunk), chunk)
        if chunk < EARLY:
            pl.when(core == 0)(gram_copies[chunk].start)
        if chunk == DELAY:
            for copy in gram_copies[:EARLY]:
                pl.when(core == 1)(copy.start)

    user_load.wait()

    def user_residual(slot, block):
        start = user0[:, block_rows(block)]
        scores = dot_nn(start.T.astype(BF16), item16[...])
        resid = jnp.where(mask32[slot] > 0, rate[slot] - scores, 0.0).astype(BF16)
        return dot_nt(item16[...], resid)

    rate_loads[0].wait()
    res_pair[0] = user_residual(0, diag_col)
    pair_copies = [copy_to(res_pair.at[slot], res_pair_recv.at[slot], pair_sem, slot, pair) for slot in range(2)]
    pair_copies[0].start()
    rate_loads[1].wait()
    far_part = user_residual(1, far_col)
    pair_copies[0].wait_recv()
    res_far[...] = (far_part + res_pair_recv[0]).astype(BF16)
    far_copy = copy_to(res_far, res_far_recv, far_sem, 0, far)
    far_copy.start()
    for copy in gram_copies[EARLY:]:
        copy.start()
    for chunk in range(LAST):
        convert(2, chunk)
    own_mask_copy = copy_to(mask16.at[2], mask16_peer.at[1], mask_sem, CHUNKS, pair)
    own_mask_copy.start()
    for chunk in range(LAST):
        convert(3, chunk)
    rate_loads[2].wait()
    res_pair[1] = user_residual(2, pair_col)
    pair_copies[1].start()
    rate_loads[3].wait()
    own_part = user_residual(3, col)
    own_mask_copy.wait_recv()
    for chunk in range(CHUNKS):
        gram_own[chunk] = gram_part(3, chunk)
    pair_copies[1].wait_recv()
    res_own[...] = own_part + res_pair_recv[1] - user_ridge * user0[:, block_rows(col)]

    def three_terms(values):
        high = values.astype(BF16)
        rest = values - high.astype(F32)
        middle = rest.astype(BF16)
        return jnp.concatenate([high, middle, (rest - middle.astype(F32)).astype(BF16)], axis=1)

    late_copies[0].wait_recv()
    for slot in range(COLS):
        seen_rate = jnp.where(mask32[slot] > 0, rate[slot], 0.0)
        split = three_terms(seen_rate)
        zrate[slot] = split[:early]
        late_rated[row * COLS + order[slot]] = split[early:]

    def item_part(entries, acc):
        factors = jnp.concatenate([fac[source, chunk] for source, _, chunk in entries], axis=1)
        rows = [pl.ds(chunk * width, width) for _, _, chunk in entries]
        seen = jnp.concatenate([mask16[slot, r, :] for (_, slot, _), r in zip(entries, rows)], axis=0)
        rated = jnp.concatenate([zrate[slot, r, :] for (_, slot, _), r in zip(entries, rows)], axis=0)
        pairs = jnp.concatenate(pair_products(factors.astype(F32)), axis=0)
        sums = (dot_nn(pairs, seen), dot_nn(factors, rated))
        return sums if acc is None else (acc[0] + sums[0], acc[1] + sums[1])

    def arrived(chunk):
        for copy in fac_copies[chunk]:
            copy.wait_recv()
        return [(source, slot, chunk) for _, source, slot in peers]

    def late_part(index):
        factors = late_fac[index]
        pairs = jnp.concatenate(pair_products(factors.astype(F32)), axis=0)
        gram = dot_nn(pairs, late_seen[index])
        rated = dot_nn(factors, late_rated[index])
        late_sums[index, :terms] = gram[:terms] + gram[terms:]
        late_sums[index, terms:] = rated[:, :items] + rated[:, items:2 * items] + rated[:, 2 * items:]

    far_copy.wait_recv()
    sums = None
    fac_copies = []
    user_copies = []

    def send_users(half, chunks):
        mine = user1.at[col, chunks]
        for lane, device in enumerate((pair, far)):
            user_copies.append(copy_to(mine, mine, user_sem, half * 3 + lane, device))
            user_copies[-1].start()

    def forward_users(half, chunks):
        user_copies[half * 2 + 1].wait_recv()
        theirs = user1.at[far_col, chunks]
        forwards.append(copy_to(theirs, theirs, user_sem, half * 3 + 2, pair))
        forwards[-1].start()

    forwards = []
    def solve(chunk):
        lanes = pl.ds(chunk * width, width)
        gram_copies[chunk].wait_recv()
        far_diags = unpack(chunk)
        diags = [gram_own[chunk, d * RANK:(d + 1) * RANK, :] + far_diags[d] for d in range(DIAGS)]
        start = user0[:, pl.ds(pl.multiple_of(col * span + chunk * width, width), width)]
        residual = res_own[:, lanes] + res_far_recv[:, lanes].astype(F32)
        return cg_solve(diags, residual, start, user_ridge)

    for chunk in range(LAST):
        solved = solve(chunk)
        fac[col, chunk] = solved.astype(BF16)
        sent = []
        for lane, (device, _, _) in enumerate(peers):
            sent.append(copy_to(fac.at[col, chunk], fac.at[col, chunk], fac_sem, chunk * 3 + lane, device))
        for copy in sent[::-1]:
            copy.start()
        fac_copies.append(sent)
        user1[col, chunk] = solved
        sums = item_part([(col, 3, chunk)], sums)
    send_users(0, pl.ds(0, LAST))
    solved = solve(LAST)
    mine = row * COLS + col
    late_fac[mine] = solved.astype(BF16)
    late_fac_copies = []
    for lane, device in enumerate(others):
        late_fac_copies.append(copy_to(late_fac.at[mine], late_fac.at[mine], late_fac_sem, lane, device))
    for copy in late_fac_copies[::-1]:
        copy.start()
    user1[col, LAST] = solved
    send_users(1, pl.ds(LAST, 1))
    entries = sum([arrived(chunk) for chunk in range(LAST - 1)], [])
    sums = item_part(entries, sums)
    entries = arrived(LAST - 1)
    sums = item_part(entries, sums)
    gram = sums[0][:terms] + sums[0][terms:]
    start = item16[...].astype(F32)

    def diagonals(full):
        return [full[d * RANK:(d + 1) * RANK] for d in range(DIAGS)]

    residual = sums[1][:, :items] + sums[1][:, items:2 * items] + sums[1][:, 2 * items:]
    residual = residual - apply_gram(diagonals(gram), start)
    high = residual.astype(BF16)
    item_send[:terms] = gram.astype(BF16)
    item_send[terms:terms + RANK] = high
    item_send[terms + RANK:] = (residual - high.astype(F32)).astype(BF16)
    cross_copy = copy_to(item_send, item_recv, cross_sem, 0, cross)
    pl.when(core == 0)(cross_copy.start)
    late_part(mine)
    pl.when(core == 1)(cross_copy.start)
    forward_users(0, pl.ds(0, LAST))
    for copy in late_fac_copies[:3]:
        copy.wait_recv()
    for _, source, _ in peers:
        late_part(row * COLS + source)
    forward_users(1, pl.ds(LAST, 1))
    for copy in late_copies[1:]:
        copy.wait_recv()
    for block in range(COLS):
        value = late_recv[block]
        seen = value < jnp.inf
        late_seen[(1 - row) * COLS + block] = seen.astype(F32).astype(BF16)
        late_rated[(1 - row) * COLS + block] = three_terms(jnp.where(seen, value, 0.0))
    for copy in late_fac_copies[3:]:
        copy.wait_recv()
    for block in range(COLS):
        late_part((1 - row) * COLS + block)
    late = late_sums[0]
    for index in range(1, 2 * COLS):
        late = late + late_sums[index]
    late_gram = late[:terms]
    late_residual = late[terms:] - apply_gram(diagonals(late_gram), start)

    for copy in [user_copies[0], user_copies[2]] + forwards:
        copy.wait_recv()
    for source in range(COLS):
        for chunk in range(CHUNKS):
            user_out[:, pl.ds(source * span + chunk * width, width)] = user1[source, chunk]

    cross_copy.wait_recv()
    full = item_send[...].astype(F32) + item_recv[...].astype(F32)
    residual = full[terms:terms + RANK] + full[terms + RANK:] + late_residual - item_ridge * item0[...]
    item_out[...] = cg_solve(diagonals(full[:terms] + late_gram), residual, item0[...], item_ridge)

    remote = [item_copy, own_mask_copy, far_copy, cross_copy] + late_copies + late_fac_copies + mask_copies + pair_copies + gram_copies + user_copies
    for copy in remote + sum(fac_copies, []) + forwards:
        copy.wait_send()


def write_kernel(user_ref, item_ref, user_out, item_out, sems):
    copies = [
        pltpu.make_async_copy(user_ref, user_out, sems.at[0]),
        pltpu.make_async_copy(item_ref, item_out, sems.at[1]),
    ]
    for copy in copies:
        copy.start()
    for copy in copies:
        copy.wait()


def solution(mesh):
    row_size = mesh.shape["row"]
    col_size = mesh.shape["col"]
    grid_spec = P(("part", "row"), "col")
    user_spec = P(("part", "row"), None)
    item_spec = P(("part", "col"), None)

    def local_step(ratings_blk, mask_blk, user_blk, item_blk):
        users, items = ratings_blk.shape
        span = users // COLS
        width = span // CHUNKS
        hbm_spec = pl.BlockSpec(memory_space=pltpu.HBM)
        vmem = pltpu.VMEM
        dma = pltpu.SemaphoreType.DMA
        terms = DIAGS * RANK
        packed = (RANK + 1) * width // (2 * LANES)
        user_new, item_new = pl.pallas_call(
            functools.partial(sweep_kernel, RIDGE_WEIGHT * items * col_size, RIDGE_WEIGHT * users * row_size),
            out_shape=(
                pltpu.VMEM((RANK, users), F32),
                pltpu.VMEM((RANK, items), F32),
            ),
            in_specs=[hbm_spec] * 4,
            out_specs=(pl.BlockSpec(memory_space=pltpu.VMEM),) * 2,
            scratch_shapes=[
                vmem((COLS, span, items), F32),
                vmem((COLS, span, items), jnp.int32),
                vmem((RANK, users), F32),
                vmem((RANK, items), F32),
                vmem((COLS, span, items), BF16),
                vmem((2, span, items), BF16),
                vmem((RANK, items), BF16),
                vmem((RANK, items), BF16),
                vmem((2, terms, 2 * items), BF16),
                vmem((COLS, LAST * width, 3 * items), BF16),
                vmem((CHUNKS, packed, RANK, LANES), BF16),
                vmem((CHUNKS, packed, RANK, LANES), BF16),
                vmem((CHUNKS, terms, width), F32),
                vmem((2, RANK, span), F32),
                vmem((2, RANK, span), F32),
                vmem((RANK, span), BF16),
                vmem((RANK, span), BF16),
                vmem((RANK, span), F32),
                vmem((COLS, LAST, RANK, width), BF16),
                vmem((COLS, CHUNKS, RANK, width), F32),
                vmem((terms + 2 * RANK, items), BF16),
                vmem((terms + 2 * RANK, items), BF16),
                vmem((COLS, width, items), F32),
                vmem((COLS, width, items), F32),
                vmem((2 * COLS, width, items), BF16),
                vmem((2 * COLS, width, 3 * items), BF16),
                vmem((2 * COLS, RANK, width), BF16),
                vmem((2 * COLS, terms + RANK, items), F32),
                dma((10 + COLS * CHUNKS,)),
                dma((2, 1)),
                dma((2, CHUNKS + 1)),
                dma((2, 2)),
                dma((2, 1)),
                dma((2, CHUNKS)),
                dma((2, LAST * 3)),
                dma((2, 6)),
                dma((2, 1)),
                dma((2, COLS)),
                dma((2, 2 * COLS - 1)),
            ],
            compiler_params=pltpu.CompilerParams(collective_id=0, has_side_effects=True, vmem_limit_bytes=60000 * 1024),
        )(ratings_blk, mask_blk, user_blk.T, item_blk.T)
        user_new, item_new = pl.pallas_call(
            write_kernel,
            out_shape=(
                jax.ShapeDtypeStruct((RANK, users), F32),
                jax.ShapeDtypeStruct((RANK, items), F32),
            ),
            in_specs=[pl.BlockSpec(memory_space=pltpu.VMEM)] * 2,
            out_specs=(hbm_spec, hbm_spec),
            scratch_shapes=[dma((2,))],
            compiler_params=pltpu.CompilerParams(vmem_limit_bytes=2**20),
        )(user_new, item_new)
        return user_new.T, item_new.T

    return jax.shard_map(local_step, mesh=mesh, in_specs=(grid_spec, grid_spec, user_spec, item_spec), out_specs=(user_spec, item_spec), check_vma=False)
```

```python
import functools

import jax
import jax.numpy as jnp
from jax import lax
from jax.experimental import pallas as pl
from jax.experimental.pallas import tpu as pltpu
from jax.sharding import PartitionSpec as P

CG_STEPS = 4
RIDGE_WEIGHT = 0.0005
RANK = 16
DIAGS = RANK // 2 + 1
MESH = pl.DeviceIdType.MESH
F32 = jnp.float32
BF16 = jnp.bfloat16
COLS = 4
CHUNKS = 4
EARLY = 2
DELAY = 2
LAST = CHUNKS - 1
LANES = 128


def dot_nt(a, b):
    return lax.dot_general(a, b, (((1,), (1,)), ((), ())), preferred_element_type=F32)


def dot_nn(a, b):
    return lax.dot_general(a, b, (((1,), (0,)), ((), ())), preferred_element_type=F32)


def turn(x, shift):
    return x if shift % RANK == 0 else pltpu.roll(x, shift % RANK, 0)


def pair_products(fac):
    prods = jnp.concatenate([fac * turn(fac, -d) for d in range(DIAGS)], axis=0)
    high = prods.astype(BF16)
    low = (prods - high.astype(F32)).astype(BF16)
    return high, low


def apply_gram(diags, vec):
    parts = [diags[d] * turn(vec, -d) for d in range(DIAGS)]
    parts += [turn(diags[d] * vec, d) for d in range(1, RANK // 2)]
    while len(parts) > 1:
        parts = [sum(parts[i:i + 2][1:], parts[i]) for i in range(0, len(parts), 2)]
    return parts[0]


def cg_solve(diags, residual, start, ridge):
    direction = residual
    estimate = start
    res_sq = jnp.sum(residual * residual, axis=0, keepdims=True)
    for cg_step in range(CG_STEPS):
        gram_dir = apply_gram(diags, direction) + ridge * direction
        step_size = res_sq / jnp.sum(direction * gram_dir, axis=0, keepdims=True)
        estimate = estimate + step_size * direction
        if cg_step + 1 < CG_STEPS:
            residual = residual - step_size * gram_dir
            new_sq = jnp.sum(residual * residual, axis=0, keepdims=True)
            direction = residual + (new_sq / res_sq) * direction
            res_sq = new_sq
    return estimate


def sweep_kernel(
    user_ridge, item_ridge,
    ratings_hbm, mask_hbm, user_hbm, item_hbm,
    user_out, item_out,
    rate, mask32, user0, item0,
    mask16, mask16_peer, item16, item16_peer, ffs, zrate,
    gram_send, gram_recv, gram_own,
    res_pair, res_pair_recv, res_far, res_far_recv, res_own,
    fac, user1, item_send, item_recv,
    late_send, late_recv, late_seen, late_rated, late_fac, late_sums,
    in_sem, item_sem, mask_sem, pair_sem, far_sem, gram_sem, fac_sem, user_sem, cross_sem, late_sem, late_fac_sem,
):
    part = lax.axis_index("part")
    row = lax.axis_index("row")
    col = lax.axis_index("col")
    chip = col // 2
    core = col % 2
    pair_col = chip * 2 + (1 - core)
    far_col = (1 - chip) * 2 + core
    diag_col = (1 - chip) * 2 + (1 - core)
    pair = (part, row, pair_col)
    far = (part, row, far_col)
    diag = (part, row, diag_col)
    cross = (part, 1 - row, col)
    peers = ((pair, pair_col, 2), (far, far_col, 1), (diag, diag_col, 0))
    others = [device for device, _, _ in peers] + [cross] + [(part, 1 - row, source) for _, source, _ in peers]

    span = mask16.shape[1]
    width = span // CHUNKS
    items = item0.shape[1]
    terms = DIAGS * RANK

    def copy_to(src, dst, sems, slot, device):
        return pltpu.make_async_remote_copy(
            src_ref=src, dst_ref=dst, send_sem=sems.at[0, slot], recv_sem=sems.at[1, slot],
            device_id=device, device_id_type=MESH,
        )

    barrier = pltpu.get_barrier_semaphore()
    for device in (pair, far, diag, cross):
        pl.semaphore_signal(barrier, inc=1, device_id=device, device_id_type=MESH)

    order = (diag_col, far_col, pair_col, col)

    def load(src, dst, slot):
        return pltpu.make_async_copy(src, dst, in_sem.at[slot])

    def block_rows(block):
        return pl.ds(pl.multiple_of(block * span, span), span)

    item_load = load(item_hbm, item0, 0)
    user_load = load(user_hbm, user0, 1)
    early = LAST * width
    rate_loads = []
    rate_late_loads = []
    for slot, block in enumerate(order):
        rows = pl.ds(pl.multiple_of(block * span, span), early)
        rate_loads.append(load(ratings_hbm.at[rows], rate.at[slot, pl.ds(0, early)], 2 + slot))
        rows = pl.ds(pl.multiple_of(block * span + early, width), width)
        rate_late_loads.append(load(ratings_hbm.at[rows], rate.at[slot, pl.ds(early, width)], 6 + slot))
    mask_loads = []
    for slot, block in enumerate(order):
        pieces = []
        for chunk in range(CHUNKS):
            rows = pl.ds(pl.multiple_of(block * span + chunk * width, width), width)
            dst = mask32.at[slot, pl.ds(chunk * width, width)]
            pieces.append(load(mask_hbm.at[rows], dst, 10 + slot * CHUNKS + chunk))
        mask_loads.append(pieces)

    def convert(slot, chunk):
        mask_loads[slot][chunk].wait()
        rows = pl.ds(chunk * width, width)
        seen = mask32[slot, rows].astype(F32).astype(BF16)
        mask16[slot, rows] = seen
        if chunk == LAST:
            late_seen[row * COLS + order[slot]] = seen

    item_load.start()
    for pieces in mask_loads[:2]:
        for copy in pieces:
            copy.start()
    for slot in range(COLS):
        if slot >= 2:
            mask_loads[slot][LAST].start()
        rate_late_loads[slot].start()

    item_load.wait()
    item16[...] = item0[...].astype(BF16)
    pl.semaphore_wait(barrier, 4)
    item_copy = copy_to(item16, item16_peer, item_sem, 0, pair)
    item_copy.start()
    mask_copies = []
    for chunk in range(CHUNKS):
        rows = pl.ds(chunk * width, width)
        convert(0, chunk)
        mask_copies.append(copy_to(mask16.at[0, rows], mask16_peer.at[0, rows], mask_sem, chunk, pair))
        mask_copies[-1].start()
    user_load.start()
    for pieces in mask_loads[2:]:
        for copy in pieces[:LAST]:
            copy.start()
    for copy in rate_loads:
        copy.start()
    late_copies = []
    for slot in range(COLS):
        if slot:
            convert(slot, LAST)
        rate_late_loads[slot].wait()
        rows = pl.ds(early, width)
        late_send[order[slot]] = jnp.where(mask32[slot, rows] > 0, rate[slot, rows], jnp.inf)
        late_copies.append(
            copy_to(late_send.at[order[slot]], late_recv.at[order[slot]], late_sem, slot, cross)
        )
        late_copies[-1].start()
    high, low = pair_products(item16[...].astype(F32))
    ffs[0, :, :items] = high
    ffs[0, :, items:] = low
    for chunk in range(LAST):
        convert(1, chunk)
    item_copy.wait_recv()
    high, low = pair_products(item16_peer[...].astype(F32))
    ffs[1, :, :items] = high
    ffs[1, :, items:] = low

    def gram_part(slot, chunk):
        mine = mask16[slot, pl.ds(chunk * width, width), :]
        peer = mask16_peer[slot // 2, pl.ds(chunk * width, width), :]
        total = dot_nt(ffs[0], jnp.concatenate([mine, mine], axis=1))
        return total + dot_nt(ffs[1], jnp.concatenate([peer, peer], axis=1))

    tiles = width // LANES
    whole_diags = RANK // 2

    def pack(gram, chunk):
        for d in range(whole_diags):
            for t in range(tiles):
                piece = gram[d * RANK:(d + 1) * RANK, t * LANES:(t + 1) * LANES]
                gram_send[chunk, d * tiles + t] = piece.astype(BF16)
        half = gram[whole_diags * RANK:whole_diags * RANK + RANK // 2]
        for t in range(0, tiles, 2):
            both = [half[:, u * LANES:(u + 1) * LANES] for u in (t, t + 1)]
            gram_send[chunk, whole_diags * tiles + t // 2] = jnp.concatenate(both, axis=0).astype(BF16)

    def unpack(chunk):
        diags = []
        for d in range(whole_diags):
            diags.append(jnp.concatenate([gram_recv[chunk, d * tiles + t].astype(F32) for t in range(tiles)], axis=1))
        pieces = []
        for t in range(0, tiles, 2):
            both = gram_recv[chunk, whole_diags * tiles + t // 2].astype(F32)
            for half in (both[:RANK // 2], both[RANK // 2:]):
                pieces.append(jnp.concatenate([half, half], axis=0))
        return diags + [jnp.concatenate(pieces, axis=1)]

    gram_copies = [copy_to(gram_send.at[chunk], gram_recv.at[chunk], gram_sem, chunk, far) for chunk in range(CHUNKS)]
    for chunk in range(CHUNKS):
        mask_copies[chunk].wait_recv()
        pack(gram_part(1, chunk), chunk)
        if chunk < EARLY:
            pl.when(core == 0)(gram_copies[chunk].start)
        if chunk == DELAY:
            for copy in gram_copies[:EARLY]:
                pl.when(core == 1)(copy.start)

    user_load.wait()

    def user_residual(slot, block):
        start = user0[:, block_rows(block)]
        scores = dot_nn(start.T.astype(BF16), item16[...])
        resid = jnp.where(mask32[slot] > 0, rate[slot] - scores, 0.0).astype(BF16)
        return dot_nt(item16[...], resid)

    rate_loads[0].wait()
    res_pair[0] = user_residual(0, diag_col)
    pair_copies = [copy_to(res_pair.at[slot], res_pair_recv.at[slot], pair_sem, slot, pair) for slot in range(2)]
    pair_copies[0].start()
    rate_loads[1].wait()
    far_part = user_residual(1, far_col)
    pair_copies[0].wait_recv()
    total = (far_part + res_pair_recv[0]).astype(BF16)
    for chunk in range(CHUNKS):
        res_far[chunk] = total[:, chunk * width:(chunk + 1) * width]
    far_copies = []
    for half, chunks in enumerate((pl.ds(0, LAST), pl.ds(LAST, 1))):
        far_copies.append(copy_to(res_far.at[chunks], res_far_recv.at[chunks], far_sem, half, far))
    far_copies[0].start()
    for copy in gram_copies[EARLY:LAST] + [far_copies[1], gram_copies[LAST]]:
        copy.start()
    for chunk in range(LAST):
        convert(2, chunk)
    own_mask_copy = copy_to(mask16.at[2], mask16_peer.at[1], mask_sem, CHUNKS, pair)
    own_mask_copy.start()
    for chunk in range(LAST):
        convert(3, chunk)
    rate_loads[2].wait()
    res_pair[1] = user_residual(2, pair_col)
    pair_copies[1].start()
    rate_loads[3].wait()
    own_part = user_residual(3, col)
    own_mask_copy.wait_recv()
    for chunk in range(CHUNKS):
        gram_own[chunk] = gram_part(3, chunk)
    pair_copies[1].wait_recv()
    res_own[...] = own_part + res_pair_recv[1] - user_ridge * user0[:, block_rows(col)]

    def three_terms(values):
        high = values.astype(BF16)
        rest = values - high.astype(F32)
        middle = rest.astype(BF16)
        return jnp.concatenate([high, middle, (rest - middle.astype(F32)).astype(BF16)], axis=1)

    late_copies[0].wait_recv()
    for slot in range(COLS):
        seen_rate = jnp.where(mask32[slot] > 0, rate[slot], 0.0)
        split = three_terms(seen_rate)
        zrate[slot] = split[:early]
        late_rated[row * COLS + order[slot]] = split[early:]

    def item_part(entries, acc):
        factors = jnp.concatenate([fac[source, chunk] for source, _, chunk in entries], axis=1)
        rows = [pl.ds(chunk * width, width) for _, _, chunk in entries]
        seen = jnp.concatenate([mask16[slot, r, :] for (_, slot, _), r in zip(entries, rows)], axis=0)
        rated = jnp.concatenate([zrate[slot, r, :] for (_, slot, _), r in zip(entries, rows)], axis=0)
        pairs = jnp.concatenate(pair_products(factors.astype(F32)), axis=0)
        sums = (dot_nn(pairs, seen), dot_nn(factors, rated))
        return sums if acc is None else (acc[0] + sums[0], acc[1] + sums[1])

    def split_late(slot):
        value = late_recv[order[slot]]
        seen = value < jnp.inf
        late_seen[(1 - row) * COLS + order[slot]] = seen.astype(F32).astype(BF16)
        late_rated[(1 - row) * COLS + order[slot]] = three_terms(jnp.where(seen, value, 0.0))

    def arrived(chunk, lanes):
        for lane in lanes:
            fac_copies[chunk][lane].wait_recv()
        return [(peers[lane][1], peers[lane][2], chunk) for lane in lanes]

    def late_part(index):
        factors = late_fac[index]
        pairs = jnp.concatenate(pair_products(factors.astype(F32)), axis=0)
        gram = dot_nn(pairs, late_seen[index])
        rated = dot_nn(factors, late_rated[index])
        late_sums[index, :terms] = gram[:terms] + gram[terms:]
        late_sums[index, terms:] = rated[:, :items] + rated[:, items:2 * items] + rated[:, 2 * items:]

    far_copies[0].wait_recv()
    sums = None
    fac_copies = []
    user_copies = []

    def send_users(half, chunks):
        mine = user1.at[col, chunks]
        for lane, device in enumerate((pair, far)):
            user_copies.append(copy_to(mine, mine, user_sem, half * 3 + lane, device))
            user_copies[-1].start()

    def forward_users(half, chunks):
        user_copies[half * 2 + 1].wait_recv()
        theirs = user1.at[far_col, chunks]
        forwards.append(copy_to(theirs, theirs, user_sem, half * 3 + 2, pair))
        forwards[-1].start()

    forwards = []
    def solve(chunk):
        lanes = pl.ds(chunk * width, width)
        gram_copies[chunk].wait_recv()
        far_diags = unpack(chunk)
        diags = [gram_own[chunk, d * RANK:(d + 1) * RANK, :] + far_diags[d] for d in range(DIAGS)]
        start = user0[:, pl.ds(pl.multiple_of(col * span + chunk * width, width), width)]
        residual = res_own[:, lanes] + res_far_recv[chunk].astype(F32)
        return cg_solve(diags, residual, start, user_ridge)

    for chunk in range(LAST):
        solved = solve(chunk)
        fac[col, chunk] = solved.astype(BF16)
        sent = []
        for lane, (device, _, _) in enumerate(peers):
            sent.append(copy_to(fac.at[col, chunk], fac.at[col, chunk], fac_sem, chunk * 3 + lane, device))
        for copy in sent[::-1]:
            copy.start()
        fac_copies.append(sent)
        user1[col, chunk] = solved
        sums = item_part([(col, 3, chunk)], sums)
    send_users(0, pl.ds(0, LAST))
    far_copies[1].wait_recv()
    solved = solve(LAST)
    mine = row * COLS + col
    late_fac[mine] = solved.astype(BF16)
    late_fac_copies = []
    for lane, device in enumerate(others):
        late_fac_copies.append(copy_to(late_fac.at[mine], late_fac.at[mine], late_fac_sem, lane, device))
    for copy in late_fac_copies[::-1]:
        copy.start()
    user1[col, LAST] = solved
    send_users(1, pl.ds(LAST, 1))
    entries = sum([arrived(chunk, (0, 1, 2)) for chunk in range(LAST - 1)], arrived(LAST - 1, (0,)))
    sums = item_part(entries, sums)
    entries = arrived(LAST - 1, (1, 2))
    sums = item_part(entries, sums)
    gram = sums[0][:terms] + sums[0][terms:]
    start = item16[...].astype(F32)

    def diagonals(full):
        return [full[d * RANK:(d + 1) * RANK] for d in range(DIAGS)]

    residual = sums[1][:, :items] + sums[1][:, items:2 * items] + sums[1][:, 2 * items:]
    residual = residual - apply_gram(diagonals(gram), start)
    high = residual.astype(BF16)
    item_send[:terms] = gram.astype(BF16)
    item_send[terms:terms + RANK] = high
    item_send[terms + RANK:] = (residual - high.astype(F32)).astype(BF16)
    cross_copy = copy_to(item_send, item_recv, cross_sem, 0, cross)
    cross_copy.start()
    late_part(mine)
    forward_users(0, pl.ds(0, LAST))
    for slot in range(COLS - 1):
        if slot:
            late_copies[slot].wait_recv()
        split_late(slot)
    for copy in late_fac_copies[:3]:
        copy.wait_recv()
    for _, source, _ in peers:
        late_part(row * COLS + source)
    forward_users(1, pl.ds(LAST, 1))
    for copy in late_fac_copies[3:]:
        copy.wait_recv()
    for slot in range(COLS - 1):
        late_part((1 - row) * COLS + order[slot])
    late_copies[COLS - 1].wait_recv()
    split_late(COLS - 1)
    late_part((1 - row) * COLS + order[COLS - 1])
    late = late_sums[0]
    for index in range(1, 2 * COLS):
        late = late + late_sums[index]
    late_gram = late[:terms]
    late_residual = late[terms:] - apply_gram(diagonals(late_gram), start)

    for copy in [user_copies[0], user_copies[2]] + forwards:
        copy.wait_recv()
    for source in range(COLS):
        for chunk in range(CHUNKS):
            user_out[:, pl.ds(source * span + chunk * width, width)] = user1[source, chunk]

    cross_copy.wait_recv()
    full = item_send[...].astype(F32) + item_recv[...].astype(F32)
    residual = full[terms:terms + RANK] + full[terms + RANK:] + late_residual - item_ridge * item0[...]
    item_out[...] = cg_solve(diagonals(full[:terms] + late_gram), residual, item0[...], item_ridge)

    remote = [item_copy, own_mask_copy, cross_copy] + far_copies + late_copies + late_fac_copies + mask_copies + pair_copies + gram_copies + user_copies
    for copy in remote + sum(fac_copies, []) + forwards:
        copy.wait_send()


def write_kernel(user_ref, item_ref, user_out, item_out, sems):
    copies = [
        pltpu.make_async_copy(user_ref, user_out, sems.at[0]),
        pltpu.make_async_copy(item_ref, item_out, sems.at[1]),
    ]
    for copy in copies:
        copy.start()
    for copy in copies:
        copy.wait()


def solution(mesh):
    row_size = mesh.shape["row"]
    col_size = mesh.shape["col"]
    grid_spec = P(("part", "row"), "col")
    user_spec = P(("part", "row"), None)
    item_spec = P(("part", "col"), None)

    def local_step(ratings_blk, mask_blk, user_blk, item_blk):
        users, items = ratings_blk.shape
        span = users // COLS
        width = span // CHUNKS
        hbm_spec = pl.BlockSpec(memory_space=pltpu.HBM)
        vmem = pltpu.VMEM
        dma = pltpu.SemaphoreType.DMA
        terms = DIAGS * RANK
        packed = (RANK + 1) * width // (2 * LANES)
        user_new, item_new = pl.pallas_call(
            functools.partial(sweep_kernel, RIDGE_WEIGHT * items * col_size, RIDGE_WEIGHT * users * row_size),
            out_shape=(
                pltpu.VMEM((RANK, users), F32),
                pltpu.VMEM((RANK, items), F32),
            ),
            in_specs=[hbm_spec] * 4,
            out_specs=(pl.BlockSpec(memory_space=pltpu.VMEM),) * 2,
            scratch_shapes=[
                vmem((COLS, span, items), F32),
                vmem((COLS, span, items), jnp.int32),
                vmem((RANK, users), F32),
                vmem((RANK, items), F32),
                vmem((COLS, span, items), BF16),
                vmem((2, span, items), BF16),
                vmem((RANK, items), BF16),
                vmem((RANK, items), BF16),
                vmem((2, terms, 2 * items), BF16),
                vmem((COLS, LAST * width, 3 * items), BF16),
                vmem((CHUNKS, packed, RANK, LANES), BF16),
                vmem((CHUNKS, packed, RANK, LANES), BF16),
                vmem((CHUNKS, terms, width), F32),
                vmem((2, RANK, span), F32),
                vmem((2, RANK, span), F32),
                vmem((CHUNKS, RANK, width), BF16),
                vmem((CHUNKS, RANK, width), BF16),
                vmem((RANK, span), F32),
                vmem((COLS, LAST, RANK, width), BF16),
                vmem((COLS, CHUNKS, RANK, width), F32),
                vmem((terms + 2 * RANK, items), BF16),
                vmem((terms + 2 * RANK, items), BF16),
                vmem((COLS, width, items), F32),
                vmem((COLS, width, items), F32),
                vmem((2 * COLS, width, items), BF16),
                vmem((2 * COLS, width, 3 * items), BF16),
                vmem((2 * COLS, RANK, width), BF16),
                vmem((2 * COLS, terms + RANK, items), F32),
                dma((10 + COLS * CHUNKS,)),
                dma((2, 1)),
                dma((2, CHUNKS + 1)),
                dma((2, 2)),
                dma((2, 2)),
                dma((2, CHUNKS)),
                dma((2, LAST * 3)),
                dma((2, 6)),
                dma((2, 1)),
                dma((2, COLS)),
                dma((2, 2 * COLS - 1)),
            ],
            compiler_params=pltpu.CompilerParams(collective_id=0, has_side_effects=True, vmem_limit_bytes=60000 * 1024),
        )(ratings_blk, mask_blk, user_blk.T, item_blk.T)
        user_new, item_new = pl.pallas_call(
            write_kernel,
            out_shape=(
                jax.ShapeDtypeStruct((RANK, users), F32),
                jax.ShapeDtypeStruct((RANK, items), F32),
            ),
            in_specs=[pl.BlockSpec(memory_space=pltpu.VMEM)] * 2,
            out_specs=(hbm_spec, hbm_spec),
            scratch_shapes=[dma((2,))],
            compiler_params=pltpu.CompilerParams(vmem_limit_bytes=2**20),
        )(user_new, item_new)
        return user_new.T, item_new.T

    return jax.shard_map(local_step, mesh=mesh, in_specs=(grid_spec, grid_spec, user_spec, item_spec), out_specs=(user_spec, item_spec), check_vma=False)
```

```python
import functools

import jax
import jax.numpy as jnp
from jax import lax
from jax.experimental import pallas as pl
from jax.experimental.pallas import tpu as pltpu
from jax.sharding import PartitionSpec as P

CG_STEPS = 4
RIDGE_WEIGHT = 0.0005
RANK = 16
DIAGS = RANK // 2 + 1
MESH = pl.DeviceIdType.MESH
F32 = jnp.float32
BF16 = jnp.bfloat16
COLS = 4
LANES = 128
HALF = RANK // 2
WIDTHS = (256, 256, 128, 256, 128)
STARTS = tuple(sum(WIDTHS[:i]) for i in range(len(WIDTHS)))
CHUNKS = len(WIDTHS)
LATE = 3
DIRECT = 128


def dot_nt(a, b):
    return lax.dot_general(a, b, (((1,), (1,)), ((), ())), preferred_element_type=F32)


def dot_nn(a, b):
    return lax.dot_general(a, b, (((1,), (0,)), ((), ())), preferred_element_type=F32)


def turn(x, shift):
    return x if shift % RANK == 0 else pltpu.roll(x, shift % RANK, 0)


def pair_products(fac):
    prods = jnp.concatenate([fac * turn(fac, -d) for d in range(DIAGS)], axis=0)
    high = prods.astype(BF16)
    low = (prods - high.astype(F32)).astype(BF16)
    return high, low


def apply_gram(diags, vec):
    parts = [diags[d] * turn(vec, -d) for d in range(DIAGS)]
    parts += [turn(diags[d] * vec, d) for d in range(1, RANK // 2)]
    while len(parts) > 1:
        parts = [sum(parts[i:i + 2][1:], parts[i]) for i in range(0, len(parts), 2)]
    return parts[0]


def cg_solve(diags, residual, start, ridge):
    direction = residual
    estimate = start
    res_sq = jnp.sum(residual * residual, axis=0, keepdims=True)
    for cg_step in range(CG_STEPS):
        gram_dir = apply_gram(diags, direction) + ridge * direction
        step_size = res_sq / jnp.sum(direction * gram_dir, axis=0, keepdims=True)
        estimate = estimate + step_size * direction
        if cg_step + 1 < CG_STEPS:
            residual = residual - step_size * gram_dir
            new_sq = jnp.sum(residual * residual, axis=0, keepdims=True)
            direction = residual + (new_sq / res_sq) * direction
            res_sq = new_sq
    return estimate


def far_span(chunk):
    skip = DIRECT if chunk == 0 else 0
    return STARTS[chunk] + skip, WIDTHS[chunk] - skip


def packed_tiles(chunk):
    tiles = far_span(chunk)[1] // LANES
    return HALF * tiles + (tiles + 1) // 2


PACKED = tuple(packed_tiles(chunk) for chunk in range(CHUNKS))


def chunk_tiles(chunk):
    return range(STARTS[chunk] // LANES, (STARTS[chunk] + WIDTHS[chunk]) // LANES)


def side_by_side(blocks):
    return jnp.concatenate(list(blocks), axis=1)


def stacked(blocks):
    return jnp.concatenate(list(blocks), axis=0)


def three_terms(values):
    high = values.astype(BF16)
    rest = values - high.astype(F32)
    middle = rest.astype(BF16)
    return side_by_side([high, middle, (rest - middle.astype(F32)).astype(BF16)])


def diagonals(full):
    return [full[d * RANK:(d + 1) * RANK] for d in range(DIAGS)]


def sweep_kernel(
    user_ridge, item_ridge,
    ratings_hbm, mask_hbm, user_hbm, item_hbm,
    user_out, item_out,
    rate, mask32, user0, item0,
    mask16, mask16_peer, mask16_direct, item16, item16_peer, ffs, zrate,
    gram_send, gram_recv, gram_own,
    res_pair, res_pair_recv, res_far, res_far_recv, res_own,
    fac, user1, item_send, item_recv,
    late_send, late_recv, late_seen, late_rated, late_fac,
    in_sem, direct_sem, item_sem, mask_sem, pair_sem, far_sem, gram_sem, fac_sem, user_sem, cross_sem, late_sem, late_fac_sem,
):
    part = lax.axis_index("part")
    row = lax.axis_index("row")
    col = lax.axis_index("col")
    chip = col // 2
    core = col % 2
    pair_col = chip * 2 + (1 - core)
    far_col = (1 - chip) * 2 + core
    diag_col = (1 - chip) * 2 + (1 - core)
    pair = (part, row, pair_col)
    far = (part, row, far_col)
    diag = (part, row, diag_col)
    cross = (part, 1 - row, col)
    peers = ((pair, pair_col, 2), (far, far_col, 1), (diag, diag_col, 0))
    others = [device for device, _, _ in peers] + [cross] + [(part, 1 - row, source) for _, source, _ in peers]

    span = mask16.shape[1]
    items = item0.shape[1]
    terms = DIAGS * RANK
    early = STARTS[LATE]
    late = span - early

    def copy_to(src, dst, sems, slot, device):
        return pltpu.make_async_remote_copy(
            src_ref=src, dst_ref=dst, send_sem=sems.at[0, slot], recv_sem=sems.at[1, slot],
            device_id=device, device_id_type=MESH,
        )

    barrier = pltpu.get_barrier_semaphore()
    for device in (pair, far, diag, cross):
        pl.semaphore_signal(barrier, inc=1, device_id=device, device_id_type=MESH)

    order = (diag_col, far_col, pair_col, col)

    def load(src, dst, slot):
        return pltpu.make_async_copy(src, dst, in_sem.at[slot])

    def block_rows(block, start=0, size=span):
        return pl.ds(pl.multiple_of(block * span + start, LANES), size)

    def chunk_rows(chunk):
        return pl.ds(STARTS[chunk], WIDTHS[chunk])

    item_load = load(item_hbm, item0, 0)
    user_load = load(user_hbm, user0, 1)
    rate_loads = []
    rate_late_loads = []
    mask_loads = []
    for slot, block in enumerate(order):
        rate_loads.append(load(ratings_hbm.at[block_rows(block, 0, early)], rate.at[slot, pl.ds(0, early)], 2 + slot))
        rate_late_loads.append(load(ratings_hbm.at[block_rows(block, early, late)], rate.at[slot, pl.ds(early, late)], 6 + slot))
        pieces = []
        for chunk in range(CHUNKS):
            src = mask_hbm.at[block_rows(block, STARTS[chunk], WIDTHS[chunk])]
            pieces.append(load(src, mask32.at[slot, chunk_rows(chunk)], 10 + slot * CHUNKS + chunk))
        mask_loads.append(pieces)

    def convert(slot, chunks):
        for chunk in chunks:
            mask_loads[slot][chunk].wait()
            rows = chunk_rows(chunk)
            seen = mask32[slot, rows].astype(F32).astype(BF16)
            mask16[slot, rows] = seen
            if chunk >= LATE:
                late_seen[row * COLS + order[slot], pl.ds(STARTS[chunk] - early, WIDTHS[chunk])] = seen

    item_load.start()
    for pieces in mask_loads[:2]:
        for copy in pieces:
            copy.start()
    for slot in range(COLS):
        if slot >= 2:
            for copy in mask_loads[slot][LATE:]:
                copy.start()
        rate_late_loads[slot].start()

    item_load.wait()
    item16[...] = item0[...].astype(BF16)
    pl.semaphore_wait(barrier, 4)
    item_copies = [copy_to(item16, item16_peer.at[lane], item_sem, lane, device) for lane, (device, _, _) in enumerate(peers)]
    for copy in item_copies:
        copy.start()
    mask_copies = []
    direct_copies = []
    first = pl.ds(0, DIRECT)
    late_copies = []

    def send_late(slot):
        rate_late_loads[slot].wait()
        rows = pl.ds(early, late)
        late_send[order[slot]] = jnp.where(mask32[slot, rows] > 0, rate[slot, rows], jnp.inf).astype(BF16)
        late_copies.append(copy_to(late_send.at[order[slot]], late_recv.at[order[slot]], late_sem, slot, cross))
        late_copies[-1].start()

    for chunk in range(CHUNKS):
        rows = pl.ds(*far_span(chunk))
        convert(0, (chunk,))
        mask_copies.append(copy_to(mask16.at[0, rows], mask16_peer.at[0, rows], mask_sem, chunk, pair))
        mask_copies[-1].start()
        if chunk == 0:
            direct_copies.append(copy_to(mask16.at[0, first], mask16_direct.at[1], direct_sem, 1, diag))
            direct_copies[-1].start()
            convert(1, (0,))
            direct_copies.append(copy_to(mask16.at[1, first], mask16_direct.at[0], direct_sem, 0, far))
            direct_copies[-1].start()
    user_load.start()
    for pieces in mask_loads[2:]:
        for copy in pieces[:LATE]:
            copy.start()
    for copy in rate_loads:
        copy.start()
    send_late(0)
    for slot in range(1, COLS):
        convert(slot, range(LATE, CHUNKS))
        send_late(slot)

    def put_products(index, factors):
        high, low = pair_products(factors.astype(F32))
        ffs[index, :, :items] = high
        ffs[index, :, items:] = low

    put_products(0, item16[...])
    convert(1, range(1, LATE))
    item_copies[0].wait_recv()
    put_products(1, item16_peer[0])

    def gram_of(index, seen):
        return dot_nt(ffs[index], side_by_side([seen, seen]))

    def gram_part(slot, rows):
        return gram_of(0, mask16[slot, rows, :]) + gram_of(1, mask16_peer[slot // 2, rows, :])

    def pack(gram, chunk):
        tiles = gram.shape[1] // LANES
        base = sum(PACKED[:chunk])
        for d in range(HALF):
            for t in range(tiles):
                piece = gram[d * RANK:(d + 1) * RANK, t * LANES:(t + 1) * LANES]
                gram_send[base + d * tiles + t] = piece.astype(BF16)
        half = gram[HALF * RANK:HALF * RANK + HALF]
        for t in range(0, tiles, 2):
            both = [half[:, min(u, tiles - 1) * LANES:][:, :LANES] for u in (t, t + 1)]
            gram_send[base + HALF * tiles + t // 2] = stacked(both).astype(BF16)

    def unpack(chunk):
        gap = far_span(chunk)[1]
        tiles = gap // LANES
        base = sum(PACKED[:chunk])
        diags = [side_by_side(gram_recv[base + d * tiles + t].astype(F32) for t in range(tiles)) for d in range(HALF)]
        pieces = []
        for t in range(0, tiles, 2):
            both = gram_recv[base + HALF * tiles + t // 2].astype(F32)
            for half in (both[:HALF], both[HALF:])[:tiles - t]:
                pieces.append(stacked([half, half]))
        diags.append(side_by_side(pieces))
        pad = WIDTHS[chunk] - gap
        return [side_by_side([jnp.zeros((RANK, pad), F32), d]) if pad else d for d in diags]

    gram_copies = []
    for chunk in range(CHUNKS):
        part_of = pl.ds(sum(PACKED[:chunk]), PACKED[chunk])
        gram_copies.append(copy_to(gram_send.at[part_of], gram_recv.at[part_of], gram_sem, chunk, far))

    def far_gram(chunk):
        mask_copies[chunk].wait_recv()
        pack(gram_part(1, pl.ds(*far_span(chunk))), chunk)

    for chunk in range(2):
        far_gram(chunk)
        gram_copies[chunk].start()

    user_load.wait()

    def user_residual(slot, block):
        start = user0[:, block_rows(block)]
        scores = dot_nn(start.T.astype(BF16), item16[...])
        resid = jnp.where(mask32[slot] > 0, rate[slot] - scores, 0.0).astype(BF16)
        return dot_nt(item16[...], resid)

    rate_loads[0].wait()
    res_pair[0] = user_residual(0, diag_col)
    pair_copies = [copy_to(res_pair.at[slot], res_pair_recv.at[slot], pair_sem, slot, pair) for slot in range(2)]
    pair_copies[0].start()
    rate_loads[1].wait()
    far_part = user_residual(1, far_col)
    far_gram(2)
    pair_copies[0].wait_recv()
    total = (far_part + res_pair_recv[0]).astype(BF16)
    for t in range(span // LANES):
        res_far[t] = total[:, t * LANES:(t + 1) * LANES]
    far_copies = []
    for half, tiles in enumerate((pl.ds(0, early // LANES), pl.ds(early // LANES, late // LANES))):
        far_copies.append(copy_to(res_far.at[tiles], res_far_recv.at[tiles], far_sem, half, far))
    for copy in (far_copies[0], gram_copies[2], far_copies[1]):
        copy.start()
    for chunk in range(LATE, CHUNKS):
        far_gram(chunk)
        gram_copies[chunk].start()
    convert(2, range(LATE))
    own_mask_copy = copy_to(mask16.at[2], mask16_peer.at[1], mask_sem, CHUNKS, pair)
    own_mask_copy.start()
    convert(3, range(LATE))
    rate_loads[2].wait()
    res_pair[1] = user_residual(2, pair_col)
    pair_copies[1].start()
    rate_loads[3].wait()
    own_part = user_residual(3, col)
    own_mask_copy.wait_recv()
    for chunk in range(CHUNKS):
        gram_own[:, chunk_rows(chunk)] = gram_part(3, chunk_rows(chunk))
    for lane in range(2):
        item_copies[1 + lane].wait_recv()
        direct_copies[1 - lane].wait_recv()
        put_products(2 + lane, item16_peer[1 + lane])
        gram_own[:, :DIRECT] += gram_of(2 + lane, mask16_direct[lane])
    pair_copies[1].wait_recv()
    res_own[...] = own_part + res_pair_recv[1] - user_ridge * user0[:, block_rows(col)]

    late_copies[0].wait_recv()
    for slot in range(COLS):
        seen_rate = jnp.where(mask32[slot] > 0, rate[slot], 0.0)
        zrate[slot] = three_terms(seen_rate[:early])
        late_rated[row * COLS + order[slot]] = seen_rate[early:].astype(BF16)

    def item_sums(factors, seen, rated):
        pairs = stacked(pair_products(factors.astype(F32)))
        return dot_nn(pairs, seen), dot_nn(factors, rated)

    def item_part(entries, acc):
        factors = side_by_side(fac[source, t] for source, _, chunk in entries for t in chunk_tiles(chunk))
        seen = stacked(mask16[slot, chunk_rows(chunk), :] for _, slot, chunk in entries)
        rated = stacked(zrate[slot, chunk_rows(chunk), :] for _, slot, chunk in entries)
        sums = item_sums(factors, seen, rated)
        return sums if acc is None else (acc[0] + sums[0], acc[1] + sums[1])

    def late_part(of_row, chunk, acc):
        tiles = [t - early // LANES for t in chunk_tiles(chunk)]
        rows = pl.ds(STARTS[chunk] - early, WIDTHS[chunk])
        factors = side_by_side(late_fac[of_row * COLS + block, t] for block in range(COLS) for t in tiles)
        seen = stacked(late_seen[of_row * COLS + block, rows, :] for block in range(COLS))
        rated = stacked(late_rated[of_row * COLS + block, rows, :] for block in range(COLS))
        sums = item_sums(factors, seen, rated)
        return sums if acc is None else (acc[0] + sums[0], acc[1] + sums[1])

    def split_late(slot):
        value = late_recv[order[slot]].astype(F32)
        seen = value < jnp.inf
        late_seen[(1 - row) * COLS + order[slot]] = seen.astype(F32).astype(BF16)
        late_rated[(1 - row) * COLS + order[slot]] = jnp.where(seen, value, 0.0).astype(BF16)

    def arrived(chunks, lanes):
        for chunk in chunks:
            for lane in lanes:
                fac_copies[chunk][lane].wait_recv()
        return [(peers[lane][1], peers[lane][2], chunk) for chunk in chunks for lane in lanes]

    user_copies = []
    forwards = []
    groups = (range(0, early // LANES), range(early // LANES, span // LANES))

    def send_users(group):
        mine = user1.at[col, pl.ds(groups[group][0], len(groups[group]))]
        for lane, (device, _, _) in enumerate(peers[:2 + group]):
            user_copies.append(copy_to(mine, mine, user_sem, group * 3 + lane, device))
            user_copies[-1].start()

    def forward_users():
        user_copies[1].wait_recv()
        theirs = user1.at[far_col, pl.ds(groups[0][0], len(groups[0]))]
        forwards.append(copy_to(theirs, theirs, user_sem, 2, pair))
        forwards[-1].start()

    def solve(chunk):
        lanes = chunk_rows(chunk)
        gram_copies[chunk].wait_recv()
        far_diags = unpack(chunk)
        diags = [gram_own[d * RANK:(d + 1) * RANK, lanes] + far_diags[d] for d in range(DIAGS)]
        start = user0[:, block_rows(col, STARTS[chunk], WIDTHS[chunk])]
        residual = res_own[:, lanes] + side_by_side(res_far_recv[t].astype(F32) for t in chunk_tiles(chunk))
        solved = cg_solve(diags, residual, start, user_ridge)
        return [solved[:, i * LANES:(i + 1) * LANES] for i in range(WIDTHS[chunk] // LANES)]

    far_copies[0].wait_recv()
    fac_copies = []
    for chunk in range(LATE):
        pieces = solve(chunk)
        tiles = chunk_tiles(chunk)
        for t, piece in zip(tiles, pieces):
            fac[col, t] = piece.astype(BF16)
            user1[col, t] = piece
        mine = fac.at[col, pl.ds(tiles[0], len(tiles))]
        sent = [copy_to(mine, mine, fac_sem, chunk * 3 + lane, device) for lane, (device, _, _) in enumerate(peers)]
        for copy in sent[::-1]:
            copy.start()
        fac_copies.append(sent)
    send_users(0)
    sums = item_part([(col, 3, chunk) for chunk in range(LATE)], None)
    sums = item_part(arrived(range(LATE), (0,)), sums)
    late_fac_copies = []
    for chunk in range(LATE, CHUNKS):
        if chunk == LATE:
            far_copies[1].wait_recv()
        pieces = solve(chunk)
        tiles = chunk_tiles(chunk)
        for t, piece in zip(tiles, pieces):
            late_fac[row * COLS + col, t - early // LANES] = piece.astype(BF16)
            user1[col, t] = piece
        mine = late_fac.at[row * COLS + col, pl.ds(tiles[0] - early // LANES, len(tiles))]
        sent = []
        for lane, device in enumerate(others):
            sent.append(copy_to(mine, mine, late_fac_sem, (chunk - LATE) * len(others) + lane, device))
        for copy in sent[::-1]:
            copy.start()
        late_fac_copies.append(sent)
    send_users(1)
    entries = arrived(range(LATE - 1), (1, 2))
    sums = item_part(entries, sums)
    entries = arrived((LATE - 1,), (1, 2))
    sums = item_part(entries, sums)
    gram = sums[0][:terms] + sums[0][terms:]
    start = item16[...].astype(F32)
    residual = sums[1][:, :items] + sums[1][:, items:2 * items] + sums[1][:, 2 * items:]
    residual = residual - apply_gram(diagonals(gram), start)
    high = residual.astype(BF16)
    item_send[:terms] = gram.astype(BF16)
    item_send[terms:terms + RANK] = high
    item_send[terms + RANK:] = (residual - high.astype(F32)).astype(BF16)
    cross_copy = copy_to(item_send, item_recv, cross_sem, 0, cross)
    cross_copy.start()
    for slot in range(COLS):
        if slot:
            late_copies[slot].wait_recv()
        split_late(slot)
    forward_users()

    def late_arrived(chunk, lanes):
        for lane in lanes:
            late_fac_copies[chunk - LATE][lane].wait_recv()

    same = range(3)
    other = range(3, len(others))
    late_sums = [None, None]
    late_arrived(LATE, same)
    late_sums[0] = late_part(row, LATE, late_sums[0])
    late_arrived(LATE, other)
    late_sums[1] = late_part(1 - row, LATE, late_sums[1])
    late_arrived(LATE + 1, same)
    late_sums[0] = late_part(row, LATE + 1, late_sums[0])
    late_arrived(LATE + 1, other)
    late_sums[1] = late_part(1 - row, LATE + 1, late_sums[1])
    late_total = [late_sums[0][i] + late_sums[1][i] for i in range(2)]
    late_gram = late_total[0][:terms] + late_total[0][terms:]
    late_residual = late_total[1] - apply_gram(diagonals(late_gram), start)

    for copy in user_copies[:1] + user_copies[2:] + forwards:
        copy.wait_recv()
    for source in range(COLS):
        for t in range(span // LANES):
            user_out[:, pl.ds(source * span + t * LANES, LANES)] = user1[source, t]

    cross_copy.wait_recv()
    full = item_send[...].astype(F32) + item_recv[...].astype(F32)
    residual = full[terms:terms + RANK] + full[terms + RANK:] + late_residual - item_ridge * item0[...]
    item_out[...] = cg_solve(diagonals(full[:terms] + late_gram), residual, item0[...], item_ridge)

    remote = item_copies + direct_copies + [own_mask_copy, cross_copy] + far_copies + late_copies + mask_copies + pair_copies
    for copy in remote + gram_copies + user_copies + forwards + sum(fac_copies + late_fac_copies, []):
        copy.wait_send()


def write_kernel(user_ref, item_ref, user_out, item_out, sems):
    copies = [
        pltpu.make_async_copy(user_ref, user_out, sems.at[0]),
        pltpu.make_async_copy(item_ref, item_out, sems.at[1]),
    ]
    for copy in copies:
        copy.start()
    for copy in copies:
        copy.wait()


def solution(mesh):
    row_size = mesh.shape["row"]
    col_size = mesh.shape["col"]
    grid_spec = P(("part", "row"), "col")
    user_spec = P(("part", "row"), None)
    item_spec = P(("part", "col"), None)

    def local_step(ratings_blk, mask_blk, user_blk, item_blk):
        users, items = ratings_blk.shape
        span = users // COLS
        early = STARTS[LATE]
        late = span - early
        tiles = span // LANES
        hbm_spec = pl.BlockSpec(memory_space=pltpu.HBM)
        vmem = pltpu.VMEM
        dma = pltpu.SemaphoreType.DMA
        terms = DIAGS * RANK
        user_new, item_new = pl.pallas_call(
            functools.partial(sweep_kernel, RIDGE_WEIGHT * items * col_size, RIDGE_WEIGHT * users * row_size),
            out_shape=(
                pltpu.VMEM((RANK, users), F32),
                pltpu.VMEM((RANK, items), F32),
            ),
            in_specs=[hbm_spec] * 4,
            out_specs=(pl.BlockSpec(memory_space=pltpu.VMEM),) * 2,
            scratch_shapes=[
                vmem((COLS, span, items), F32),
                vmem((COLS, span, items), jnp.int32),
                vmem((RANK, users), F32),
                vmem((RANK, items), F32),
                vmem((COLS, span, items), BF16),
                vmem((2, span, items), BF16),
                vmem((2, DIRECT, items), BF16),
                vmem((RANK, items), BF16),
                vmem((3, RANK, items), BF16),
                vmem((COLS, terms, 2 * items), BF16),
                vmem((COLS, early, 3 * items), BF16),
                vmem((sum(PACKED), RANK, LANES), BF16),
                vmem((sum(PACKED), RANK, LANES), BF16),
                vmem((terms, span), F32),
                vmem((2, RANK, span), F32),
                vmem((2, RANK, span), F32),
                vmem((tiles, RANK, LANES), BF16),
                vmem((tiles, RANK, LANES), BF16),
                vmem((RANK, span), F32),
                vmem((COLS, early // LANES, RANK, LANES), BF16),
                vmem((COLS, tiles, RANK, LANES), F32),
                vmem((terms + 2 * RANK, items), BF16),
                vmem((terms + 2 * RANK, items), BF16),
                vmem((COLS, late, items), BF16),
                vmem((COLS, late, items), BF16),
                vmem((2 * COLS, late, items), BF16),
                vmem((2 * COLS, late, items), BF16),
                vmem((2 * COLS, late // LANES, RANK, LANES), BF16),
                dma((10 + COLS * CHUNKS,)),
                dma((2, 2)),
                dma((2, 3)),
                dma((2, CHUNKS + 1)),
                dma((2, 2)),
                dma((2, 2)),
                dma((2, CHUNKS)),
                dma((2, LATE * 3)),
                dma((2, 6)),
                dma((2, 1)),
                dma((2, COLS)),
                dma((2, (CHUNKS - LATE) * (2 * COLS - 1))),
            ],
            compiler_params=pltpu.CompilerParams(collective_id=0, has_side_effects=True, vmem_limit_bytes=60000 * 1024),
        )(ratings_blk, mask_blk, user_blk.T, item_blk.T)
        user_new, item_new = pl.pallas_call(
            write_kernel,
            out_shape=(
                jax.ShapeDtypeStruct((RANK, users), F32),
                jax.ShapeDtypeStruct((RANK, items), F32),
            ),
            in_specs=[pl.BlockSpec(memory_space=pltpu.VMEM)] * 2,
            out_specs=(hbm_spec, hbm_spec),
            scratch_shapes=[dma((2,))],
            compiler_params=pltpu.CompilerParams(vmem_limit_bytes=2**20),
        )(user_new, item_new)
        return user_new.T, item_new.T

    return jax.shard_map(local_step, mesh=mesh, in_specs=(grid_spec, grid_spec, user_spec, item_spec), out_specs=(user_spec, item_spec), check_vma=False)
```

```python
import functools

import jax
import jax.numpy as jnp
from jax import lax
from jax.experimental import pallas as pl
from jax.experimental.pallas import tpu as pltpu
from jax.sharding import PartitionSpec as P

CG_STEPS = 4
RIDGE_WEIGHT = 0.0005
RANK = 16
DIAGS = RANK // 2 + 1
MESH = pl.DeviceIdType.MESH
F32 = jnp.float32
BF16 = jnp.bfloat16
COLS = 4
LANES = 128
HALF = RANK // 2
WIDTHS = (256, 256, 128, 256, 128)
STARTS = tuple(sum(WIDTHS[:i]) for i in range(len(WIDTHS)))
CHUNKS = len(WIDTHS)
LATE = 3
SENDS = 4
DIRECT = 128


def dot_nt(a, b):
    return lax.dot_general(a, b, (((1,), (1,)), ((), ())), preferred_element_type=F32)


def dot_nn(a, b):
    return lax.dot_general(a, b, (((1,), (0,)), ((), ())), preferred_element_type=F32)


def turn(x, shift):
    return x if shift % RANK == 0 else pltpu.roll(x, shift % RANK, 0)


def pair_products(fac):
    prods = jnp.concatenate([fac * turn(fac, -d) for d in range(DIAGS)], axis=0)
    high = prods.astype(BF16)
    low = (prods - high.astype(F32)).astype(BF16)
    return high, low


def apply_gram(diags, vec):
    parts = [diags[d] * turn(vec, -d) for d in range(DIAGS)]
    parts += [turn(diags[d] * vec, d) for d in range(1, RANK // 2)]
    while len(parts) > 1:
        parts = [sum(parts[i:i + 2][1:], parts[i]) for i in range(0, len(parts), 2)]
    return parts[0]


def cg_solve(diags, residual, start, ridge):
    direction = residual
    estimate = start
    res_sq = jnp.sum(residual * residual, axis=0, keepdims=True)
    for cg_step in range(CG_STEPS):
        gram_dir = apply_gram(diags, direction) + ridge * direction
        step_size = res_sq / jnp.sum(direction * gram_dir, axis=0, keepdims=True)
        estimate = estimate + step_size * direction
        if cg_step + 1 < CG_STEPS:
            residual = residual - step_size * gram_dir
            new_sq = jnp.sum(residual * residual, axis=0, keepdims=True)
            direction = residual + (new_sq / res_sq) * direction
            res_sq = new_sq
    return estimate


def far_span(chunk):
    skip = DIRECT if chunk == 0 else 0
    return STARTS[chunk] + skip, WIDTHS[chunk] - skip


def packed_tiles(chunk):
    tiles = far_span(chunk)[1] // LANES
    return HALF * tiles + (tiles + 1) // 2


PACKED = tuple(packed_tiles(chunk) for chunk in range(CHUNKS))


def chunk_tiles(chunk):
    return range(STARTS[chunk] // LANES, (STARTS[chunk] + WIDTHS[chunk]) // LANES)


def side_by_side(blocks):
    return jnp.concatenate(list(blocks), axis=1)


def stacked(blocks):
    return jnp.concatenate(list(blocks), axis=0)


def three_terms(values):
    high = values.astype(BF16)
    rest = values - high.astype(F32)
    middle = rest.astype(BF16)
    return side_by_side([high, middle, (rest - middle.astype(F32)).astype(BF16)])


def diagonals(full):
    return [full[d * RANK:(d + 1) * RANK] for d in range(DIAGS)]


def sweep_kernel(
    user_ridge, item_ridge,
    ratings_hbm, mask_hbm, user_hbm, item_hbm,
    user_out, item_out,
    rate, mask32, user0, item0,
    mask16, mask16_peer, mask16_direct, item16, item16_peer, ffs, zrate,
    gram_send, gram_recv, gram_own,
    res_pair, res_pair_recv, res_far, res_far_recv, res_own,
    fac, user1, item_send, item_recv,
    late_send, late_recv, late_seen, late_rated, late_fac,
    in_sem, send_sem, item_sem, direct_sem, mask_sem, pair_sem, far_sem, gram_sem, fac_sem, user_sem, cross_sem, late_sem, late_fac_sem,
):
    part = lax.axis_index("part")
    row = lax.axis_index("row")
    col = lax.axis_index("col")
    chip = col // 2
    core = col % 2
    pair_col = chip * 2 + (1 - core)
    far_col = (1 - chip) * 2 + core
    diag_col = (1 - chip) * 2 + (1 - core)
    pair = (part, row, pair_col)
    far = (part, row, far_col)
    diag = (part, row, diag_col)
    cross = (part, 1 - row, col)
    peers = ((pair, pair_col, 2), (far, far_col, 1), (diag, diag_col, 0))
    others = [device for device, _, _ in peers] + [cross] + [(part, 1 - row, source) for _, source, _ in peers]

    span = mask16.shape[1]
    items = item0.shape[1]
    terms = DIAGS * RANK
    early = STARTS[LATE]
    late = span - early

    sent_rows = [0] * SENDS

    def copy_to(src, dst, recv_sem, device, group):
        size = 1
        for extent in src.shape:
            size *= extent
        sent_rows[group] += size * src.dtype.itemsize // (items * rate.dtype.itemsize)
        return pltpu.make_async_remote_copy(
            src_ref=src, dst_ref=dst, send_sem=send_sem.at[group], recv_sem=recv_sem,
            device_id=device, device_id_type=MESH,
        )

    def wait_for(ref, sem):
        pltpu.make_async_copy(ref, ref, sem).wait()

    barrier = pltpu.get_barrier_semaphore()
    for device in (pair, far, diag, cross):
        pl.semaphore_signal(barrier, inc=1, device_id=device, device_id_type=MESH)

    order = (diag_col, far_col, pair_col, col)

    def load(src, dst, slot):
        return pltpu.make_async_copy(src, dst, in_sem.at[slot])

    def block_rows(block, start=0, size=span):
        return pl.ds(pl.multiple_of(block * span + start, LANES), size)

    def chunk_rows(chunk):
        return pl.ds(STARTS[chunk], WIDTHS[chunk])

    item_load = load(item_hbm, item0, 0)
    user_load = load(user_hbm, user0, 1)
    rate_loads = []
    rate_late_loads = []
    mask_loads = []
    splits = (WIDTHS[0], WIDTHS[0], early, early)
    for slot, block in enumerate(order):
        rate_loads.append(load(ratings_hbm.at[block_rows(block, 0, early)], rate.at[slot, pl.ds(0, early)], 2 + slot))
        rate_late_loads.append(load(ratings_hbm.at[block_rows(block, early, late)], rate.at[slot, pl.ds(early, late)], 6 + slot))
        pieces = []
        for half, (start, size) in enumerate(((0, splits[slot]), (splits[slot], span - splits[slot]))):
            src = mask_hbm.at[block_rows(block, start, size)]
            pieces.append(load(src, mask32.at[slot, pl.ds(start, size)], 10 + slot * 2 + half))
        mask_loads.append(pieces)

    def convert(slot, start, size):
        rows = pl.ds(start, size)
        seen = mask32[slot, rows].astype(F32).astype(BF16)
        mask16[slot, rows] = seen
        if start + size == span:
            late_seen[row * COLS + order[slot]] = seen[early - start:]

    item_load.start()
    for pieces in mask_loads[:2]:
        for copy in pieces:
            copy.start()
    for slot in range(COLS):
        if slot >= 2:
            mask_loads[slot][1].start()
        rate_late_loads[slot].start()

    item_load.wait()
    item16[...] = item0[...].astype(BF16)
    pl.semaphore_wait(barrier, 4)
    item_copies = []
    for lane, (device, _, _) in enumerate(peers):
        item_copies.append(copy_to(item16, item16_peer.at[lane], item_sem.at[min(lane, 1)], device, 1))
        item_copies[-1].start()
    first = pl.ds(0, DIRECT)

    def send_late(slot):
        rate_late_loads[slot].wait()
        rows = pl.ds(early, late)
        late_send[order[slot]] = jnp.where(mask32[slot, rows] > 0, rate[slot, rows], jnp.inf).astype(BF16)
        copy_to(late_send.at[order[slot]], late_recv.at[order[slot]], late_sem.at[min(slot, 1)], cross, 1).start()

    def mask_copy(half):
        rows = pl.ds(*((splits[0], span - splits[0]) if half else (DIRECT, splits[0] - DIRECT)))
        return copy_to(mask16.at[0, rows], mask16_peer.at[0, rows], mask_sem.at[half], pair, 0)

    mask_copies = [mask_copy(half) for half in range(2)]
    mask_loads[0][0].wait()
    convert(0, 0, splits[0])
    mask_copies[0].start()
    copy_to(mask16.at[0, first], mask16_direct.at[1], direct_sem.at[0], diag, 1).start()
    mask_loads[1][0].wait()
    convert(1, 0, splits[1])
    copy_to(mask16.at[1, first], mask16_direct.at[0], direct_sem.at[0], far, 1).start()
    mask_loads[0][1].wait()
    convert(0, splits[0], span - splits[0])
    mask_copies[1].start()
    user_load.start()
    for pieces in mask_loads[2:]:
        pieces[0].start()
    for copy in rate_loads:
        copy.start()
    send_late(0)
    mask_loads[1][1].wait()
    convert(1, splits[1], span - splits[1])
    send_late(1)
    for slot in (2, 3):
        mask_loads[slot][1].wait()
        convert(slot, early, late)
        send_late(slot)

    def put_products(index, factors):
        high, low = pair_products(factors.astype(F32))
        ffs[index, :, :items] = high
        ffs[index, :, items:] = low

    put_products(0, item16[...])
    item_copies[0].wait_recv()
    put_products(1, item16_peer[0])

    def gram_of(index, seen):
        return dot_nt(ffs[index], side_by_side([seen, seen]))

    def gram_part(slot, rows):
        return gram_of(0, mask16[slot, rows, :]) + gram_of(1, mask16_peer[slot // 2, rows, :])

    def pack(gram, chunk):
        tiles = gram.shape[1] // LANES
        base = sum(PACKED[:chunk])
        for d in range(HALF):
            for t in range(tiles):
                piece = gram[d * RANK:(d + 1) * RANK, t * LANES:(t + 1) * LANES]
                gram_send[base + d * tiles + t] = piece.astype(BF16)
        half = gram[HALF * RANK:HALF * RANK + HALF]
        for t in range(0, tiles, 2):
            both = [half[:, min(u, tiles - 1) * LANES:][:, :LANES] for u in (t, t + 1)]
            gram_send[base + HALF * tiles + t // 2] = stacked(both).astype(BF16)

    def unpack(chunk):
        gap = far_span(chunk)[1]
        tiles = gap // LANES
        base = sum(PACKED[:chunk])
        diags = [side_by_side(gram_recv[base + d * tiles + t].astype(F32) for t in range(tiles)) for d in range(HALF)]
        pieces = []
        for t in range(0, tiles, 2):
            both = gram_recv[base + HALF * tiles + t // 2].astype(F32)
            for half in (both[:HALF], both[HALF:])[:tiles - t]:
                pieces.append(stacked([half, half]))
        diags.append(side_by_side(pieces))
        pad = WIDTHS[chunk] - gap
        return [side_by_side([jnp.zeros((RANK, pad), F32), d]) if pad else d for d in diags]

    gram_copies = []
    for chunk in range(CHUNKS):
        part_of = pl.ds(sum(PACKED[:chunk]), PACKED[chunk])
        gram_copies.append(copy_to(gram_send.at[part_of], gram_recv.at[part_of], gram_sem.at[chunk], far, 2))

    def far_gram(chunk):
        if chunk < 2:
            mask_copies[chunk].wait_recv()
        pack(gram_part(1, pl.ds(*far_span(chunk))), chunk)

    for chunk in range(2):
        far_gram(chunk)
        gram_copies[chunk].start()

    user_load.wait()

    def user_residual(slot, block):
        start = user0[:, block_rows(block)]
        scores = dot_nn(start.T.astype(BF16), item16[...])
        resid = jnp.where(mask32[slot] > 0, rate[slot] - scores, 0.0).astype(BF16)
        return dot_nt(item16[...], resid)

    rate_loads[0].wait()
    res_pair[0] = user_residual(0, diag_col)
    pair_copies = [copy_to(res_pair.at[slot], res_pair_recv.at[slot], pair_sem.at[slot], pair, 2) for slot in range(2)]
    pair_copies[0].start()
    rate_loads[1].wait()
    far_part = user_residual(1, far_col)
    far_gram(2)
    pair_copies[0].wait_recv()
    total = (far_part + res_pair_recv[0]).astype(BF16)
    for t in range(span // LANES):
        res_far[t] = total[:, t * LANES:(t + 1) * LANES]
    far_copies = []
    for half, tiles in enumerate((pl.ds(0, early // LANES), pl.ds(early // LANES, late // LANES))):
        far_copies.append(copy_to(res_far.at[tiles], res_far_recv.at[tiles], far_sem.at[half], far, 2))
    for copy in (far_copies[0], gram_copies[2], far_copies[1]):
        copy.start()
    for chunk in range(LATE, CHUNKS):
        far_gram(chunk)
        gram_copies[chunk].start()
    mask_loads[2][0].wait()
    convert(2, 0, early)
    own_mask_copy = copy_to(mask16.at[2], mask16_peer.at[1], mask_sem.at[2], pair, 0)
    own_mask_copy.start()
    mask_loads[3][0].wait()
    convert(3, 0, early)
    rate_loads[2].wait()
    res_pair[1] = user_residual(2, pair_col)
    pair_copies[1].start()
    rate_loads[3].wait()
    own_part = user_residual(3, col)
    own_mask_copy.wait_recv()
    for chunk in range(CHUNKS):
        gram_own[:, chunk_rows(chunk)] = gram_part(3, chunk_rows(chunk))
    wait_for(item16_peer.at[pl.ds(1, 2)], item_sem.at[1])
    wait_for(mask16_direct, direct_sem.at[0])
    for lane in range(2):
        put_products(2 + lane, item16_peer[1 + lane])
        gram_own[:, :DIRECT] += gram_of(2 + lane, mask16_direct[lane])
    pair_copies[1].wait_recv()
    res_own[...] = own_part + res_pair_recv[1] - user_ridge * user0[:, block_rows(col)]

    wait_for(late_recv.at[0], late_sem.at[0])
    for slot in range(COLS):
        seen_rate = jnp.where(mask32[slot] > 0, rate[slot], 0.0)
        zrate[slot] = three_terms(seen_rate[:early])
        late_rated[row * COLS + order[slot]] = seen_rate[early:].astype(BF16)

    def item_sums(factors, seen, rated):
        pairs = stacked(pair_products(factors.astype(F32)))
        return dot_nn(pairs, seen), dot_nn(factors, rated)

    def item_part(entries, acc):
        factors = side_by_side(fac[source, t] for source, _, chunk in entries for t in chunk_tiles(chunk))
        seen = stacked(mask16[slot, chunk_rows(chunk), :] for _, slot, chunk in entries)
        rated = stacked(zrate[slot, chunk_rows(chunk), :] for _, slot, chunk in entries)
        sums = item_sums(factors, seen, rated)
        return sums if acc is None else (acc[0] + sums[0], acc[1] + sums[1])

    def late_part(of_row, chunk, acc):
        tiles = [t - early // LANES for t in chunk_tiles(chunk)]
        rows = pl.ds(STARTS[chunk] - early, WIDTHS[chunk])
        factors = side_by_side(late_fac[of_row * COLS + block, t] for block in range(COLS) for t in tiles)
        seen = stacked(late_seen[of_row * COLS + block, rows, :] for block in range(COLS))
        rated = stacked(late_rated[of_row * COLS + block, rows, :] for block in range(COLS))
        sums = item_sums(factors, seen, rated)
        return sums if acc is None else (acc[0] + sums[0], acc[1] + sums[1])

    def split_late(slot):
        value = late_recv[order[slot]].astype(F32)
        seen = value < jnp.inf
        late_seen[(1 - row) * COLS + order[slot]] = seen.astype(F32).astype(BF16)
        late_rated[(1 - row) * COLS + order[slot]] = jnp.where(seen, value, 0.0).astype(BF16)

    groups = (range(0, early // LANES), range(early // LANES, span // LANES))

    def send_users(group):
        mine = user1.at[col, pl.ds(groups[group][0], len(groups[group]))]
        for lane, (device, _, _) in enumerate(peers[:2 + group]):
            sem = user_sem.at[1 if (group, lane) == (0, 1) else 0]
            copy_to(mine, mine, sem, device, 3).start()

    def forward_users():
        theirs = user1.at[far_col, pl.ds(groups[0][0], len(groups[0]))]
        wait_for(theirs, user_sem.at[1])
        copy_to(theirs, theirs, user_sem.at[0], pair, 3).start()

    def solve(chunk):
        lanes = chunk_rows(chunk)
        gram_copies[chunk].wait_recv()
        far_diags = unpack(chunk)
        diags = [gram_own[d * RANK:(d + 1) * RANK, lanes] + far_diags[d] for d in range(DIAGS)]
        start = user0[:, block_rows(col, STARTS[chunk], WIDTHS[chunk])]
        residual = res_own[:, lanes] + side_by_side(res_far_recv[t].astype(F32) for t in chunk_tiles(chunk))
        solved = cg_solve(diags, residual, start, user_ridge)
        return [solved[:, i * LANES:(i + 1) * LANES] for i in range(WIDTHS[chunk] // LANES)]

    fac_groups = pl.ds(0, STARTS[2] // LANES), pl.ds(STARTS[2] // LANES, WIDTHS[2] // LANES)

    def entries_of(lanes, chunks):
        return [(peers[lane][1], peers[lane][2], chunk) for chunk in chunks for lane in lanes]

    far_copies[0].wait_recv()
    for chunk in range(LATE):
        pieces = solve(chunk)
        tiles = chunk_tiles(chunk)
        for t, piece in zip(tiles, pieces):
            fac[col, t] = piece.astype(BF16)
            user1[col, t] = piece
        if chunk:
            mine = fac.at[col, fac_groups[chunk - 1]]
            for lane, (device, _, _) in list(enumerate(peers))[::-1]:
                copy_to(mine, mine, fac_sem.at[chunk if lane else 0], device, 3).start()
    send_users(0)
    sums = item_part([(col, 3, chunk) for chunk in range(LATE)], None)
    wait_for(fac.at[0], fac_sem.at[0])
    sums = item_part(entries_of((0,), range(LATE)), sums)
    for chunk in range(LATE, CHUNKS):
        if chunk == LATE:
            far_copies[1].wait_recv()
        pieces = solve(chunk)
        tiles = chunk_tiles(chunk)
        for t, piece in zip(tiles, pieces):
            late_fac[row * COLS + col, t - early // LANES] = piece.astype(BF16)
            user1[col, t] = piece
        mine = late_fac.at[row * COLS + col, pl.ds(tiles[0] - early // LANES, len(tiles))]
        for lane, device in list(enumerate(others))[::-1]:
            copy_to(mine, mine, late_fac_sem.at[(chunk - LATE) * 2 + lane // 3 - lane // 6], device, 3).start()
    send_users(1)
    wait_for(fac.at[pl.ds(0, 2), fac_groups[0]], fac_sem.at[1])
    entries = entries_of((1, 2), range(LATE - 1))
    sums = item_part(entries, sums)
    wait_for(fac.at[pl.ds(0, 2), fac_groups[1]], fac_sem.at[2])
    entries = entries_of((1, 2), (LATE - 1,))
    sums = item_part(entries, sums)
    gram = sums[0][:terms] + sums[0][terms:]
    start = item16[...].astype(F32)
    residual = sums[1][:, :items] + sums[1][:, items:2 * items] + sums[1][:, 2 * items:]
    residual = residual - apply_gram(diagonals(gram), start)
    high = residual.astype(BF16)
    item_send[:terms] = gram.astype(BF16)
    item_send[terms:terms + RANK] = high
    item_send[terms + RANK:] = (residual - high.astype(F32)).astype(BF16)
    cross_copy = copy_to(item_send, item_recv, cross_sem.at[0], cross, 2)
    cross_copy.start()
    wait_for(late_recv.at[pl.ds(1, COLS - 1)], late_sem.at[1])
    for slot in range(COLS):
        split_late(slot)
    forward_users()

    def late_arrived(chunk, which):
        tiles = chunk_tiles(chunk)
        view = late_fac.at[pl.ds(0, COLS - 1 + which), pl.ds(tiles[0] - early // LANES, len(tiles))]
        wait_for(view, late_fac_sem.at[(chunk - LATE) * 2 + which])

    late_sums = [None, None]
    late_arrived(LATE, 0)
    late_sums[0] = late_part(row, LATE, late_sums[0])
    late_arrived(LATE, 1)
    late_sums[1] = late_part(1 - row, LATE, late_sums[1])
    late_arrived(LATE + 1, 0)
    late_sums[0] = late_part(row, LATE + 1, late_sums[0])
    late_arrived(LATE + 1, 1)
    late_sums[1] = late_part(1 - row, LATE + 1, late_sums[1])
    late_total = [late_sums[0][i] + late_sums[1][i] for i in range(2)]
    late_gram = late_total[0][:terms] + late_total[0][terms:]
    late_residual = late_total[1] - apply_gram(diagonals(late_gram), start)

    wait_for(rate.at[0, pl.ds(0, RANK * (2 * early + 3 * late) // items)], user_sem.at[0])
    for source in range(COLS):
        for t in range(span // LANES):
            user_out[:, pl.ds(source * span + t * LANES, LANES)] = user1[source, t]

    cross_copy.wait_recv()
    full = item_send[...].astype(F32) + item_recv[...].astype(F32)
    residual = full[terms:terms + RANK] + full[terms + RANK:] + late_residual - item_ridge * item0[...]
    item_out[...] = cg_solve(diagonals(full[:terms] + late_gram), residual, item0[...], item_ridge)

    for group in range(SENDS):
        wait_for(rate.at[0, pl.ds(0, sent_rows[group])], send_sem.at[group])


def write_kernel(user_ref, item_ref, user_out, item_out, sems):
    copies = [
        pltpu.make_async_copy(user_ref, user_out, sems.at[0]),
        pltpu.make_async_copy(item_ref, item_out, sems.at[1]),
    ]
    for copy in copies:
        copy.start()
    for copy in copies:
        copy.wait()


def solution(mesh):
    row_size = mesh.shape["row"]
    col_size = mesh.shape["col"]
    grid_spec = P(("part", "row"), "col")
    user_spec = P(("part", "row"), None)
    item_spec = P(("part", "col"), None)

    def local_step(ratings_blk, mask_blk, user_blk, item_blk):
        users, items = ratings_blk.shape
        span = users // COLS
        early = STARTS[LATE]
        late = span - early
        tiles = span // LANES
        hbm_spec = pl.BlockSpec(memory_space=pltpu.HBM)
        vmem = pltpu.VMEM
        dma = pltpu.SemaphoreType.DMA
        terms = DIAGS * RANK
        user_new, item_new = pl.pallas_call(
            functools.partial(sweep_kernel, RIDGE_WEIGHT * items * col_size, RIDGE_WEIGHT * users * row_size),
            out_shape=(
                pltpu.VMEM((RANK, users), F32),
                pltpu.VMEM((RANK, items), F32),
            ),
            in_specs=[hbm_spec] * 4,
            out_specs=(pl.BlockSpec(memory_space=pltpu.VMEM),) * 2,
            scratch_shapes=[
                vmem((COLS, span, items), F32),
                vmem((COLS, span, items), jnp.int32),
                vmem((RANK, users), F32),
                vmem((RANK, items), F32),
                vmem((COLS, span, items), BF16),
                vmem((2, span, items), BF16),
                vmem((2, DIRECT, items), BF16),
                vmem((RANK, items), BF16),
                vmem((3, RANK, items), BF16),
                vmem((COLS, terms, 2 * items), BF16),
                vmem((COLS, early, 3 * items), BF16),
                vmem((sum(PACKED), RANK, LANES), BF16),
                vmem((sum(PACKED), RANK, LANES), BF16),
                vmem((terms, span), F32),
                vmem((2, RANK, span), F32),
                vmem((2, RANK, span), F32),
                vmem((tiles, RANK, LANES), BF16),
                vmem((tiles, RANK, LANES), BF16),
                vmem((RANK, span), F32),
                vmem((COLS, early // LANES, RANK, LANES), BF16),
                vmem((COLS, tiles, RANK, LANES), F32),
                vmem((terms + 2 * RANK, items), BF16),
                vmem((terms + 2 * RANK, items), BF16),
                vmem((COLS, late, items), BF16),
                vmem((COLS, late, items), BF16),
                vmem((2 * COLS, late, items), BF16),
                vmem((2 * COLS, late, items), BF16),
                vmem((2 * COLS, late // LANES, RANK, LANES), BF16),
                dma((18,)),
                dma((SENDS,)),
                dma((2,)),
                dma((1,)),
                dma((3,)),
                dma((2,)),
                dma((2,)),
                dma((CHUNKS,)),
                dma((3,)),
                dma((2,)),
                dma((1,)),
                dma((2,)),
                dma((2 * (CHUNKS - LATE),)),
            ],
            compiler_params=pltpu.CompilerParams(collective_id=0, has_side_effects=True, vmem_limit_bytes=60000 * 1024),
        )(ratings_blk, mask_blk, user_blk.T, item_blk.T)
        user_new, item_new = pl.pallas_call(
            write_kernel,
            out_shape=(
                jax.ShapeDtypeStruct((RANK, users), F32),
                jax.ShapeDtypeStruct((RANK, items), F32),
            ),
            in_specs=[pl.BlockSpec(memory_space=pltpu.VMEM)] * 2,
            out_specs=(hbm_spec, hbm_spec),
            scratch_shapes=[dma((2,))],
            compiler_params=pltpu.CompilerParams(vmem_limit_bytes=2**20),
        )(user_new, item_new)
        return user_new.T, item_new.T

    return jax.shard_map(local_step, mesh=mesh, in_specs=(grid_spec, grid_spec, user_spec, item_spec), out_specs=(user_spec, item_spec), check_vma=False)
```

```python
import functools
import math

import jax
import jax.numpy as jnp
from jax import lax
from jax.experimental import pallas as pl
from jax.experimental.pallas import tpu as pltpu
from jax.sharding import PartitionSpec as P

CG_STEPS = 4
RIDGE_WEIGHT = 0.0005
RANK = 16
DIAGS = RANK // 2 + 1
MESH = pl.DeviceIdType.MESH
F32 = jnp.float32
BF16 = jnp.bfloat16
COLS = 4
LANES = 128
HALF = RANK // 2
WIDTHS = (256, 256, 128, 256, 128)
STARTS = tuple(sum(WIDTHS[:i]) for i in range(len(WIDTHS)))
CHUNKS = len(WIDTHS)
LATE = 3
DIRECT = 128


def dot_nt(a, b):
    return lax.dot_general(a, b, (((1,), (1,)), ((), ())), preferred_element_type=F32)


def dot_nn(a, b):
    return lax.dot_general(a, b, (((1,), (0,)), ((), ())), preferred_element_type=F32)


def turn(x, shift):
    return x if shift % RANK == 0 else pltpu.roll(x, shift % RANK, 0)


def pair_products(fac):
    prods = jnp.concatenate([fac * turn(fac, -d) for d in range(DIAGS)], axis=0)
    high = prods.astype(BF16)
    low = (prods - high.astype(F32)).astype(BF16)
    return high, low


def apply_gram(diags, vec):
    parts = [diags[d] * turn(vec, -d) for d in range(DIAGS)]
    parts += [turn(diags[d] * vec, d) for d in range(1, RANK // 2)]
    while len(parts) > 1:
        parts = [sum(parts[i:i + 2][1:], parts[i]) for i in range(0, len(parts), 2)]
    return parts[0]


def cg_solve(diags, residual, start, ridge):
    direction = residual
    estimate = start
    res_sq = jnp.sum(residual * residual, axis=0, keepdims=True)
    for cg_step in range(CG_STEPS):
        gram_dir = apply_gram(diags, direction) + ridge * direction
        step_size = res_sq / jnp.sum(direction * gram_dir, axis=0, keepdims=True)
        estimate = estimate + step_size * direction
        if cg_step + 1 < CG_STEPS:
            residual = residual - step_size * gram_dir
            new_sq = jnp.sum(residual * residual, axis=0, keepdims=True)
            direction = residual + (new_sq / res_sq) * direction
            res_sq = new_sq
    return estimate


def far_span(chunk):
    skip = DIRECT if chunk == 0 else 0
    return STARTS[chunk] + skip, WIDTHS[chunk] - skip


def packed_tiles(chunk):
    tiles = far_span(chunk)[1] // LANES
    return HALF * tiles + (tiles + 1) // 2


PACKED = tuple(packed_tiles(chunk) for chunk in range(CHUNKS))


def chunk_tiles(chunk):
    return range(STARTS[chunk] // LANES, (STARTS[chunk] + WIDTHS[chunk]) // LANES)


def side_by_side(blocks):
    return jnp.concatenate(list(blocks), axis=1)


def stacked(blocks):
    return jnp.concatenate(list(blocks), axis=0)


def three_terms(values):
    high = values.astype(BF16)
    rest = values - high.astype(F32)
    middle = rest.astype(BF16)
    return side_by_side([high, middle, (rest - middle.astype(F32)).astype(BF16)])


def diagonals(full):
    return [full[d * RANK:(d + 1) * RANK] for d in range(DIAGS)]


def sweep_kernel(
    user_ridge, item_ridge,
    ratings_hbm, mask_hbm, user_hbm, item_hbm,
    user_out, item_out,
    rate, mask32, user0, item0,
    mask16, mask16_peer, mask16_direct, item16, item16_peer, ffs, zrate,
    gram_send, gram_recv, gram_own,
    res_pair, res_pair_recv, res_far, res_far_recv, res_own,
    fac, user1, item_send, item_recv,
    late_send, late_recv, late_seen, late_rated, late_fac, late_sums,
    in_sem, send_sem, item_sem, own_sem, mask_sem, pair_sem, gram_sem, fac_sem, user_sem, cross_sem, late_sem, late_fac_sem,
):
    part = lax.axis_index("part")
    row = lax.axis_index("row")
    col = lax.axis_index("col")
    chip = col // 2
    core = col % 2
    pair_col = chip * 2 + (1 - core)
    far_col = (1 - chip) * 2 + core
    diag_col = (1 - chip) * 2 + (1 - core)
    pair = (part, row, pair_col)
    far = (part, row, far_col)
    diag = (part, row, diag_col)
    cross = (part, 1 - row, col)
    peers = ((pair, pair_col, 2), (far, far_col, 1), (diag, diag_col, 0))
    others = [device for device, _, _ in peers] + [cross] + [(part, 1 - row, source) for _, source, _ in peers]

    span = mask16.shape[1]
    items = item0.shape[1]
    terms = DIAGS * RANK
    early = STARTS[LATE]
    late = span - early

    sent = []

    def copy_to(src, dst, recv_sem, device):
        sent.append(src)
        return pltpu.make_async_remote_copy(
            src_ref=src, dst_ref=dst, send_sem=send_sem.at[0], recv_sem=recv_sem,
            device_id=device, device_id_type=MESH,
        )

    def wait_for(ref, sem):
        pltpu.make_async_copy(ref, ref, sem).wait()

    def wait_all(refs, sem):
        count = sum(math.prod(ref.shape) * ref.dtype.itemsize for ref in refs) // (items * rate.dtype.itemsize)
        parts = next(parts for parts in (1, 2, COLS) if count <= parts * span and count % parts == 0)
        wait_for(rate.at[pl.ds(0, parts), pl.ds(0, count // parts)], sem)

    barrier = pltpu.get_barrier_semaphore()
    for device in (pair, far, diag, cross):
        pl.semaphore_signal(barrier, inc=1, device_id=device, device_id_type=MESH)

    order = (diag_col, far_col, pair_col, col)

    def load(src, dst, slot):
        return pltpu.make_async_copy(src, dst, in_sem.at[slot])

    def block_rows(block, start=0, size=span):
        return pl.ds(pl.multiple_of(block * span + start, LANES), size)

    def chunk_rows(chunk):
        return pl.ds(STARTS[chunk], WIDTHS[chunk])

    item_load = load(item_hbm, item0, 0)
    user_load = load(user_hbm, user0, 2)
    rate_loads = []
    rate_late_loads = []
    mask_loads = []
    splits = (WIDTHS[0], WIDTHS[0], early, early)
    for slot, block in enumerate(order):
        rate_loads.append(load(ratings_hbm.at[block_rows(block, 0, early)], rate.at[slot, pl.ds(0, early)], 2 + slot // 2))
        rate_late_loads.append(load(ratings_hbm.at[block_rows(block, early, late)], rate.at[slot, pl.ds(early, late)], 4 + min(slot, 1)))
        pieces = []
        for half, (start, size) in enumerate(((0, splits[slot]), (splits[slot], span - splits[slot]))):
            src = mask_hbm.at[block_rows(block, start, size)]
            pieces.append(load(src, mask32.at[slot, pl.ds(start, size)], (6, 7, 3)[min(slot, 2)] if half == 0 else (1, 5)[slot // 2]))
        mask_loads.append(pieces)

    def convert(slot, start, size):
        rows = pl.ds(start, size)
        seen = mask32[slot, rows].astype(F32).astype(BF16)
        mask16[slot, rows] = seen
        if start + size == span:
            late_seen[row * COLS + order[slot]] = seen[early - start:]

    item_load.start()
    for pieces in mask_loads[:2]:
        for copy in pieces:
            copy.start()
    for slot in range(COLS):
        if slot >= 2:
            mask_loads[slot][1].start()
        rate_late_loads[slot].start()

    item_load.wait()
    item16[...] = item0[...].astype(BF16)
    pl.semaphore_wait(barrier, 4)
    item_copies = []
    for lane, (device, _, _) in enumerate(peers):
        item_copies.append(copy_to(item16, item16_peer.at[lane], (own_sem if lane else item_sem).at[0], device))
        item_copies[-1].start()
    first = pl.ds(0, DIRECT)

    def send_late(slot):
        rows = pl.ds(early, late)
        late_send[order[slot]] = jnp.where(mask32[slot, rows] > 0, rate[slot, rows], jnp.inf).astype(BF16)
        copy_to(late_send.at[order[slot]], late_recv.at[order[slot]], late_sem.at[min(slot, 1)], cross).start()

    def mask_copy(half):
        rows = pl.ds(*((splits[0], span - splits[0]) if half else (DIRECT, splits[0] - DIRECT)))
        return copy_to(mask16.at[0, rows], mask16_peer.at[0, rows], mask_sem.at[half], pair)

    mask_copies = [mask_copy(half) for half in range(2)]
    mask_loads[0][0].wait()
    convert(0, 0, splits[0])
    mask_copies[0].start()
    copy_to(mask16.at[0, first], mask16_direct.at[1], own_sem.at[0], diag).start()
    mask_loads[1][0].wait()
    convert(1, 0, splits[1])
    copy_to(mask16.at[1, first], mask16_direct.at[0], own_sem.at[0], far).start()
    rest = pl.ds(splits[0], span - splits[0])
    wait_for(mask32.at[pl.ds(0, 2), rest], in_sem.at[1])
    convert(0, splits[0], span - splits[0])
    mask_copies[1].start()
    user_load.start()
    for pieces in mask_loads[2:]:
        pieces[0].start()
    for copy in rate_loads:
        copy.start()
    rate_late_loads[0].wait()
    send_late(0)
    convert(1, splits[1], span - splits[1])
    wait_all([rate.at[pl.ds(1, COLS - 1), pl.ds(early, late)], mask32.at[pl.ds(2, 2), pl.ds(early, late)]], in_sem.at[5])
    send_late(1)
    for slot in (2, 3):
        convert(slot, early, late)
        send_late(slot)

    def put_products(index, factors):
        high, low = pair_products(factors.astype(F32))
        ffs[index, :, :items] = high
        ffs[index, :, items:] = low

    put_products(0, item16[...])
    item_copies[0].wait_recv()
    put_products(1, item16_peer[0])

    def gram_of(index, seen):
        return dot_nt(ffs[index], side_by_side([seen, seen]))

    def gram_part(slot, rows):
        return gram_of(0, mask16[slot, rows, :]) + gram_of(1, mask16_peer[slot // 2, rows, :])

    def pack(gram, chunk):
        tiles = gram.shape[1] // LANES
        base = sum(PACKED[:chunk])
        for d in range(HALF):
            for t in range(tiles):
                piece = gram[d * RANK:(d + 1) * RANK, t * LANES:(t + 1) * LANES]
                gram_send[base + d * tiles + t] = piece.astype(BF16)
        half = gram[HALF * RANK:HALF * RANK + HALF]
        for t in range(0, tiles, 2):
            both = [half[:, min(u, tiles - 1) * LANES:][:, :LANES] for u in (t, t + 1)]
            gram_send[base + HALF * tiles + t // 2] = stacked(both).astype(BF16)

    def unpack(chunk):
        gap = far_span(chunk)[1]
        tiles = gap // LANES
        base = sum(PACKED[:chunk])
        diags = [side_by_side(gram_recv[base + d * tiles + t].astype(F32) for t in range(tiles)) for d in range(HALF)]
        pieces = []
        for t in range(0, tiles, 2):
            both = gram_recv[base + HALF * tiles + t // 2].astype(F32)
            for half in (both[:HALF], both[HALF:])[:tiles - t]:
                pieces.append(stacked([half, half]))
        diags.append(side_by_side(pieces))
        pad = WIDTHS[chunk] - gap
        return [side_by_side([jnp.zeros((RANK, pad), F32), d]) if pad else d for d in diags]

    gram_copies = []
    for chunk in range(CHUNKS):
        part_of = pl.ds(sum(PACKED[:chunk]), PACKED[chunk])
        gram_copies.append(copy_to(gram_send.at[part_of], gram_recv.at[part_of], gram_sem.at[max(chunk - 1, 0)], far))

    def far_gram(chunk):
        if chunk < 2:
            mask_copies[chunk].wait_recv()
        pack(gram_part(1, pl.ds(*far_span(chunk))), chunk)

    for chunk in range(2):
        far_gram(chunk)
        gram_copies[chunk].start()

    def user_residual(slot, block):
        start = user0[:, block_rows(block)]
        scores = dot_nn(start.T.astype(BF16), item16[...])
        resid = jnp.where(mask32[slot] > 0, rate[slot] - scores, 0.0).astype(BF16)
        return dot_nt(item16[...], resid)

    wait_all([user0, rate.at[pl.ds(0, 2), pl.ds(0, early)]], in_sem.at[2])
    res_pair[0] = user_residual(0, diag_col)
    pair_copies = [copy_to(res_pair.at[slot], res_pair_recv.at[slot], (own_sem if slot else pair_sem).at[0], pair) for slot in range(2)]
    pair_copies[0].start()
    far_part = user_residual(1, far_col)
    far_gram(2)
    pair_copies[0].wait_recv()
    total = (far_part + res_pair_recv[0]).astype(BF16)
    for t in range(span // LANES):
        res_far[t] = total[:, t * LANES:(t + 1) * LANES]
    far_copies = []
    res_groups = pl.ds(0, early // LANES), pl.ds(early // LANES, late // LANES)
    for half, tiles in enumerate(res_groups):
        far_copies.append(copy_to(res_far.at[tiles], res_far_recv.at[tiles], gram_sem.at[half * 2], far))
    for copy in (far_copies[0], gram_copies[2], far_copies[1]):
        copy.start()
    for chunk in range(LATE, CHUNKS):
        far_gram(chunk)
        gram_copies[chunk].start()
    wait_all([mask32.at[pl.ds(2, 2), pl.ds(0, early)], rate.at[pl.ds(2, 2), pl.ds(0, early)]], in_sem.at[3])
    convert(2, 0, early)
    own_mask_copy = copy_to(mask16.at[2], mask16_peer.at[1], own_sem.at[0], pair)
    own_mask_copy.start()
    convert(3, 0, early)
    res_pair[1] = user_residual(2, pair_col)
    pair_copies[1].start()
    own_part = user_residual(3, col)
    wait_all([mask16_peer.at[1], item16_peer.at[pl.ds(1, 2)], mask16_direct, res_pair_recv.at[1]], own_sem.at[0])
    for chunk in range(CHUNKS):
        gram_own[:, chunk_rows(chunk)] = gram_part(3, chunk_rows(chunk))
    for lane in range(2):
        put_products(2 + lane, item16_peer[1 + lane])
        gram_own[:, :DIRECT] += gram_of(2 + lane, mask16_direct[lane])
    res_own[...] = own_part + res_pair_recv[1] - user_ridge * user0[:, block_rows(col)]

    wait_for(late_recv.at[0], late_sem.at[0])
    for slot in range(COLS):
        seen_rate = jnp.where(mask32[slot] > 0, rate[slot], 0.0)
        zrate[slot] = three_terms(seen_rate[:early])
        late_rated[row * COLS + order[slot]] = seen_rate[early:].astype(BF16)

    def item_sums(factors, seen, rated):
        pairs = stacked(pair_products(factors.astype(F32)))
        return dot_nn(pairs, seen), dot_nn(factors, rated)

    def item_part(entries, acc):
        factors = side_by_side(fac[source, t] for source, _, chunk in entries for t in chunk_tiles(chunk))
        seen = stacked(mask16[slot, chunk_rows(chunk), :] for _, slot, chunk in entries)
        rated = stacked(zrate[slot, chunk_rows(chunk), :] for _, slot, chunk in entries)
        sums = item_sums(factors, seen, rated)
        return sums if acc is None else (acc[0] + sums[0], acc[1] + sums[1])

    def late_part(of_row, chunk):
        tiles = [t - early // LANES for t in chunk_tiles(chunk)]
        rows = pl.ds(STARTS[chunk] - early, WIDTHS[chunk])
        factors = side_by_side(late_fac[of_row * COLS + block, t] for block in range(COLS) for t in tiles)
        seen = stacked(late_seen[of_row * COLS + block, rows, :] for block in range(COLS))
        rated = stacked(late_rated[of_row * COLS + block, rows, :] for block in range(COLS))
        gram, rated_sum = item_sums(factors, seen, rated)
        index = chunk - LATE, lax.rem(of_row + row, 2)
        late_sums[index + (pl.ds(0, terms),)] = gram[:terms] + gram[terms:]
        late_sums[index + (pl.ds(terms, RANK),)] = rated_sum

    def split_late(slot):
        value = late_recv[order[slot]].astype(F32)
        seen = value < jnp.inf
        late_seen[(1 - row) * COLS + order[slot]] = seen.astype(F32).astype(BF16)
        late_rated[(1 - row) * COLS + order[slot]] = jnp.where(seen, value, 0.0).astype(BF16)

    groups = (range(0, early // LANES), range(early // LANES, span // LANES))

    def send_users(group):
        mine = user1.at[col, pl.ds(groups[group][0], len(groups[group]))]
        for lane, (device, _, _) in enumerate(peers[:2 + group]):
            sem = user_sem.at[1 if (group, lane) == (0, 1) else 0]
            copy_to(mine, mine, sem, device).start()

    def forward_users():
        theirs = user1.at[far_col, pl.ds(groups[0][0], len(groups[0]))]
        wait_for(theirs, user_sem.at[1])
        copy_to(theirs, theirs, user_sem.at[0], pair).start()

    def solve(chunk):
        lanes = chunk_rows(chunk)
        if chunk != 1:
            together = [gram_recv.at[pl.ds(sum(PACKED[:c]), PACKED[c])] for c in ((0, 1) if chunk == 0 else (chunk,))]
            if chunk in (0, LATE):
                together.append(res_far_recv.at[res_groups[chunk // LATE]])
            wait_all(together, gram_sem.at[max(chunk - 1, 0)])
        far_diags = unpack(chunk)
        diags = [gram_own[d * RANK:(d + 1) * RANK, lanes] + far_diags[d] for d in range(DIAGS)]
        start = user0[:, block_rows(col, STARTS[chunk], WIDTHS[chunk])]
        residual = res_own[:, lanes] + side_by_side(res_far_recv[t].astype(F32) for t in chunk_tiles(chunk))
        solved = cg_solve(diags, residual, start, user_ridge)
        return [solved[:, i * LANES:(i + 1) * LANES] for i in range(WIDTHS[chunk] // LANES)]

    fac_groups = pl.ds(0, STARTS[2] // LANES), pl.ds(STARTS[2] // LANES, WIDTHS[2] // LANES)

    def entries_of(lanes, chunks):
        return [(peers[lane][1], peers[lane][2], chunk) for chunk in chunks for lane in lanes]

    for chunk in range(LATE):
        pieces = solve(chunk)
        tiles = chunk_tiles(chunk)
        for t, piece in zip(tiles, pieces):
            fac[col, t] = piece.astype(BF16)
            user1[col, t] = piece
        if chunk:
            mine = fac.at[col, fac_groups[chunk - 1]]
            for lane, (device, _, _) in list(enumerate(peers))[::-1]:
                copy_to(mine, mine, fac_sem.at[min(lane, 1)], device).start()
    send_users(0)
    sums = item_part([(col, 3, chunk) for chunk in range(LATE)], None)
    wait_for(fac.at[0], fac_sem.at[0])
    sums = item_part(entries_of((0,), range(LATE)), sums)
    for chunk in range(LATE, CHUNKS):
        pieces = solve(chunk)
        tiles = chunk_tiles(chunk)
        for t, piece in zip(tiles, pieces):
            late_fac[row * COLS + col, t - early // LANES] = piece.astype(BF16)
            user1[col, t] = piece
        mine = late_fac.at[row * COLS + col, pl.ds(tiles[0] - early // LANES, len(tiles))]
        for lane, device in list(enumerate(others))[::-1]:
            copy_to(mine, mine, late_fac_sem.at[(chunk - LATE) * 2 + lane // 3 - lane // 6], device).start()
    send_users(1)
    wait_for(fac.at[pl.ds(0, 2)], fac_sem.at[1])
    sums = item_part(entries_of((1, 2), range(LATE)), sums)
    gram = sums[0][:terms] + sums[0][terms:]
    start = item16[...].astype(F32)
    residual = sums[1][:, :items] + sums[1][:, items:2 * items] + sums[1][:, 2 * items:]
    residual = residual - apply_gram(diagonals(gram), start)
    high = residual.astype(BF16)
    item_send[:terms] = gram.astype(BF16)
    item_send[terms:terms + RANK] = high
    item_send[terms + RANK:] = (residual - high.astype(F32)).astype(BF16)
    cross_copy = copy_to(item_send, item_recv, cross_sem.at[0], cross)
    cross_copy.start()
    wait_for(late_recv.at[pl.ds(1, COLS - 1)], late_sem.at[1])
    for slot in range(COLS):
        split_late(slot)
    forward_users()

    def late_arrived(chunk, which):
        tiles = chunk_tiles(chunk)
        view = late_fac.at[pl.ds(0, COLS - 1 + which), pl.ds(tiles[0] - early // LANES, len(tiles))]
        wait_for(view, late_fac_sem.at[(chunk - LATE) * 2 + which])

    for chunk in range(LATE, CHUNKS):
        for which, of_row in enumerate((row, 1 - row)):
            late_arrived(chunk, which)
            pl.when(col < COLS)(functools.partial(late_part, of_row, chunk))
    late_total = sum((late_sums[chunk, 0] for chunk in range(1, CHUNKS - LATE)), late_sums[0, 0])
    late_total = late_total + sum((late_sums[chunk, 1] for chunk in range(1, CHUNKS - LATE)), late_sums[0, 1])
    late_gram = late_total[:terms]
    late_residual = late_total[terms:] - apply_gram(diagonals(late_gram), start)

    wait_all([user1.at[0, pl.ds(0, early // LANES)]] * 2 + [user1.at[0, pl.ds(0, late // LANES)]] * 3, user_sem.at[0])
    for source in range(COLS):
        for t in range(span // LANES):
            user_out[:, pl.ds(source * span + t * LANES, LANES)] = user1[source, t]

    cross_copy.wait_recv()
    full = item_send[...].astype(F32) + item_recv[...].astype(F32)
    residual = full[terms:terms + RANK] + full[terms + RANK:] + late_residual - item_ridge * item0[...]
    item_out[...] = cg_solve(diagonals(full[:terms] + late_gram), residual, item0[...], item_ridge)

    wait_all(sent, send_sem.at[0])


def write_kernel(user_ref, item_ref, user_out, item_out, sems):
    copies = [
        pltpu.make_async_copy(user_ref, user_out, sems.at[0]),
        pltpu.make_async_copy(item_ref, item_out, sems.at[1]),
    ]
    for copy in copies:
        copy.start()
    for copy in copies:
        copy.wait()


def solution(mesh):
    row_size = mesh.shape["row"]
    col_size = mesh.shape["col"]
    grid_spec = P(("part", "row"), "col")
    user_spec = P(("part", "row"), None)
    item_spec = P(("part", "col"), None)

    def local_step(ratings_blk, mask_blk, user_blk, item_blk):
        users, items = ratings_blk.shape
        span = users // COLS
        early = STARTS[LATE]
        late = span - early
        tiles = span // LANES
        hbm_spec = pl.BlockSpec(memory_space=pltpu.HBM)
        vmem = pltpu.VMEM
        dma = pltpu.SemaphoreType.DMA
        terms = DIAGS * RANK
        user_new, item_new = pl.pallas_call(
            functools.partial(sweep_kernel, RIDGE_WEIGHT * items * col_size, RIDGE_WEIGHT * users * row_size),
            out_shape=(
                pltpu.VMEM((RANK, users), F32),
                pltpu.VMEM((RANK, items), F32),
            ),
            in_specs=[hbm_spec] * 4,
            out_specs=(pl.BlockSpec(memory_space=pltpu.VMEM),) * 2,
            scratch_shapes=[
                vmem((COLS, span, items), F32),
                vmem((COLS, span, items), jnp.int32),
                vmem((RANK, users), F32),
                vmem((RANK, items), F32),
                vmem((COLS, span, items), BF16),
                vmem((2, span, items), BF16),
                vmem((2, DIRECT, items), BF16),
                vmem((RANK, items), BF16),
                vmem((3, RANK, items), BF16),
                vmem((COLS, terms, 2 * items), BF16),
                vmem((COLS, early, 3 * items), BF16),
                vmem((sum(PACKED), RANK, LANES), BF16),
                vmem((sum(PACKED), RANK, LANES), BF16),
                vmem((terms, span), F32),
                vmem((2, RANK, span), F32),
                vmem((2, RANK, span), F32),
                vmem((tiles, RANK, LANES), BF16),
                vmem((tiles, RANK, LANES), BF16),
                vmem((RANK, span), F32),
                vmem((COLS, early // LANES, RANK, LANES), BF16),
                vmem((COLS, tiles, RANK, LANES), F32),
                vmem((terms + 2 * RANK, items), BF16),
                vmem((terms + 2 * RANK, items), BF16),
                vmem((COLS, late, items), BF16),
                vmem((COLS, late, items), BF16),
                vmem((2 * COLS, late, items), BF16),
                vmem((2 * COLS, late, items), BF16),
                vmem((2 * COLS, late // LANES, RANK, LANES), BF16),
                vmem((CHUNKS - LATE, 2, terms + RANK, items), F32),
                dma((8,)),
                dma((1,)),
                dma((1,)),
                dma((1,)),
                dma((2,)),
                dma((1,)),
                dma((CHUNKS - 1,)),
                dma((2,)),
                dma((2,)),
                dma((1,)),
                dma((2,)),
                dma((2 * (CHUNKS - LATE),)),
            ],
            compiler_params=pltpu.CompilerParams(collective_id=0, has_side_effects=True, vmem_limit_bytes=60000 * 1024),
        )(ratings_blk, mask_blk, user_blk.T, item_blk.T)
        user_new, item_new = pl.pallas_call(
            write_kernel,
            out_shape=(
                jax.ShapeDtypeStruct((RANK, users), F32),
                jax.ShapeDtypeStruct((RANK, items), F32),
            ),
            in_specs=[pl.BlockSpec(memory_space=pltpu.VMEM)] * 2,
            out_specs=(hbm_spec, hbm_spec),
            scratch_shapes=[dma((2,))],
            compiler_params=pltpu.CompilerParams(vmem_limit_bytes=2**20),
        )(user_new, item_new)
        return user_new.T, item_new.T

    return jax.shard_map(local_step, mesh=mesh, in_specs=(grid_spec, grid_spec, user_spec, item_spec), out_specs=(user_spec, item_spec), check_vma=False)
```

```python
import functools
import math

import jax
import jax.numpy as jnp
from jax import lax
from jax.experimental import pallas as pl
from jax.experimental.pallas import tpu as pltpu
from jax.sharding import PartitionSpec as P

CG_STEPS = 4
RIDGE_WEIGHT = 0.0005
RANK = 16
DIAGS = RANK // 2 + 1
MESH = pl.DeviceIdType.MESH
F32 = jnp.float32
BF16 = jnp.bfloat16
COLS = 4
LANES = 128
HALF = RANK // 2
WIDTHS = (256, 256, 128, 256, 128)
STARTS = tuple(sum(WIDTHS[:i]) for i in range(len(WIDTHS)))
CHUNKS = len(WIDTHS)
LATE = 3
DIRECT = 128


def dot_nt(a, b):
    return lax.dot_general(a, b, (((1,), (1,)), ((), ())), preferred_element_type=F32)


def dot_nn(a, b):
    return lax.dot_general(a, b, (((1,), (0,)), ((), ())), preferred_element_type=F32)


def turn(x, shift):
    return x if shift % RANK == 0 else pltpu.roll(x, shift % RANK, 0)


def pair_products(fac):
    prods = jnp.concatenate([fac * turn(fac, -d) for d in range(DIAGS)], axis=0)
    high = prods.astype(BF16)
    low = (prods - high.astype(F32)).astype(BF16)
    return high, low


def apply_gram(diags, vec):
    parts = [diags[d] * turn(vec, -d) for d in range(DIAGS)]
    parts += [turn(diags[d] * vec, d) for d in range(1, RANK // 2)]
    while len(parts) > 1:
        parts = [sum(parts[i:i + 2][1:], parts[i]) for i in range(0, len(parts), 2)]
    return parts[0]


def cg_solve(diags, residual, start, ridge):
    direction = residual
    estimate = start
    res_sq = jnp.sum(residual * residual, axis=0, keepdims=True)
    for cg_step in range(CG_STEPS):
        gram_dir = apply_gram(diags, direction) + ridge * direction
        step_size = res_sq / jnp.sum(direction * gram_dir, axis=0, keepdims=True)
        estimate = estimate + step_size * direction
        if cg_step + 1 < CG_STEPS:
            residual = residual - step_size * gram_dir
            new_sq = jnp.sum(residual * residual, axis=0, keepdims=True)
            direction = residual + (new_sq / res_sq) * direction
            res_sq = new_sq
    return estimate


def far_span(chunk):
    skip = DIRECT if chunk == 0 else 0
    return STARTS[chunk] + skip, WIDTHS[chunk] - skip


def packed_tiles(chunk):
    tiles = far_span(chunk)[1] // LANES
    return HALF * tiles + (tiles + 1) // 2


PACKED = tuple(packed_tiles(chunk) for chunk in range(CHUNKS))


def chunk_tiles(chunk):
    return range(STARTS[chunk] // LANES, (STARTS[chunk] + WIDTHS[chunk]) // LANES)


def side_by_side(blocks):
    return jnp.concatenate(list(blocks), axis=1)


def stacked(blocks):
    return jnp.concatenate(list(blocks), axis=0)


def three_terms(values):
    high = values.astype(BF16)
    rest = values - high.astype(F32)
    middle = rest.astype(BF16)
    return side_by_side([high, middle, (rest - middle.astype(F32)).astype(BF16)])


def diagonals(full):
    return [full[d * RANK:(d + 1) * RANK] for d in range(DIAGS)]


def sweep_kernel(
    user_ridge, item_ridge,
    ratings_hbm, mask_hbm, user_hbm, item_hbm,
    user_out, item_out,
    rate, mask32, user0, item0,
    mask16, mask16_peer, mask16_direct, item16, item16_peer, ffs, zrate,
    gram_send, gram_recv, gram_own,
    res_pair, res_pair_recv, res_far, res_far_recv, res_own,
    fac, user1, item_send, item_recv,
    late_send, late_recv, late_seen, late_rated, late_fac, late_sums, early_sums,
    in_sem, send_sem, item_sem, own_sem, mask_sem, pair_sem, gram_sem, fac_sem, user_sem, cross_sem, late_sem, late_fac_sem,
):
    part = lax.axis_index("part")
    row = lax.axis_index("row")
    col = lax.axis_index("col")
    chip = col // 2
    core = col % 2
    pair_col = chip * 2 + (1 - core)
    far_col = (1 - chip) * 2 + core
    diag_col = (1 - chip) * 2 + (1 - core)
    pair = (part, row, pair_col)
    far = (part, row, far_col)
    diag = (part, row, diag_col)
    cross = (part, 1 - row, col)
    peers = ((pair, pair_col, 2), (far, far_col, 1), (diag, diag_col, 0))
    far_chip = [(part, row, (1 - chip) * 2 + k) for k in range(2)]
    cross_chip = [(part, 1 - row, chip * 2 + k) for k in range(2)]
    diag_chip = [(part, 1 - row, (1 - chip) * 2 + k) for k in range(2)]

    span = mask16.shape[1]
    items = item0.shape[1]
    terms = DIAGS * RANK
    early = STARTS[LATE]
    late = span - early

    sent = []

    def copy_to(src, dst, recv_sem, device):
        sent.append(src)
        return pltpu.make_async_remote_copy(
            src_ref=src, dst_ref=dst, send_sem=send_sem.at[0], recv_sem=recv_sem,
            device_id=device, device_id_type=MESH,
        )

    def wait_for(ref, sem):
        pltpu.make_async_copy(ref, ref, sem).wait()

    def wait_all(refs, sem):
        count = sum(math.prod(ref.shape) * ref.dtype.itemsize for ref in refs) // (items * rate.dtype.itemsize)
        parts = next(parts for parts in (1, 2, COLS) if count <= parts * span and count % parts == 0)
        wait_for(rate.at[pl.ds(0, parts), pl.ds(0, count // parts)], sem)

    barrier = pltpu.get_barrier_semaphore()
    for device in (pair, far, diag, cross):
        pl.semaphore_signal(barrier, inc=1, device_id=device, device_id_type=MESH)

    order = (diag_col, far_col, pair_col, col)

    def load(src, dst, slot):
        return pltpu.make_async_copy(src, dst, in_sem.at[slot])

    def block_rows(block, start=0, size=span):
        return pl.ds(pl.multiple_of(block * span + start, LANES), size)

    def chunk_rows(chunk):
        return pl.ds(STARTS[chunk], WIDTHS[chunk])

    item_load = load(item_hbm, item0, 0)
    user_load = load(user_hbm, user0, 2)
    rate_loads = []
    rate_late_loads = []
    mask_loads = []
    splits = (WIDTHS[0], WIDTHS[0], early, early)
    for slot, block in enumerate(order):
        rate_loads.append(load(ratings_hbm.at[block_rows(block, 0, early)], rate.at[slot, pl.ds(0, early)], 2 + slot // 2))
        rate_late_loads.append(load(ratings_hbm.at[block_rows(block, early, late)], rate.at[slot, pl.ds(early, late)], 4 + min(slot, 1)))
        pieces = []
        for half, (start, size) in enumerate(((0, splits[slot]), (splits[slot], span - splits[slot]))):
            src = mask_hbm.at[block_rows(block, start, size)]
            pieces.append(load(src, mask32.at[slot, pl.ds(start, size)], (6, 7, 3)[min(slot, 2)] if half == 0 else (1, 5)[slot // 2]))
        mask_loads.append(pieces)

    def convert(slot, start, size):
        rows = pl.ds(start, size)
        seen = mask32[slot, rows].astype(F32).astype(BF16)
        mask16[slot, rows] = seen
        if start + size == span:
            late_seen[row * COLS + order[slot]] = seen[early - start:]

    item_load.start()
    for pieces in mask_loads[:2]:
        for copy in pieces:
            copy.start()
    for slot in range(COLS):
        if slot >= 2:
            mask_loads[slot][1].start()
        rate_late_loads[slot].start()

    item_load.wait()
    item16[...] = item0[...].astype(BF16)
    pl.semaphore_wait(barrier, 4)
    item_copies = []
    for lane, (device, _, _) in enumerate(peers):
        item_copies.append(copy_to(item16, item16_peer.at[lane], (own_sem if lane else item_sem).at[0], device))
        item_copies[-1].start()
    first = pl.ds(0, DIRECT)

    def send_late(slot):
        rows = pl.ds(early, late)
        late_send[order[slot]] = jnp.where(mask32[slot, rows] > 0, rate[slot, rows], jnp.inf).astype(BF16)
        copy_to(late_send.at[order[slot]], late_recv.at[order[slot]], late_sem.at[min(slot, 1)], cross).start()

    def mask_copy(half):
        rows = pl.ds(*((splits[0], span - splits[0]) if half else (DIRECT, splits[0] - DIRECT)))
        return copy_to(mask16.at[0, rows], mask16_peer.at[0, rows], mask_sem.at[half], pair)

    mask_copies = [mask_copy(half) for half in range(2)]
    mask_loads[0][0].wait()
    convert(0, 0, splits[0])
    mask_copies[0].start()
    copy_to(mask16.at[0, first], mask16_direct.at[1], own_sem.at[0], diag).start()
    mask_loads[1][0].wait()
    convert(1, 0, splits[1])
    copy_to(mask16.at[1, first], mask16_direct.at[0], own_sem.at[0], far).start()
    rest = pl.ds(splits[0], span - splits[0])
    wait_for(mask32.at[pl.ds(0, 2), rest], in_sem.at[1])
    convert(0, splits[0], span - splits[0])
    mask_copies[1].start()
    user_load.start()
    for pieces in mask_loads[2:]:
        pieces[0].start()
    for copy in rate_loads:
        copy.start()
    rate_late_loads[0].wait()
    send_late(0)
    convert(1, splits[1], span - splits[1])
    wait_all([rate.at[pl.ds(1, COLS - 1), pl.ds(early, late)], mask32.at[pl.ds(2, 2), pl.ds(early, late)]], in_sem.at[5])
    send_late(1)
    for slot in (2, 3):
        convert(slot, early, late)
        send_late(slot)

    def put_products(index, factors):
        high, low = pair_products(factors.astype(F32))
        ffs[index, :, :items] = high
        ffs[index, :, items:] = low

    put_products(0, item16[...])
    item_copies[0].wait_recv()
    put_products(1, item16_peer[0])

    def gram_of(index, seen):
        return dot_nt(ffs[index], side_by_side([seen, seen]))

    def gram_part(slot, rows):
        return gram_of(0, mask16[slot, rows, :]) + gram_of(1, mask16_peer[slot // 2, rows, :])

    def pack(gram, chunk):
        tiles = gram.shape[1] // LANES
        base = sum(PACKED[:chunk])
        for d in range(HALF):
            for t in range(tiles):
                piece = gram[d * RANK:(d + 1) * RANK, t * LANES:(t + 1) * LANES]
                gram_send[base + d * tiles + t] = piece.astype(BF16)
        half = gram[HALF * RANK:HALF * RANK + HALF]
        for t in range(0, tiles, 2):
            both = [half[:, min(u, tiles - 1) * LANES:][:, :LANES] for u in (t, t + 1)]
            gram_send[base + HALF * tiles + t // 2] = stacked(both).astype(BF16)

    def unpack(chunk):
        gap = far_span(chunk)[1]
        tiles = gap // LANES
        base = sum(PACKED[:chunk])
        diags = [side_by_side(gram_recv[base + d * tiles + t].astype(F32) for t in range(tiles)) for d in range(HALF)]
        pieces = []
        for t in range(0, tiles, 2):
            both = gram_recv[base + HALF * tiles + t // 2].astype(F32)
            for half in (both[:HALF], both[HALF:])[:tiles - t]:
                pieces.append(stacked([half, half]))
        diags.append(side_by_side(pieces))
        pad = WIDTHS[chunk] - gap
        return [side_by_side([jnp.zeros((RANK, pad), F32), d]) if pad else d for d in diags]

    gram_copies = []
    for chunk in range(CHUNKS):
        part_of = pl.ds(sum(PACKED[:chunk]), PACKED[chunk])
        gram_copies.append(copy_to(gram_send.at[part_of], gram_recv.at[part_of], gram_sem.at[max(chunk - 1, 0)], far))

    def far_gram(chunk):
        if chunk < 2:
            mask_copies[chunk].wait_recv()
        pack(gram_part(1, pl.ds(*far_span(chunk))), chunk)

    for chunk in range(2):
        far_gram(chunk)
        gram_copies[chunk].start()

    def user_residual(slot, block):
        start = user0[:, block_rows(block)]
        scores = dot_nn(start.T.astype(BF16), item16[...])
        resid = jnp.where(mask32[slot] > 0, rate[slot] - scores, 0.0).astype(BF16)
        return dot_nt(item16[...], resid)

    wait_all([user0, rate.at[pl.ds(0, 2), pl.ds(0, early)]], in_sem.at[2])
    res_pair[0] = user_residual(0, diag_col)
    pair_copies = [copy_to(res_pair.at[slot], res_pair_recv.at[slot], (own_sem if slot else pair_sem).at[0], pair) for slot in range(2)]
    pair_copies[0].start()
    far_part = user_residual(1, far_col)
    far_gram(2)
    pair_copies[0].wait_recv()
    total = (far_part + res_pair_recv[0]).astype(BF16)
    for t in range(span // LANES):
        res_far[t] = total[:, t * LANES:(t + 1) * LANES]
    far_copies = []
    res_groups = pl.ds(0, early // LANES), pl.ds(early // LANES, late // LANES)
    for half, tiles in enumerate(res_groups):
        far_copies.append(copy_to(res_far.at[tiles], res_far_recv.at[tiles], gram_sem.at[half * 2], far))
    for copy in (far_copies[0], gram_copies[2], far_copies[1]):
        copy.start()
    for chunk in range(LATE, CHUNKS):
        far_gram(chunk)
        gram_copies[chunk].start()
    wait_all([mask32.at[pl.ds(2, 2), pl.ds(0, early)], rate.at[pl.ds(2, 2), pl.ds(0, early)]], in_sem.at[3])
    convert(2, 0, early)
    own_mask_copy = copy_to(mask16.at[2], mask16_peer.at[1], own_sem.at[0], pair)
    own_mask_copy.start()
    convert(3, 0, early)
    res_pair[1] = user_residual(2, pair_col)
    pair_copies[1].start()
    own_part = user_residual(3, col)
    wait_all([mask16_peer.at[1], item16_peer.at[pl.ds(1, 2)], mask16_direct, res_pair_recv.at[1]], own_sem.at[0])
    for chunk in range(CHUNKS):
        gram_own[:, chunk_rows(chunk)] = gram_part(3, chunk_rows(chunk))
    for lane in range(2):
        put_products(2 + lane, item16_peer[1 + lane])
        gram_own[:, :DIRECT] += gram_of(2 + lane, mask16_direct[lane])
    res_own[...] = own_part + res_pair_recv[1] - user_ridge * user0[:, block_rows(col)]

    wait_for(late_recv.at[0], late_sem.at[0])
    for slot in range(COLS):
        seen_rate = jnp.where(mask32[slot] > 0, rate[slot], 0.0)
        zrate[slot] = three_terms(seen_rate[:early])
        late_rated[row * COLS + order[slot]] = seen_rate[early:].astype(BF16)

    def item_sums(factors, seen, rated):
        pairs = stacked(pair_products(factors.astype(F32)))
        return dot_nn(pairs, seen), dot_nn(factors, rated)

    def item_part(entries):
        factors = side_by_side(fac[source, t] for source, _, chunk in entries for t in chunk_tiles(chunk))
        seen = stacked(mask16[slot, chunk_rows(chunk), :] for _, slot, chunk in entries)
        rated = stacked(zrate[slot, chunk_rows(chunk), :] for _, slot, chunk in entries)
        gram, rated_sum = item_sums(factors, seen, rated)
        return gram[:terms] + gram[terms:], sum((rated_sum[:, i * items:(i + 1) * items] for i in (1, 2)), rated_sum[:, :items])

    def add_part(entries, index):
        @pl.when(col < COLS)
        def _():
            early_sums[index, :terms], early_sums[index, terms:] = item_part(entries)

    def late_part(of_row, chunk):
        tiles = [t - early // LANES for t in chunk_tiles(chunk)]
        rows = pl.ds(STARTS[chunk] - early, WIDTHS[chunk])
        factors = side_by_side(late_fac[of_row * COLS + block, t] for block in range(COLS) for t in tiles)
        seen = stacked(late_seen[of_row * COLS + block, rows, :] for block in range(COLS))
        rated = stacked(late_rated[of_row * COLS + block, rows, :] for block in range(COLS))
        gram, rated_sum = item_sums(factors, seen, rated)
        index = chunk - LATE, lax.rem(of_row + row, 2)
        late_sums[index + (pl.ds(0, terms),)] = gram[:terms] + gram[terms:]
        late_sums[index + (pl.ds(terms, RANK),)] = rated_sum

    def split_late(slot):
        value = late_recv[order[slot]].astype(F32)
        seen = value < jnp.inf
        late_seen[(1 - row) * COLS + order[slot]] = seen.astype(F32).astype(BF16)
        late_rated[(1 - row) * COLS + order[slot]] = jnp.where(seen, value, 0.0).astype(BF16)

    groups = (range(0, early // LANES), range(early // LANES, span // LANES))

    def send_users(group):
        mine = user1.at[col, pl.ds(groups[group][0], len(groups[group]))]
        for lane, (device, _, _) in enumerate(peers[:2 + group]):
            sem = user_sem.at[1 if (group, lane) == (0, 1) else 0]
            copy_to(mine, mine, sem, device).start()

    def forward_users():
        theirs = user1.at[far_col, pl.ds(groups[0][0], len(groups[0]))]
        wait_for(theirs, user_sem.at[1])
        copy_to(theirs, theirs, user_sem.at[0], pair).start()

    def solve(chunk):
        lanes = chunk_rows(chunk)
        if chunk != 1:
            together = [gram_recv.at[pl.ds(sum(PACKED[:c]), PACKED[c])] for c in ((0, 1) if chunk == 0 else (chunk,))]
            if chunk in (0, LATE):
                together.append(res_far_recv.at[res_groups[chunk // LATE]])
            wait_all(together, gram_sem.at[max(chunk - 1, 0)])
        far_diags = unpack(chunk)
        diags = [gram_own[d * RANK:(d + 1) * RANK, lanes] + far_diags[d] for d in range(DIAGS)]
        start = user0[:, block_rows(col, STARTS[chunk], WIDTHS[chunk])]
        residual = res_own[:, lanes] + side_by_side(res_far_recv[t].astype(F32) for t in chunk_tiles(chunk))
        solved = cg_solve(diags, residual, start, user_ridge)
        return [solved[:, i * LANES:(i + 1) * LANES] for i in range(WIDTHS[chunk] // LANES)]

    fac_groups = pl.ds(0, STARTS[2] // LANES), pl.ds(STARTS[2] // LANES, WIDTHS[2] // LANES)

    def entries_of(lanes, chunks):
        return [(peers[lane][1], peers[lane][2], chunk) for chunk in chunks for lane in lanes]

    for chunk in range(LATE):
        pieces = solve(chunk)
        tiles = chunk_tiles(chunk)
        for t, piece in zip(tiles, pieces):
            fac[col, t] = piece.astype(BF16)
            user1[col, t] = piece
        if chunk:
            mine = fac.at[col, fac_groups[chunk - 1]]
            for device in far_chip:
                copy_to(mine, mine, fac_sem.at[chunk], device).start()
            copy_to(mine, mine, fac_sem.at[0], pair).start()
    send_users(0)
    add_part([(col, 3, chunk) for chunk in range(LATE)], 0)
    wait_for(fac.at[0], fac_sem.at[0])
    add_part(entries_of((0,), range(LATE)), 1)
    for chunk in range(LATE, CHUNKS):
        pieces = solve(chunk)
        tiles = chunk_tiles(chunk)
        for t, piece in zip(tiles, pieces):
            late_fac[row * COLS + col, t - early // LANES] = piece.astype(BF16)
            user1[col, t] = piece
        mine = late_fac.at[row * COLS + col, pl.ds(tiles[0] - early // LANES, len(tiles))]
        for device, other_row in [(diag_chip[1], 1), (diag_chip[0], 1), (cross_chip[1], 1), (cross_chip[0], 1), (far_chip[1], 0), (far_chip[0], 0), (pair, 0)]:
            copy_to(mine, mine, late_fac_sem.at[(chunk - LATE) * 2 + other_row], device).start()
    send_users(1)
    wait_for(fac.at[pl.ds(0, 2), fac_groups[0]], fac_sem.at[1])
    add_part(entries_of((1, 2), range(LATE - 1)), 2)
    wait_for(fac.at[pl.ds(0, 2), fac_groups[1]], fac_sem.at[2])
    gram, residual = item_part(entries_of((1, 2), (LATE - 1,)))
    before = early_sums[0] + early_sums[1] + early_sums[2]
    gram = gram + before[:terms]
    start = item16[...].astype(F32)
    residual = residual + before[terms:] - apply_gram(diagonals(gram), start)
    high = residual.astype(BF16)
    item_send[:terms] = gram.astype(BF16)
    item_send[terms:terms + RANK] = high
    item_send[terms + RANK:] = (residual - high.astype(F32)).astype(BF16)
    cross_copy = copy_to(item_send, item_recv, cross_sem.at[0], cross)
    cross_copy.start()
    wait_for(late_recv.at[pl.ds(1, COLS - 1)], late_sem.at[1])
    for slot in range(COLS):
        split_late(slot)
    forward_users()

    def late_arrived(chunk, which):
        tiles = chunk_tiles(chunk)
        view = late_fac.at[pl.ds(0, COLS - 1 + which), pl.ds(tiles[0] - early // LANES, len(tiles))]
        wait_for(view, late_fac_sem.at[(chunk - LATE) * 2 + which])

    for which, of_row in enumerate((row, 1 - row)):
        for chunk in range(LATE, CHUNKS):
            late_arrived(chunk, which)
            pl.when(col < COLS)(functools.partial(late_part, of_row, chunk))
    late_total = sum((late_sums[chunk, 0] for chunk in range(1, CHUNKS - LATE)), late_sums[0, 0])
    late_total = late_total + sum((late_sums[chunk, 1] for chunk in range(1, CHUNKS - LATE)), late_sums[0, 1])
    late_gram = late_total[:terms]
    late_residual = late_total[terms:] - apply_gram(diagonals(late_gram), start)

    wait_all([user1.at[0, pl.ds(0, early // LANES)]] * 2 + [user1.at[0, pl.ds(0, late // LANES)]] * 3, user_sem.at[0])
    for source in range(COLS):
        for t in range(span // LANES):
            user_out[:, pl.ds(source * span + t * LANES, LANES)] = user1[source, t]

    cross_copy.wait_recv()
    full = item_send[...].astype(F32) + item_recv[...].astype(F32)
    residual = full[terms:terms + RANK] + full[terms + RANK:] + late_residual - item_ridge * item0[...]
    item_out[...] = cg_solve(diagonals(full[:terms] + late_gram), residual, item0[...], item_ridge)

    wait_all(sent, send_sem.at[0])


def write_kernel(user_ref, item_ref, user_out, item_out, sems):
    copies = [
        pltpu.make_async_copy(user_ref, user_out, sems.at[0]),
        pltpu.make_async_copy(item_ref, item_out, sems.at[1]),
    ]
    for copy in copies:
        copy.start()
    for copy in copies:
        copy.wait()


def solution(mesh):
    row_size = mesh.shape["row"]
    col_size = mesh.shape["col"]
    grid_spec = P(("part", "row"), "col")
    user_spec = P(("part", "row"), None)
    item_spec = P(("part", "col"), None)

    def local_step(ratings_blk, mask_blk, user_blk, item_blk):
        users, items = ratings_blk.shape
        span = users // COLS
        early = STARTS[LATE]
        late = span - early
        tiles = span // LANES
        hbm_spec = pl.BlockSpec(memory_space=pltpu.HBM)
        vmem = pltpu.VMEM
        dma = pltpu.SemaphoreType.DMA
        terms = DIAGS * RANK
        user_new, item_new = pl.pallas_call(
            functools.partial(sweep_kernel, RIDGE_WEIGHT * items * col_size, RIDGE_WEIGHT * users * row_size),
            out_shape=(
                pltpu.VMEM((RANK, users), F32),
                pltpu.VMEM((RANK, items), F32),
            ),
            in_specs=[hbm_spec] * 4,
            out_specs=(pl.BlockSpec(memory_space=pltpu.VMEM),) * 2,
            scratch_shapes=[
                vmem((COLS, span, items), F32),
                vmem((COLS, span, items), jnp.int32),
                vmem((RANK, users), F32),
                vmem((RANK, items), F32),
                vmem((COLS, span, items), BF16),
                vmem((2, span, items), BF16),
                vmem((2, DIRECT, items), BF16),
                vmem((RANK, items), BF16),
                vmem((3, RANK, items), BF16),
                vmem((COLS, terms, 2 * items), BF16),
                vmem((COLS, early, 3 * items), BF16),
                vmem((sum(PACKED), RANK, LANES), BF16),
                vmem((sum(PACKED), RANK, LANES), BF16),
                vmem((terms, span), F32),
                vmem((2, RANK, span), F32),
                vmem((2, RANK, span), F32),
                vmem((tiles, RANK, LANES), BF16),
                vmem((tiles, RANK, LANES), BF16),
                vmem((RANK, span), F32),
                vmem((COLS, early // LANES, RANK, LANES), BF16),
                vmem((COLS, tiles, RANK, LANES), F32),
                vmem((terms + 2 * RANK, items), BF16),
                vmem((terms + 2 * RANK, items), BF16),
                vmem((COLS, late, items), BF16),
                vmem((COLS, late, items), BF16),
                vmem((2 * COLS, late, items), BF16),
                vmem((2 * COLS, late, items), BF16),
                vmem((2 * COLS, late // LANES, RANK, LANES), BF16),
                vmem((CHUNKS - LATE, 2, terms + RANK, items), F32),
                vmem((3, terms + RANK, items), F32),
                dma((8,)),
                dma((1,)),
                dma((1,)),
                dma((1,)),
                dma((2,)),
                dma((1,)),
                dma((CHUNKS - 1,)),
                dma((3,)),
                dma((2,)),
                dma((1,)),
                dma((2,)),
                dma((2 * (CHUNKS - LATE),)),
            ],
            compiler_params=pltpu.CompilerParams(collective_id=0, has_side_effects=True, vmem_limit_bytes=60000 * 1024),
        )(ratings_blk, mask_blk, user_blk.T, item_blk.T)
        user_new, item_new = pl.pallas_call(
            write_kernel,
            out_shape=(
                jax.ShapeDtypeStruct((RANK, users), F32),
                jax.ShapeDtypeStruct((RANK, items), F32),
            ),
            in_specs=[pl.BlockSpec(memory_space=pltpu.VMEM)] * 2,
            out_specs=(hbm_spec, hbm_spec),
            scratch_shapes=[dma((2,))],
            compiler_params=pltpu.CompilerParams(vmem_limit_bytes=2**20),
        )(user_new, item_new)
        return user_new.T, item_new.T

    return jax.shard_map(local_step, mesh=mesh, in_specs=(grid_spec, grid_spec, user_spec, item_spec), out_specs=(user_spec, item_spec), check_vma=False)
```

```python
import functools
import math

import jax
import jax.numpy as jnp
from jax import lax
from jax.experimental import pallas as pl
from jax.experimental.pallas import tpu as pltpu
from jax.sharding import PartitionSpec as P

CG_STEPS = 4
RIDGE_WEIGHT = 0.0005
RANK = 16
DIAGS = RANK // 2 + 1
MESH = pl.DeviceIdType.MESH
F32 = jnp.float32
BF16 = jnp.bfloat16
COLS = 4
LANES = 128
HALF = RANK // 2
WIDTHS = (256, 256, 128, 256, 128)
STARTS = tuple(sum(WIDTHS[:i]) for i in range(len(WIDTHS)))
CHUNKS = len(WIDTHS)
LATE = 3
DIRECT = 128


def dot_nt(a, b):
    return lax.dot_general(a, b, (((1,), (1,)), ((), ())), preferred_element_type=F32)


def dot_nn(a, b):
    return lax.dot_general(a, b, (((1,), (0,)), ((), ())), preferred_element_type=F32)


def turn(x, shift):
    return x if shift % RANK == 0 else pltpu.roll(x, shift % RANK, 0)


def pair_products(fac):
    prods = jnp.concatenate([fac * turn(fac, -d) for d in range(DIAGS)], axis=0)
    high = prods.astype(BF16)
    low = (prods - high.astype(F32)).astype(BF16)
    return high, low


def apply_gram(diags, vec):
    parts = [diags[d] * turn(vec, -d) for d in range(DIAGS)]
    parts += [turn(diags[d] * vec, d) for d in range(1, RANK // 2)]
    while len(parts) > 1:
        parts = [sum(parts[i:i + 2][1:], parts[i]) for i in range(0, len(parts), 2)]
    return parts[0]


def cg_solve(diags, residual, start, ridge):
    direction = residual
    estimate = start
    res_sq = jnp.sum(residual * residual, axis=0, keepdims=True)
    for cg_step in range(CG_STEPS):
        gram_dir = apply_gram(diags, direction) + ridge * direction
        step_size = res_sq / jnp.sum(direction * gram_dir, axis=0, keepdims=True)
        estimate = estimate + step_size * direction
        if cg_step + 1 < CG_STEPS:
            residual = residual - step_size * gram_dir
            new_sq = jnp.sum(residual * residual, axis=0, keepdims=True)
            direction = residual + (new_sq / res_sq) * direction
            res_sq = new_sq
    return estimate


def far_span(chunk):
    skip = DIRECT if chunk == 0 else 0
    return STARTS[chunk] + skip, WIDTHS[chunk] - skip


def packed_tiles(chunk):
    tiles = far_span(chunk)[1] // LANES
    return HALF * tiles + (tiles + 1) // 2


PACKED = tuple(packed_tiles(chunk) for chunk in range(CHUNKS))


def chunk_tiles(chunk):
    return range(STARTS[chunk] // LANES, (STARTS[chunk] + WIDTHS[chunk]) // LANES)


def side_by_side(blocks):
    return jnp.concatenate(list(blocks), axis=1)


def stacked(blocks):
    return jnp.concatenate(list(blocks), axis=0)


def three_terms(values):
    high = values.astype(BF16)
    rest = values - high.astype(F32)
    middle = rest.astype(BF16)
    return side_by_side([high, middle, (rest - middle.astype(F32)).astype(BF16)])


def diagonals(full):
    return [full[d * RANK:(d + 1) * RANK] for d in range(DIAGS)]


def sweep_kernel(
    user_ridge, item_ridge,
    ratings_hbm, mask_hbm, user_hbm, item_hbm,
    user_out, item_out,
    rate, mask32, user0, item0,
    mask16, mask16_peer, mask16_direct, item16, item16_peer, ffs, zrate,
    gram_send, gram_recv, gram_own,
    res_pair, res_pair_recv, res_far, res_far_recv, res_own,
    fac, user1, item_send, item_recv,
    late_send, late_recv, late_seen, late_rated, late_fac, late_sums, early_sums,
    in_sem, send_sem, item_sem, own_sem, mask_sem, pair_sem, gram_sem, fac_sem, user_sem, cross_sem, late_sem, late_fac_sem,
):
    part = lax.axis_index("part")
    row = lax.axis_index("row")
    col = lax.axis_index("col")
    chip = col // 2
    core = col % 2
    pair_col = chip * 2 + (1 - core)
    far_col = (1 - chip) * 2 + core
    diag_col = (1 - chip) * 2 + (1 - core)
    pair = (part, row, pair_col)
    far = (part, row, far_col)
    diag = (part, row, diag_col)
    cross = (part, 1 - row, col)
    peers = ((pair, pair_col, 2), (far, far_col, 1), (diag, diag_col, 0))
    far_chip = [(part, row, (1 - chip) * 2 + k) for k in range(2)]
    cross_chip = [(part, 1 - row, chip * 2 + k) for k in range(2)]
    diag_chip = [(part, 1 - row, (1 - chip) * 2 + k) for k in range(2)]

    span = mask16.shape[1]
    items = item0.shape[1]
    terms = DIAGS * RANK
    early = STARTS[LATE]
    late = span - early

    sent = []

    def copy_to(src, dst, recv_sem, device):
        sent.append(src)
        return pltpu.make_async_remote_copy(
            src_ref=src, dst_ref=dst, send_sem=send_sem.at[0], recv_sem=recv_sem,
            device_id=device, device_id_type=MESH,
        )

    def wait_for(ref, sem):
        pltpu.make_async_copy(ref, ref, sem).wait()

    def wait_all(refs, sem):
        count = sum(math.prod(ref.shape) * ref.dtype.itemsize for ref in refs) // (items * rate.dtype.itemsize)
        parts = next(parts for parts in (1, 2, COLS) if count <= parts * span and count % parts == 0)
        wait_for(rate.at[pl.ds(0, parts), pl.ds(0, count // parts)], sem)

    barrier = pltpu.get_barrier_semaphore()
    for device in (pair, far, diag, cross):
        pl.semaphore_signal(barrier, inc=1, device_id=device, device_id_type=MESH)

    order = (diag_col, far_col, pair_col, col)

    def load(src, dst, slot):
        return pltpu.make_async_copy(src, dst, in_sem.at[slot])

    def block_rows(block, start=0, size=span):
        return pl.ds(pl.multiple_of(block * span + start, LANES), size)

    def chunk_rows(chunk):
        return pl.ds(STARTS[chunk], WIDTHS[chunk])

    item_load = load(item_hbm, item0, 0)
    user_load = load(user_hbm, user0, 2)
    rate_loads = []
    rate_late_loads = []
    mask_loads = []
    splits = (WIDTHS[0], WIDTHS[0], early, early)
    for slot, block in enumerate(order):
        rate_loads.append(load(ratings_hbm.at[block_rows(block, 0, early)], rate.at[slot, pl.ds(0, early)], 2 + slot // 2))
        rate_late_loads.append(load(ratings_hbm.at[block_rows(block, early, late)], rate.at[slot, pl.ds(early, late)], 4 + min(slot, 1)))
        pieces = []
        for half, (start, size) in enumerate(((0, splits[slot]), (splits[slot], span - splits[slot]))):
            src = mask_hbm.at[block_rows(block, start, size)]
            pieces.append(load(src, mask32.at[slot, pl.ds(start, size)], (6, 7, 3)[min(slot, 2)] if half == 0 else (1, 5)[slot // 2]))
        mask_loads.append(pieces)

    def convert(slot, start, size):
        rows = pl.ds(start, size)
        seen = mask32[slot, rows].astype(F32).astype(BF16)
        mask16[slot, rows] = seen
        if start + size == span:
            late_seen[row * COLS + order[slot]] = seen[early - start:]

    item_load.start()
    for pieces in mask_loads[:2]:
        for copy in pieces:
            copy.start()
    for slot in range(COLS):
        if slot >= 2:
            mask_loads[slot][1].start()
        rate_late_loads[slot].start()

    item_load.wait()
    item16[...] = item0[...].astype(BF16)
    pl.semaphore_wait(barrier, 4)
    item_copies = []
    for lane, (device, _, _) in enumerate(peers[:2]):
        item_copies.append(copy_to(item16, item16_peer.at[lane], item_sem.at[lane], device))
        item_copies[-1].start()
    first = pl.ds(0, DIRECT)

    def send_late(slot):
        rows = pl.ds(early, late)
        late_send[order[slot]] = jnp.where(mask32[slot, rows] > 0, rate[slot, rows], jnp.inf).astype(BF16)
        copy_to(late_send.at[order[slot]], late_recv.at[order[slot]], late_sem.at[min(slot, 1)], cross).start()

    def mask_copy(half):
        rows = pl.ds(*((splits[0], span - splits[0]) if half else (DIRECT, splits[0] - DIRECT)))
        return copy_to(mask16.at[0, rows], mask16_peer.at[0, rows], mask_sem.at[half], pair)

    mask_copies = [mask_copy(half) for half in range(2)]
    mask_loads[0][0].wait()
    convert(0, 0, splits[0])
    mask_copies[0].start()
    copy_to(mask16.at[0, first], mask16_direct.at[1], own_sem.at[0], diag).start()
    mask_loads[1][0].wait()
    convert(1, 0, splits[1])
    copy_to(mask16.at[1, first], mask16_direct.at[0], own_sem.at[0], far).start()
    rest = pl.ds(splits[0], span - splits[0])
    wait_for(mask32.at[pl.ds(0, 2), rest], in_sem.at[1])
    convert(0, splits[0], span - splits[0])
    mask_copies[1].start()
    user_load.start()
    for pieces in mask_loads[2:]:
        pieces[0].start()
    for copy in rate_loads:
        copy.start()
    rate_late_loads[0].wait()
    send_late(0)
    convert(1, splits[1], span - splits[1])
    wait_all([rate.at[pl.ds(1, COLS - 1), pl.ds(early, late)], mask32.at[pl.ds(2, 2), pl.ds(early, late)]], in_sem.at[5])
    send_late(1)
    for slot in (2, 3):
        convert(slot, early, late)
        send_late(slot)

    def put_products(index, factors):
        high, low = pair_products(factors.astype(F32))
        ffs[index, :, :items] = high
        ffs[index, :, items:] = low

    put_products(0, item16[...])
    item_copies[0].wait_recv()
    put_products(1, item16_peer[0])

    def gram_of(index, seen):
        return dot_nt(ffs[index], side_by_side([seen, seen]))

    def gram_part(slot, rows):
        return gram_of(0, mask16[slot, rows, :]) + gram_of(1, mask16_peer[slot // 2, rows, :])

    def pack(gram, chunk):
        tiles = gram.shape[1] // LANES
        base = sum(PACKED[:chunk])
        for d in range(HALF):
            for t in range(tiles):
                piece = gram[d * RANK:(d + 1) * RANK, t * LANES:(t + 1) * LANES]
                gram_send[base + d * tiles + t] = piece.astype(BF16)
        half = gram[HALF * RANK:HALF * RANK + HALF]
        for t in range(0, tiles, 2):
            both = [half[:, min(u, tiles - 1) * LANES:][:, :LANES] for u in (t, t + 1)]
            gram_send[base + HALF * tiles + t // 2] = stacked(both).astype(BF16)

    def unpack(chunk):
        gap = far_span(chunk)[1]
        tiles = gap // LANES
        base = sum(PACKED[:chunk])
        diags = [side_by_side(gram_recv[base + d * tiles + t].astype(F32) for t in range(tiles)) for d in range(HALF)]
        pieces = []
        for t in range(0, tiles, 2):
            both = gram_recv[base + HALF * tiles + t // 2].astype(F32)
            for half in (both[:HALF], both[HALF:])[:tiles - t]:
                pieces.append(stacked([half, half]))
        diags.append(side_by_side(pieces))
        pad = WIDTHS[chunk] - gap
        return [side_by_side([jnp.zeros((RANK, pad), F32), d]) if pad else d for d in diags]

    gram_copies = []
    for chunk in range(CHUNKS):
        part_of = pl.ds(sum(PACKED[:chunk]), PACKED[chunk])
        gram_copies.append(copy_to(gram_send.at[part_of], gram_recv.at[part_of], gram_sem.at[max(chunk - 1, 0)], far))

    def far_gram(chunk):
        if chunk < 2:
            mask_copies[chunk].wait_recv()
        pack(gram_part(1, pl.ds(*far_span(chunk))), chunk)

    for chunk in range(2):
        far_gram(chunk)
        gram_copies[chunk].start()

    def user_residual(slot, block):
        start = user0[:, block_rows(block)]
        scores = dot_nn(start.T.astype(BF16), item16[...])
        resid = jnp.where(mask32[slot] > 0, rate[slot] - scores, 0.0).astype(BF16)
        return dot_nt(item16[...], resid)

    wait_all([user0, rate.at[pl.ds(0, 2), pl.ds(0, early)]], in_sem.at[2])
    res_pair[0] = user_residual(0, diag_col)
    pair_copies = [copy_to(res_pair.at[slot], res_pair_recv.at[slot], (own_sem if slot else pair_sem).at[0], pair) for slot in range(2)]
    pair_copies[0].start()
    far_part = user_residual(1, far_col)
    far_gram(2)
    pair_copies[0].wait_recv()
    total = (far_part + res_pair_recv[0]).astype(BF16)
    for t in range(span // LANES):
        res_far[t] = total[:, t * LANES:(t + 1) * LANES]
    far_copies = []
    res_groups = pl.ds(0, early // LANES), pl.ds(early // LANES, late // LANES)
    for half, tiles in enumerate(res_groups):
        far_copies.append(copy_to(res_far.at[tiles], res_far_recv.at[tiles], gram_sem.at[half * 2], far))
    for copy in (far_copies[0], gram_copies[2], far_copies[1]):
        copy.start()
    for chunk in range(LATE, CHUNKS):
        far_gram(chunk)
        gram_copies[chunk].start()
    item_copies[1].wait_recv()
    copy_to(item16_peer.at[1], item16_peer.at[2], own_sem.at[0], pair).start()
    wait_all([mask32.at[pl.ds(2, 2), pl.ds(0, early)], rate.at[pl.ds(2, 2), pl.ds(0, early)]], in_sem.at[3])
    convert(2, 0, early)
    own_mask_copy = copy_to(mask16.at[2], mask16_peer.at[1], own_sem.at[0], pair)
    own_mask_copy.start()
    convert(3, 0, early)
    res_pair[1] = user_residual(2, pair_col)
    pair_copies[1].start()
    own_part = user_residual(3, col)
    wait_all([mask16_peer.at[1], item16_peer.at[2], mask16_direct, res_pair_recv.at[1]], own_sem.at[0])
    for chunk in range(CHUNKS):
        gram_own[:, chunk_rows(chunk)] = gram_part(3, chunk_rows(chunk))
    for lane in range(2):
        put_products(2 + lane, item16_peer[1 + lane])
        gram_own[:, :DIRECT] += gram_of(2 + lane, mask16_direct[lane])
    res_own[...] = own_part + res_pair_recv[1] - user_ridge * user0[:, block_rows(col)]

    wait_for(late_recv.at[0], late_sem.at[0])
    for slot in range(COLS):
        seen_rate = jnp.where(mask32[slot] > 0, rate[slot], 0.0)
        zrate[slot] = three_terms(seen_rate[:early])
        late_rated[row * COLS + order[slot]] = seen_rate[early:].astype(BF16)

    def item_sums(factors, seen, rated):
        pairs = stacked(pair_products(factors.astype(F32)))
        return dot_nn(pairs, seen), dot_nn(factors, rated)

    def item_part(entries):
        factors = side_by_side(fac[source, t] for source, _, chunk in entries for t in chunk_tiles(chunk))
        seen = stacked(mask16[slot, chunk_rows(chunk), :] for _, slot, chunk in entries)
        rated = stacked(zrate[slot, chunk_rows(chunk), :] for _, slot, chunk in entries)
        gram, rated_sum = item_sums(factors, seen, rated)
        return gram[:terms] + gram[terms:], sum((rated_sum[:, i * items:(i + 1) * items] for i in (1, 2)), rated_sum[:, :items])

    def add_part(entries, index):
        @pl.when(col < COLS)
        def _():
            early_sums[index, :terms], early_sums[index, terms:] = item_part(entries)

    def late_part(of_row, chunk):
        tiles = [t - early // LANES for t in chunk_tiles(chunk)]
        rows = pl.ds(STARTS[chunk] - early, WIDTHS[chunk])
        factors = side_by_side(late_fac[of_row * COLS + block, t] for block in range(COLS) for t in tiles)
        seen = stacked(late_seen[of_row * COLS + block, rows, :] for block in range(COLS))
        rated = stacked(late_rated[of_row * COLS + block, rows, :] for block in range(COLS))
        gram, rated_sum = item_sums(factors, seen, rated)
        index = chunk - LATE, lax.rem(of_row + row, 2)
        late_sums[index + (pl.ds(0, terms),)] = gram[:terms] + gram[terms:]
        late_sums[index + (pl.ds(terms, RANK),)] = rated_sum

    def split_late(slot):
        value = late_recv[order[slot]].astype(F32)
        seen = value < jnp.inf
        late_seen[(1 - row) * COLS + order[slot]] = seen.astype(F32).astype(BF16)
        late_rated[(1 - row) * COLS + order[slot]] = jnp.where(seen, value, 0.0).astype(BF16)

    groups = (range(0, early // LANES), range(early // LANES, span // LANES))

    def send_users(group):
        mine = user1.at[col, pl.ds(groups[group][0], len(groups[group]))]
        for lane, (device, _, _) in enumerate(peers[:2 + group]):
            sem = user_sem.at[1 if (group, lane) == (0, 1) else 0]
            copy_to(mine, mine, sem, device).start()

    def forward_users():
        theirs = user1.at[far_col, pl.ds(groups[0][0], len(groups[0]))]
        wait_for(theirs, user_sem.at[1])
        copy_to(theirs, theirs, user_sem.at[0], pair).start()

    def solve(chunk):
        lanes = chunk_rows(chunk)
        if chunk != 1:
            together = [gram_recv.at[pl.ds(sum(PACKED[:c]), PACKED[c])] for c in ((0, 1) if chunk == 0 else (chunk,))]
            if chunk in (0, LATE):
                together.append(res_far_recv.at[res_groups[chunk // LATE]])
            wait_all(together, gram_sem.at[max(chunk - 1, 0)])
        far_diags = unpack(chunk)
        diags = [gram_own[d * RANK:(d + 1) * RANK, lanes] + far_diags[d] for d in range(DIAGS)]
        start = user0[:, block_rows(col, STARTS[chunk], WIDTHS[chunk])]
        residual = res_own[:, lanes] + side_by_side(res_far_recv[t].astype(F32) for t in chunk_tiles(chunk))
        solved = cg_solve(diags, residual, start, user_ridge)
        return [solved[:, i * LANES:(i + 1) * LANES] for i in range(WIDTHS[chunk] // LANES)]

    fac_groups = pl.ds(0, STARTS[2] // LANES), pl.ds(STARTS[2] // LANES, WIDTHS[2] // LANES)

    def hand_on(group):
        theirs = fac.at[far_col, fac_groups[group]]
        copy = pltpu.make_async_remote_copy(
            src_ref=theirs, dst_ref=theirs, send_sem=send_sem.at[0], recv_sem=fac_sem.at[1 + group],
            device_id=pair, device_id_type=MESH,
        )
        pl.when(core == 0)(copy.start)

    def entries_of(lanes, chunks):
        return [(peers[lane][1], peers[lane][2], chunk) for chunk in chunks for lane in lanes]

    for chunk in range(LATE):
        pieces = solve(chunk)
        tiles = chunk_tiles(chunk)
        for t, piece in zip(tiles, pieces):
            fac[col, t] = piece.astype(BF16)
            user1[col, t] = piece
        if chunk:
            mine = fac.at[col, fac_groups[chunk - 1]]
            copy_to(mine, mine, fac_sem.at[chunk], far_chip[0]).start()
            copy = copy_to(mine, mine, fac_sem.at[chunk], far_chip[1])
            pl.when(core == 1)(copy.start)
            copy_to(mine, mine, fac_sem.at[0], pair).start()
    send_users(0)
    add_part([(col, 3, chunk) for chunk in range(LATE)], 0)
    wait_for(fac.at[0], fac_sem.at[0])
    add_part(entries_of((0,), range(LATE)), 1)
    for chunk in range(LATE, CHUNKS):
        pieces = solve(chunk)
        tiles = chunk_tiles(chunk)
        for t, piece in zip(tiles, pieces):
            late_fac[row * COLS + col, t - early // LANES] = piece.astype(BF16)
            user1[col, t] = piece
        mine = late_fac.at[row * COLS + col, pl.ds(tiles[0] - early // LANES, len(tiles))]
        for device, other_row in [(diag_chip[1], 1), (diag_chip[0], 1), (cross_chip[1], 1), (cross_chip[0], 1), (far_chip[1], 0), (far_chip[0], 0), (pair, 0)]:
            copy_to(mine, mine, late_fac_sem.at[(chunk - LATE) * 2 + other_row], device).start()
    send_users(1)
    wait_for(fac.at[pl.ds(0, 2), fac_groups[0]], fac_sem.at[1])
    hand_on(0)
    add_part(entries_of((1, 2), range(LATE - 1)), 2)
    wait_for(fac.at[pl.ds(0, 2), fac_groups[1]], fac_sem.at[2])
    hand_on(1)
    gram, residual = item_part(entries_of((1, 2), (LATE - 1,)))
    before = early_sums[0] + early_sums[1] + early_sums[2]
    gram = gram + before[:terms]
    start = item16[...].astype(F32)
    residual = residual + before[terms:] - apply_gram(diagonals(gram), start)
    high = residual.astype(BF16)
    item_send[:terms] = gram.astype(BF16)
    item_send[terms:terms + RANK] = high
    item_send[terms + RANK:] = (residual - high.astype(F32)).astype(BF16)
    cross_copy = copy_to(item_send, item_recv, cross_sem.at[0], cross)
    cross_copy.start()
    wait_for(late_recv.at[pl.ds(1, COLS - 1)], late_sem.at[1])
    for slot in range(COLS):
        split_late(slot)
    forward_users()

    def late_arrived(chunk, which):
        tiles = chunk_tiles(chunk)
        view = late_fac.at[pl.ds(0, COLS - 1 + which), pl.ds(tiles[0] - early // LANES, len(tiles))]
        wait_for(view, late_fac_sem.at[(chunk - LATE) * 2 + which])

    for which, of_row in enumerate((row, 1 - row)):
        for chunk in range(LATE, CHUNKS):
            late_arrived(chunk, which)
            pl.when(col < COLS)(functools.partial(late_part, of_row, chunk))
    late_total = sum((late_sums[chunk, 0] for chunk in range(1, CHUNKS - LATE)), late_sums[0, 0])
    late_total = late_total + sum((late_sums[chunk, 1] for chunk in range(1, CHUNKS - LATE)), late_sums[0, 1])
    late_gram = late_total[:terms]
    late_residual = late_total[terms:] - apply_gram(diagonals(late_gram), start)

    wait_all([user1.at[0, pl.ds(0, early // LANES)]] * 2 + [user1.at[0, pl.ds(0, late // LANES)]] * 3, user_sem.at[0])
    for source in range(COLS):
        for t in range(span // LANES):
            user_out[:, pl.ds(source * span + t * LANES, LANES)] = user1[source, t]

    cross_copy.wait_recv()
    full = item_send[...].astype(F32) + item_recv[...].astype(F32)
    residual = full[terms:terms + RANK] + full[terms + RANK:] + late_residual - item_ridge * item0[...]
    item_out[...] = cg_solve(diagonals(full[:terms] + late_gram), residual, item0[...], item_ridge)

    wait_all(sent, send_sem.at[0])


def write_kernel(user_ref, item_ref, user_out, item_out, sems):
    copies = [
        pltpu.make_async_copy(user_ref, user_out, sems.at[0]),
        pltpu.make_async_copy(item_ref, item_out, sems.at[1]),
    ]
    for copy in copies:
        copy.start()
    for copy in copies:
        copy.wait()


def solution(mesh):
    row_size = mesh.shape["row"]
    col_size = mesh.shape["col"]
    grid_spec = P(("part", "row"), "col")
    user_spec = P(("part", "row"), None)
    item_spec = P(("part", "col"), None)

    def local_step(ratings_blk, mask_blk, user_blk, item_blk):
        users, items = ratings_blk.shape
        span = users // COLS
        early = STARTS[LATE]
        late = span - early
        tiles = span // LANES
        hbm_spec = pl.BlockSpec(memory_space=pltpu.HBM)
        vmem = pltpu.VMEM
        dma = pltpu.SemaphoreType.DMA
        terms = DIAGS * RANK
        user_new, item_new = pl.pallas_call(
            functools.partial(sweep_kernel, RIDGE_WEIGHT * items * col_size, RIDGE_WEIGHT * users * row_size),
            out_shape=(
                pltpu.VMEM((RANK, users), F32),
                pltpu.VMEM((RANK, items), F32),
            ),
            in_specs=[hbm_spec] * 4,
            out_specs=(pl.BlockSpec(memory_space=pltpu.VMEM),) * 2,
            scratch_shapes=[
                vmem((COLS, span, items), F32),
                vmem((COLS, span, items), jnp.int32),
                vmem((RANK, users), F32),
                vmem((RANK, items), F32),
                vmem((COLS, span, items), BF16),
                vmem((2, span, items), BF16),
                vmem((2, DIRECT, items), BF16),
                vmem((RANK, items), BF16),
                vmem((3, RANK, items), BF16),
                vmem((COLS, terms, 2 * items), BF16),
                vmem((COLS, early, 3 * items), BF16),
                vmem((sum(PACKED), RANK, LANES), BF16),
                vmem((sum(PACKED), RANK, LANES), BF16),
                vmem((terms, span), F32),
                vmem((2, RANK, span), F32),
                vmem((2, RANK, span), F32),
                vmem((tiles, RANK, LANES), BF16),
                vmem((tiles, RANK, LANES), BF16),
                vmem((RANK, span), F32),
                vmem((COLS, early // LANES, RANK, LANES), BF16),
                vmem((COLS, tiles, RANK, LANES), F32),
                vmem((terms + 2 * RANK, items), BF16),
                vmem((terms + 2 * RANK, items), BF16),
                vmem((COLS, late, items), BF16),
                vmem((COLS, late, items), BF16),
                vmem((2 * COLS, late, items), BF16),
                vmem((2 * COLS, late, items), BF16),
                vmem((2 * COLS, late // LANES, RANK, LANES), BF16),
                vmem((CHUNKS - LATE, 2, terms + RANK, items), F32),
                vmem((3, terms + RANK, items), F32),
                dma((8,)),
                dma((1,)),
                dma((2,)),
                dma((1,)),
                dma((2,)),
                dma((1,)),
                dma((CHUNKS - 1,)),
                dma((3,)),
                dma((2,)),
                dma((1,)),
                dma((2,)),
                dma((2 * (CHUNKS - LATE),)),
            ],
            compiler_params=pltpu.CompilerParams(collective_id=0, has_side_effects=True, vmem_limit_bytes=60000 * 1024),
        )(ratings_blk, mask_blk, user_blk.T, item_blk.T)
        user_new, item_new = pl.pallas_call(
            write_kernel,
            out_shape=(
                jax.ShapeDtypeStruct((RANK, users), F32),
                jax.ShapeDtypeStruct((RANK, items), F32),
            ),
            in_specs=[pl.BlockSpec(memory_space=pltpu.VMEM)] * 2,
            out_specs=(hbm_spec, hbm_spec),
            scratch_shapes=[dma((2,))],
            compiler_params=pltpu.CompilerParams(vmem_limit_bytes=2**20),
        )(user_new, item_new)
        return user_new.T, item_new.T

    return jax.shard_map(local_step, mesh=mesh, in_specs=(grid_spec, grid_spec, user_spec, item_spec), out_specs=(user_spec, item_spec), check_vma=False)
```

```python
import functools
import math

import jax
import jax.numpy as jnp
from jax import lax
from jax.experimental import pallas as pl
from jax.experimental.pallas import tpu as pltpu
from jax.sharding import PartitionSpec as P

CG_STEPS = 4
RIDGE_WEIGHT = 0.0005
RANK = 16
DIAGS = RANK // 2 + 1
MESH = pl.DeviceIdType.MESH
F32 = jnp.float32
BF16 = jnp.bfloat16
COLS = 4
LANES = 128
HALF = RANK // 2
WIDTHS = (256, 256, 128, 256, 128)
STARTS = tuple(sum(WIDTHS[:i]) for i in range(len(WIDTHS)))
CHUNKS = len(WIDTHS)
LATE = 3
DIRECT = 128


def dot_nt(a, b):
    return lax.dot_general(a, b, (((1,), (1,)), ((), ())), preferred_element_type=F32)


def dot_nn(a, b):
    return lax.dot_general(a, b, (((1,), (0,)), ((), ())), preferred_element_type=F32)


def turn(x, shift):
    return x if shift % RANK == 0 else pltpu.roll(x, shift % RANK, 0)


def pair_products(fac):
    prods = jnp.concatenate([fac * turn(fac, -d) for d in range(DIAGS)], axis=0)
    high = prods.astype(BF16)
    low = (prods - high.astype(F32)).astype(BF16)
    return high, low


def apply_gram(diags, vec):
    parts = [diags[d] * turn(vec, -d) for d in range(DIAGS)]
    parts += [turn(diags[d] * vec, d) for d in range(1, RANK // 2)]
    while len(parts) > 1:
        parts = [sum(parts[i:i + 2][1:], parts[i]) for i in range(0, len(parts), 2)]
    return parts[0]


def cg_solve(diags, residual, start, ridge):
    direction = residual
    estimate = start
    res_sq = jnp.sum(residual * residual, axis=0, keepdims=True)
    for cg_step in range(CG_STEPS):
        gram_dir = apply_gram(diags, direction) + ridge * direction
        step_size = res_sq / jnp.sum(direction * gram_dir, axis=0, keepdims=True)
        estimate = estimate + step_size * direction
        if cg_step + 1 < CG_STEPS:
            residual = residual - step_size * gram_dir
            new_sq = jnp.sum(residual * residual, axis=0, keepdims=True)
            direction = residual + (new_sq / res_sq) * direction
            res_sq = new_sq
    return estimate


def far_span(chunk):
    skip = DIRECT if chunk == 0 else 0
    return STARTS[chunk] + skip, WIDTHS[chunk] - skip


def packed_tiles(chunk):
    tiles = far_span(chunk)[1] // LANES
    return HALF * tiles + (tiles + 1) // 2


PACKED = tuple(packed_tiles(chunk) for chunk in range(CHUNKS))


def chunk_tiles(chunk):
    return range(STARTS[chunk] // LANES, (STARTS[chunk] + WIDTHS[chunk]) // LANES)


def side_by_side(blocks):
    return jnp.concatenate(list(blocks), axis=1)


def stacked(blocks):
    return jnp.concatenate(list(blocks), axis=0)


def three_terms(values):
    high = values.astype(BF16)
    rest = values - high.astype(F32)
    middle = rest.astype(BF16)
    return side_by_side([high, middle, (rest - middle.astype(F32)).astype(BF16)])


def diagonals(full):
    return [full[d * RANK:(d + 1) * RANK] for d in range(DIAGS)]


def sweep_kernel(
    user_ridge, item_ridge,
    ratings_hbm, mask_hbm, user_hbm, item_hbm,
    user_out, item_out,
    rate, mask32, user0, item0,
    mask16, mask16_peer, mask16_direct, item16, item16_peer, ffs, zrate,
    gram_send, gram_recv, gram_own,
    res_pair, res_pair_recv, res_far, res_far_recv, res_own,
    fac, user1, item_send, item_recv,
    late_send, late_recv, late_seen, late_rated, late_fac, late_sums, early_sums,
    in_sem, send_sem, item_sem, own_sem, mask_sem, pair_sem, gram_sem, fac_sem, user_sem, cross_sem, late_sem, late_fac_sem,
):
    part = lax.axis_index("part")
    row = lax.axis_index("row")
    col = lax.axis_index("col")
    chip = col // 2
    core = col % 2
    pair_col = chip * 2 + (1 - core)
    far_col = (1 - chip) * 2 + core
    diag_col = (1 - chip) * 2 + (1 - core)
    pair = (part, row, pair_col)
    far = (part, row, far_col)
    diag = (part, row, diag_col)
    cross = (part, 1 - row, col)
    peers = ((pair, pair_col, 2), (far, far_col, 1), (diag, diag_col, 0))
    far_chip = [(part, row, (1 - chip) * 2 + k) for k in range(2)]
    cross_chip = [(part, 1 - row, chip * 2 + k) for k in range(2)]
    diag_chip = [(part, 1 - row, (1 - chip) * 2 + k) for k in range(2)]

    span = mask16.shape[1]
    items = item0.shape[1]
    terms = DIAGS * RANK
    early = STARTS[LATE]
    late = span - early

    sent = []

    def copy_to(src, dst, recv_sem, device):
        sent.append(src)
        return pltpu.make_async_remote_copy(
            src_ref=src, dst_ref=dst, send_sem=send_sem.at[0], recv_sem=recv_sem,
            device_id=device, device_id_type=MESH,
        )

    def wait_for(ref, sem):
        pltpu.make_async_copy(ref, ref, sem).wait()

    def wait_all(refs, sem):
        count = sum(math.prod(ref.shape) * ref.dtype.itemsize for ref in refs) // (items * rate.dtype.itemsize)
        parts = next(parts for parts in (1, 2, COLS) if count <= parts * span and count % parts == 0)
        wait_for(rate.at[pl.ds(0, parts), pl.ds(0, count // parts)], sem)

    barrier = pltpu.get_barrier_semaphore()
    for device in (pair, far, diag, cross):
        pl.semaphore_signal(barrier, inc=1, device_id=device, device_id_type=MESH)

    order = (diag_col, far_col, pair_col, col)

    def load(src, dst, slot):
        return pltpu.make_async_copy(src, dst, in_sem.at[slot])

    def block_rows(block, start=0, size=span):
        return pl.ds(pl.multiple_of(block * span + start, LANES), size)

    def chunk_rows(chunk):
        return pl.ds(STARTS[chunk], WIDTHS[chunk])

    item_load = load(item_hbm, item0, 0)
    user_load = load(user_hbm, user0, 4)
    rate_loads = []
    rate_late_loads = []
    mask_loads = []
    splits = (WIDTHS[0], WIDTHS[0], early, early)
    for slot, block in enumerate(order):
        rate_loads.append(load(ratings_hbm.at[block_rows(block, 0, early)], rate.at[slot, pl.ds(0, early)], 4 + slot // 2))
        rate_late_loads.append(load(ratings_hbm.at[block_rows(block, early, late)], rate.at[slot, pl.ds(early, late)], 2 + min(slot, 1)))
        pieces = []
        for half, (start, size) in enumerate(((0, splits[slot]), (splits[slot], span - splits[slot]))):
            src = mask_hbm.at[block_rows(block, start, size)]
            pieces.append(load(src, mask32.at[slot, pl.ds(start, size)], (4, 5, 5)[min(slot, 2)] if half == 0 else (1, 3)[slot // 2]))
        mask_loads.append(pieces)

    def convert(slot, start, size):
        rows = pl.ds(start, size)
        seen = mask32[slot, rows].astype(F32).astype(BF16)
        mask16[slot, rows] = seen
        if start + size == span:
            late_seen[row * COLS + order[slot]] = seen[early - start:]

    item_load.start()
    for pieces in mask_loads[:2]:
        for copy in pieces:
            copy.start()
    for slot in range(COLS):
        if slot >= 2:
            mask_loads[slot][1].start()
        rate_late_loads[slot].start()

    item_load.wait()
    item16[...] = item0[...].astype(BF16)
    pl.semaphore_wait(barrier, 4)
    item_copies = []
    for lane, (device, _, _) in enumerate(peers[:2]):
        item_copies.append(copy_to(item16, item16_peer.at[lane], item_sem.at[lane], device))
        item_copies[-1].start()
    first = pl.ds(0, DIRECT)

    def send_late(slot):
        rows = pl.ds(early, late)
        late_send[order[slot]] = jnp.where(mask32[slot, rows] > 0, rate[slot, rows], jnp.inf).astype(BF16)
        copy_to(late_send.at[order[slot]], late_recv.at[order[slot]], late_sem.at[min(slot, 1)], cross).start()

    def mask_copy(half):
        rows = pl.ds(*((splits[0], span - splits[0]) if half else (DIRECT, splits[0] - DIRECT)))
        return copy_to(mask16.at[0, rows], mask16_peer.at[0, rows], mask_sem.at[half], pair)

    mask_copies = [mask_copy(half) for half in range(2)]
    mask_loads[0][0].wait()
    convert(0, 0, splits[0])
    mask_copies[0].start()
    copy_to(mask16.at[0, first], mask16_direct.at[1], own_sem.at[0], diag).start()
    mask_loads[1][0].wait()
    convert(1, 0, splits[1])
    copy_to(mask16.at[1, first], mask16_direct.at[0], own_sem.at[0], far).start()
    rest = pl.ds(splits[0], span - splits[0])
    wait_for(mask32.at[pl.ds(0, 2), rest], in_sem.at[1])
    convert(0, splits[0], span - splits[0])
    mask_copies[1].start()
    user_load.start()
    for pieces in mask_loads[2:]:
        pieces[0].start()
    for copy in rate_loads:
        copy.start()
    rate_late_loads[0].wait()
    send_late(0)
    convert(1, splits[1], span - splits[1])
    wait_all([rate.at[pl.ds(1, COLS - 1), pl.ds(early, late)], mask32.at[pl.ds(2, 2), pl.ds(early, late)]], in_sem.at[3])
    send_late(1)
    for slot in (2, 3):
        convert(slot, early, late)
        send_late(slot)

    def put_products(index, factors):
        high, low = pair_products(factors.astype(F32))
        ffs[index, :, :items] = high
        ffs[index, :, items:] = low

    put_products(0, item16[...])
    item_copies[0].wait_recv()
    put_products(1, item16_peer[0])

    def gram_of(index, seen):
        return dot_nt(ffs[index], side_by_side([seen, seen]))

    def gram_part(slot, rows):
        return gram_of(0, mask16[slot, rows, :]) + gram_of(1, mask16_peer[slot // 2, rows, :])

    def pack(gram, chunk):
        tiles = gram.shape[1] // LANES
        base = sum(PACKED[:chunk])
        for d in range(HALF):
            for t in range(tiles):
                piece = gram[d * RANK:(d + 1) * RANK, t * LANES:(t + 1) * LANES]
                gram_send[base + d * tiles + t] = piece.astype(BF16)
        half = gram[HALF * RANK:HALF * RANK + HALF]
        for t in range(0, tiles, 2):
            both = [half[:, min(u, tiles - 1) * LANES:][:, :LANES] for u in (t, t + 1)]
            gram_send[base + HALF * tiles + t // 2] = stacked(both).astype(BF16)

    def unpack(chunk):
        gap = far_span(chunk)[1]
        tiles = gap // LANES
        base = sum(PACKED[:chunk])
        diags = [side_by_side(gram_recv[base + d * tiles + t].astype(F32) for t in range(tiles)) for d in range(HALF)]
        pieces = []
        for t in range(0, tiles, 2):
            both = gram_recv[base + HALF * tiles + t // 2].astype(F32)
            for half in (both[:HALF], both[HALF:])[:tiles - t]:
                pieces.append(stacked([half, half]))
        diags.append(side_by_side(pieces))
        pad = WIDTHS[chunk] - gap
        return [side_by_side([jnp.zeros((RANK, pad), F32), d]) if pad else d for d in diags]

    gram_copies = []
    for chunk in range(CHUNKS):
        part_of = pl.ds(sum(PACKED[:chunk]), PACKED[chunk])
        gram_copies.append(copy_to(gram_send.at[part_of], gram_recv.at[part_of], gram_sem.at[max(chunk - 1, 0)], far))

    def far_gram(chunk):
        if chunk < 2:
            mask_copies[chunk].wait_recv()
        pack(gram_part(1, pl.ds(*far_span(chunk))), chunk)

    for chunk in range(2):
        far_gram(chunk)
        gram_copies[chunk].start()

    def user_residual(slot, block):
        start = user0[:, block_rows(block)]
        scores = dot_nn(start.T.astype(BF16), item16[...])
        resid = jnp.where(mask32[slot] > 0, rate[slot] - scores, 0.0).astype(BF16)
        return dot_nt(item16[...], resid)

    wait_all([user0, rate.at[pl.ds(0, 2), pl.ds(0, early)]], in_sem.at[4])
    res_pair[0] = user_residual(0, diag_col)
    pair_copies = [copy_to(res_pair.at[slot], res_pair_recv.at[slot], (own_sem if slot else pair_sem).at[0], pair) for slot in range(2)]
    pair_copies[0].start()
    far_part = user_residual(1, far_col)
    far_gram(2)
    pair_copies[0].wait_recv()
    total = (far_part + res_pair_recv[0]).astype(BF16)
    for t in range(span // LANES):
        res_far[t] = total[:, t * LANES:(t + 1) * LANES]
    far_copies = []
    res_groups = pl.ds(0, early // LANES), pl.ds(early // LANES, late // LANES)
    for half, tiles in enumerate(res_groups):
        far_copies.append(copy_to(res_far.at[tiles], res_far_recv.at[tiles], gram_sem.at[half * 2], far))
    for copy in (far_copies[0], gram_copies[2], far_copies[1]):
        copy.start()
    for chunk in range(LATE, CHUNKS):
        far_gram(chunk)
        if chunk < CHUNKS - 1:
            gram_copies[chunk].start()
    pl.when(core == 0)(gram_copies[-1].start)
    item_copies[1].wait_recv()
    copy_to(item16_peer.at[1], item16_peer.at[2], own_sem.at[0], pair).start()
    wait_all([mask32.at[pl.ds(2, 2), pl.ds(0, early)], rate.at[pl.ds(2, 2), pl.ds(0, early)]], in_sem.at[5])
    convert(2, 0, early)
    own_mask_copy = copy_to(mask16.at[2], mask16_peer.at[1], own_sem.at[0], pair)
    own_mask_copy.start()
    convert(3, 0, early)
    res_pair[1] = user_residual(2, pair_col)
    pair_copies[1].start()
    own_part = user_residual(3, col)
    wait_all([mask16_peer.at[1], item16_peer.at[2], mask16_direct, res_pair_recv.at[1]], own_sem.at[0])
    for chunk in range(CHUNKS):
        gram_own[:, chunk_rows(chunk)] = gram_part(3, chunk_rows(chunk))
    for lane in range(2):
        put_products(2 + lane, item16_peer[1 + lane])
        gram_own[:, :DIRECT] += gram_of(2 + lane, mask16_direct[lane])
    res_own[...] = own_part + res_pair_recv[1] - user_ridge * user0[:, block_rows(col)]

    wait_for(late_recv.at[0], late_sem.at[0])
    for slot in range(COLS):
        seen_rate = jnp.where(mask32[slot] > 0, rate[slot], 0.0)
        zrate[slot] = three_terms(seen_rate[:early])
        late_rated[row * COLS + order[slot]] = seen_rate[early:].astype(BF16)

    def item_sums(factors, seen, rated):
        pairs = stacked(pair_products(factors.astype(F32)))
        return dot_nn(pairs, seen), dot_nn(factors, rated)

    def item_part(entries):
        factors = side_by_side(fac[source, t] for source, _, chunk in entries for t in chunk_tiles(chunk))
        seen = stacked(mask16[slot, chunk_rows(chunk), :] for _, slot, chunk in entries)
        rated = stacked(zrate[slot, chunk_rows(chunk), :] for _, slot, chunk in entries)
        gram, rated_sum = item_sums(factors, seen, rated)
        return gram[:terms] + gram[terms:], sum((rated_sum[:, i * items:(i + 1) * items] for i in (1, 2)), rated_sum[:, :items])

    def add_part(entries, index):
        @pl.when(col < COLS)
        def _():
            early_sums[index, :terms], early_sums[index, terms:] = item_part(entries)

    def late_part(of_row, chunk):
        tiles = [t - early // LANES for t in chunk_tiles(chunk)]
        rows = pl.ds(STARTS[chunk] - early, WIDTHS[chunk])
        factors = side_by_side(late_fac[of_row * COLS + block, t] for block in range(COLS) for t in tiles)
        seen = stacked(late_seen[of_row * COLS + block, rows, :] for block in range(COLS))
        rated = stacked(late_rated[of_row * COLS + block, rows, :] for block in range(COLS))
        gram, rated_sum = item_sums(factors, seen, rated)
        index = chunk - LATE, lax.rem(of_row + row, 2)
        late_sums[index + (pl.ds(0, terms),)] = gram[:terms] + gram[terms:]
        late_sums[index + (pl.ds(terms, RANK),)] = rated_sum

    def split_late(slot):
        value = late_recv[order[slot]].astype(F32)
        seen = value < jnp.inf
        late_seen[(1 - row) * COLS + order[slot]] = seen.astype(F32).astype(BF16)
        late_rated[(1 - row) * COLS + order[slot]] = jnp.where(seen, value, 0.0).astype(BF16)

    groups = (range(0, early // LANES), range(early // LANES, span // LANES))

    def send_users(group):
        mine = user1.at[col, pl.ds(groups[group][0], len(groups[group]))]
        for lane, (device, _, _) in enumerate(peers[:2 + group]):
            sem = user_sem.at[1 if (group, lane) == (0, 1) else 0]
            copy_to(mine, mine, sem, device).start()

    def forward_users():
        theirs = user1.at[far_col, pl.ds(groups[0][0], len(groups[0]))]
        wait_for(theirs, user_sem.at[1])
        copy_to(theirs, theirs, user_sem.at[0], pair).start()

    def solve(chunk):
        lanes = chunk_rows(chunk)
        if chunk != 1:
            together = [gram_recv.at[pl.ds(sum(PACKED[:c]), PACKED[c])] for c in ((0, 1) if chunk == 0 else (chunk,))]
            if chunk in (0, LATE):
                together.append(res_far_recv.at[res_groups[chunk // LATE]])
            wait_all(together, gram_sem.at[max(chunk - 1, 0)])
        far_diags = unpack(chunk)
        diags = [gram_own[d * RANK:(d + 1) * RANK, lanes] + far_diags[d] for d in range(DIAGS)]
        start = user0[:, block_rows(col, STARTS[chunk], WIDTHS[chunk])]
        residual = res_own[:, lanes] + side_by_side(res_far_recv[t].astype(F32) for t in chunk_tiles(chunk))
        solved = cg_solve(diags, residual, start, user_ridge)
        return [solved[:, i * LANES:(i + 1) * LANES] for i in range(WIDTHS[chunk] // LANES)]

    fac_groups = pl.ds(0, STARTS[2] // LANES), pl.ds(STARTS[2] // LANES, WIDTHS[2] // LANES)

    def hand_on(group):
        theirs = fac.at[far_col, fac_groups[group]]
        copy = pltpu.make_async_remote_copy(
            src_ref=theirs, dst_ref=theirs, send_sem=send_sem.at[0], recv_sem=fac_sem.at[1 + group],
            device_id=pair, device_id_type=MESH,
        )
        pl.when(core == 0)(copy.start)

    def entries_of(lanes, chunks):
        return [(peers[lane][1], peers[lane][2], chunk) for chunk in chunks for lane in lanes]

    for chunk in range(LATE):
        pieces = solve(chunk)
        tiles = chunk_tiles(chunk)
        for t, piece in zip(tiles, pieces):
            fac[col, t] = piece.astype(BF16)
            user1[col, t] = piece
        if chunk:
            mine = fac.at[col, fac_groups[chunk - 1]]
            copy_to(mine, mine, fac_sem.at[chunk], far_chip[0]).start()
            copy = copy_to(mine, mine, fac_sem.at[chunk], far_chip[1])
            pl.when(core == 1)(copy.start)
            copy_to(mine, mine, fac_sem.at[0], pair).start()
            if chunk == 1:
                pl.when(core == 1)(gram_copies[-1].start)
    send_users(0)
    add_part([(col, 3, chunk) for chunk in range(LATE)], 0)
    wait_for(fac.at[0], fac_sem.at[0])
    add_part(entries_of((0,), range(LATE)), 1)
    for chunk in range(LATE, CHUNKS):
        pieces = solve(chunk)
        tiles = chunk_tiles(chunk)
        for t, piece in zip(tiles, pieces):
            late_fac[row * COLS + col, t - early // LANES] = piece.astype(BF16)
            user1[col, t] = piece
        mine = late_fac.at[row * COLS + col, pl.ds(tiles[0] - early // LANES, len(tiles))]
        for device, other_row in [(far_chip[0], 0), (diag_chip[0], 1), (cross_chip[0], 1), (diag_chip[1], 1), (cross_chip[1], 1), (far_chip[1], 0), (pair, 0)]:
            copy_to(mine, mine, late_fac_sem.at[(chunk - LATE) * 2 + other_row], device).start()
    send_users(1)
    wait_for(fac.at[pl.ds(0, 2), fac_groups[0]], fac_sem.at[1])
    hand_on(0)
    add_part(entries_of((1, 2), range(LATE - 1)), 2)
    wait_for(fac.at[pl.ds(0, 2), fac_groups[1]], fac_sem.at[2])
    hand_on(1)
    gram, residual = item_part(entries_of((1, 2), (LATE - 1,)))
    before = early_sums[0] + early_sums[1] + early_sums[2]
    gram = gram + before[:terms]
    start = item16[...].astype(F32)
    residual = residual + before[terms:] - apply_gram(diagonals(gram), start)
    high = residual.astype(BF16)
    item_send[:terms] = gram.astype(BF16)
    item_send[terms:terms + RANK] = high
    item_send[terms + RANK:] = (residual - high.astype(F32)).astype(BF16)
    cross_copy = copy_to(item_send, item_recv, cross_sem.at[0], cross)
    cross_copy.start()
    wait_for(late_recv.at[pl.ds(1, COLS - 1)], late_sem.at[1])
    for slot in range(COLS):
        split_late(slot)
    forward_users()

    def late_arrived(chunk, which):
        tiles = chunk_tiles(chunk)
        view = late_fac.at[pl.ds(0, COLS - 1 + which), pl.ds(tiles[0] - early // LANES, len(tiles))]
        wait_for(view, late_fac_sem.at[(chunk - LATE) * 2 + which])

    for which, of_row in enumerate((row, 1 - row)):
        for chunk in range(LATE, CHUNKS):
            late_arrived(chunk, which)
            pl.when(col < COLS)(functools.partial(late_part, of_row, chunk))
    late_total = sum((late_sums[chunk, 0] for chunk in range(1, CHUNKS - LATE)), late_sums[0, 0])
    late_total = late_total + sum((late_sums[chunk, 1] for chunk in range(1, CHUNKS - LATE)), late_sums[0, 1])
    late_gram = late_total[:terms]
    late_residual = late_total[terms:] - apply_gram(diagonals(late_gram), start)

    wait_all([user1.at[0, pl.ds(0, early // LANES)]] * 2 + [user1.at[0, pl.ds(0, late // LANES)]] * 3, user_sem.at[0])
    for source in range(COLS):
        for t in range(span // LANES):
            user_out[:, pl.ds(source * span + t * LANES, LANES)] = user1[source, t]

    cross_copy.wait_recv()
    full = item_send[...].astype(F32) + item_recv[...].astype(F32)
    residual = full[terms:terms + RANK] + full[terms + RANK:] + late_residual - item_ridge * item0[...]
    item_out[...] = cg_solve(diagonals(full[:terms] + late_gram), residual, item0[...], item_ridge)

    wait_all(sent, send_sem.at[0])


def write_kernel(user_ref, item_ref, user_out, item_out, sems):
    copies = [
        pltpu.make_async_copy(user_ref, user_out, sems.at[0]),
        pltpu.make_async_copy(item_ref, item_out, sems.at[1]),
    ]
    for copy in copies:
        copy.start()
    for copy in copies:
        copy.wait()


def solution(mesh):
    row_size = mesh.shape["row"]
    col_size = mesh.shape["col"]
    grid_spec = P(("part", "row"), "col")
    user_spec = P(("part", "row"), None)
    item_spec = P(("part", "col"), None)

    def local_step(ratings_blk, mask_blk, user_blk, item_blk):
        users, items = ratings_blk.shape
        span = users // COLS
        early = STARTS[LATE]
        late = span - early
        tiles = span // LANES
        hbm_spec = pl.BlockSpec(memory_space=pltpu.HBM)
        vmem = pltpu.VMEM
        dma = pltpu.SemaphoreType.DMA
        terms = DIAGS * RANK
        user_new, item_new = pl.pallas_call(
            functools.partial(sweep_kernel, RIDGE_WEIGHT * items * col_size, RIDGE_WEIGHT * users * row_size),
            out_shape=(
                pltpu.VMEM((RANK, users), F32),
                pltpu.VMEM((RANK, items), F32),
            ),
            in_specs=[hbm_spec] * 4,
            out_specs=(pl.BlockSpec(memory_space=pltpu.VMEM),) * 2,
            scratch_shapes=[
                vmem((COLS, span, items), F32),
                vmem((COLS, span, items), jnp.int32),
                vmem((RANK, users), F32),
                vmem((RANK, items), F32),
                vmem((COLS, span, items), BF16),
                vmem((2, span, items), BF16),
                vmem((2, DIRECT, items), BF16),
                vmem((RANK, items), BF16),
                vmem((3, RANK, items), BF16),
                vmem((COLS, terms, 2 * items), BF16),
                vmem((COLS, early, 3 * items), BF16),
                vmem((sum(PACKED), RANK, LANES), BF16),
                vmem((sum(PACKED), RANK, LANES), BF16),
                vmem((terms, span), F32),
                vmem((2, RANK, span), F32),
                vmem((2, RANK, span), F32),
                vmem((tiles, RANK, LANES), BF16),
                vmem((tiles, RANK, LANES), BF16),
                vmem((RANK, span), F32),
                vmem((COLS, early // LANES, RANK, LANES), BF16),
                vmem((COLS, tiles, RANK, LANES), F32),
                vmem((terms + 2 * RANK, items), BF16),
                vmem((terms + 2 * RANK, items), BF16),
                vmem((COLS, late, items), BF16),
                vmem((COLS, late, items), BF16),
                vmem((2 * COLS, late, items), BF16),
                vmem((2 * COLS, late, items), BF16),
                vmem((2 * COLS, late // LANES, RANK, LANES), BF16),
                vmem((CHUNKS - LATE, 2, terms + RANK, items), F32),
                vmem((3, terms + RANK, items), F32),
                dma((6,)),
                dma((1,)),
                dma((2,)),
                dma((1,)),
                dma((2,)),
                dma((1,)),
                dma((CHUNKS - 1,)),
                dma((3,)),
                dma((2,)),
                dma((1,)),
                dma((2,)),
                dma((2 * (CHUNKS - LATE),)),
            ],
            compiler_params=pltpu.CompilerParams(collective_id=0, has_side_effects=True, vmem_limit_bytes=60000 * 1024),
        )(ratings_blk, mask_blk, user_blk.T, item_blk.T)
        user_new, item_new = pl.pallas_call(
            write_kernel,
            out_shape=(
                jax.ShapeDtypeStruct((RANK, users), F32),
                jax.ShapeDtypeStruct((RANK, items), F32),
            ),
            in_specs=[pl.BlockSpec(memory_space=pltpu.VMEM)] * 2,
            out_specs=(hbm_spec, hbm_spec),
            scratch_shapes=[dma((2,))],
            compiler_params=pltpu.CompilerParams(vmem_limit_bytes=2**20),
        )(user_new, item_new)
        return user_new.T, item_new.T

    return jax.shard_map(local_step, mesh=mesh, in_specs=(grid_spec, grid_spec, user_spec, item_spec), out_specs=(user_spec, item_spec), check_vma=False)
```

```python
import functools
import math

import jax
import jax.numpy as jnp
from jax import lax
from jax.experimental import pallas as pl
from jax.experimental.pallas import tpu as pltpu
from jax.sharding import PartitionSpec as P

CG_STEPS = 4
RIDGE_WEIGHT = 0.0005
RANK = 16
DIAGS = RANK // 2 + 1
MESH = pl.DeviceIdType.MESH
F32 = jnp.float32
BF16 = jnp.bfloat16
COLS = 4
LANES = 128
HALF = RANK // 2
WIDTHS = (256, 256, 128, 256, 128)
STARTS = tuple(sum(WIDTHS[:i]) for i in range(len(WIDTHS)))
CHUNKS = len(WIDTHS)
LATE = 3
DIRECT = 128


def dot_nt(a, b):
    return lax.dot_general(a, b, (((1,), (1,)), ((), ())), preferred_element_type=F32)


def dot_nn(a, b):
    return lax.dot_general(a, b, (((1,), (0,)), ((), ())), preferred_element_type=F32)


def turn(x, shift):
    return x if shift % RANK == 0 else pltpu.roll(x, shift % RANK, 0)


def pair_products(fac):
    prods = jnp.concatenate([fac * turn(fac, -d) for d in range(DIAGS)], axis=0)
    high = prods.astype(BF16)
    low = (prods - high.astype(F32)).astype(BF16)
    return high, low


def apply_gram(diags, vec):
    parts = [diags[d] * turn(vec, -d) for d in range(DIAGS)]
    parts += [turn(diags[d] * vec, d) for d in range(1, RANK // 2)]
    while len(parts) > 1:
        parts = [sum(parts[i:i + 2][1:], parts[i]) for i in range(0, len(parts), 2)]
    return parts[0]


def cg_solve(diags, residual, start, ridge):
    direction = residual
    estimate = start
    res_sq = jnp.sum(residual * residual, axis=0, keepdims=True)
    for cg_step in range(CG_STEPS):
        gram_dir = apply_gram(diags, direction) + ridge * direction
        step_size = res_sq / jnp.sum(direction * gram_dir, axis=0, keepdims=True)
        estimate = estimate + step_size * direction
        if cg_step + 1 < CG_STEPS:
            residual = residual - step_size * gram_dir
            new_sq = jnp.sum(residual * residual, axis=0, keepdims=True)
            direction = residual + (new_sq / res_sq) * direction
            res_sq = new_sq
    return estimate


def far_span(chunk):
    skip = DIRECT if chunk == 0 else 0
    return STARTS[chunk] + skip, WIDTHS[chunk] - skip


def packed_tiles(chunk):
    tiles = far_span(chunk)[1] // LANES
    return HALF * tiles + (tiles + 1) // 2


PACKED = tuple(packed_tiles(chunk) for chunk in range(CHUNKS))


def chunk_tiles(chunk):
    return range(STARTS[chunk] // LANES, (STARTS[chunk] + WIDTHS[chunk]) // LANES)


def side_by_side(blocks):
    return jnp.concatenate(list(blocks), axis=1)


def stacked(blocks):
    return jnp.concatenate(list(blocks), axis=0)


def three_terms(values):
    high = values.astype(BF16)
    rest = values - high.astype(F32)
    middle = rest.astype(BF16)
    return side_by_side([high, middle, (rest - middle.astype(F32)).astype(BF16)])


def diagonals(full):
    return [full[d * RANK:(d + 1) * RANK] for d in range(DIAGS)]


def sweep_kernel(
    user_ridge, item_ridge,
    ratings_hbm, mask_hbm, user_hbm, item_hbm,
    user_out, item_out,
    rate, mask32, user0, item0,
    mask16, mask16_peer, mask16_direct, item16, item16_peer, ffs, zrate,
    gram_send, gram_recv, gram_own,
    res_pair, res_pair_recv, res_far, res_far_recv, res_own,
    fac, user1, item_send, item_recv,
    late_send, late_recv, late_seen, late_rated, late_fac, late_sums, early_sums,
    in_sem, send_sem, item_sem, own_sem, mask_sem, pair_sem, gram_sem, fac_sem, user_sem, cross_sem, late_sem, late_fac_sem,
):
    part = lax.axis_index("part")
    row = lax.axis_index("row")
    col = lax.axis_index("col")
    chip = col // 2
    core = col % 2
    pair_col = chip * 2 + (1 - core)
    far_col = (1 - chip) * 2 + core
    diag_col = (1 - chip) * 2 + (1 - core)
    pair = (part, row, pair_col)
    far = (part, row, far_col)
    diag = (part, row, diag_col)
    cross = (part, 1 - row, col)
    peers = ((pair, pair_col, 2), (far, far_col, 1), (diag, diag_col, 0))
    far_chip = [(part, row, (1 - chip) * 2 + k) for k in range(2)]
    cross_chip = [(part, 1 - row, chip * 2 + k) for k in range(2)]
    diag_chip = [(part, 1 - row, (1 - chip) * 2 + k) for k in range(2)]

    span = mask16.shape[1]
    items = item0.shape[1]
    terms = DIAGS * RANK
    early = STARTS[LATE]
    late = span - early

    sent = []

    def copy_to(src, dst, recv_sem, device):
        sent.append(src)
        return pltpu.make_async_remote_copy(
            src_ref=src, dst_ref=dst, send_sem=send_sem.at[0], recv_sem=recv_sem,
            device_id=device, device_id_type=MESH,
        )

    def wait_for(ref, sem):
        pltpu.make_async_copy(ref, ref, sem).wait()

    def wait_all(refs, sem):
        count = sum(math.prod(ref.shape) * ref.dtype.itemsize for ref in refs) // (items * rate.dtype.itemsize)
        parts = next(parts for parts in (1, 2, COLS) if count <= parts * span and count % parts == 0)
        wait_for(rate.at[pl.ds(0, parts), pl.ds(0, count // parts)], sem)

    barrier = pltpu.get_barrier_semaphore()
    for device in (pair, far, diag, cross):
        pl.semaphore_signal(barrier, inc=1, device_id=device, device_id_type=MESH)

    order = (diag_col, far_col, pair_col, col)

    def load(src, dst, slot):
        return pltpu.make_async_copy(src, dst, in_sem.at[slot])

    def block_rows(block, start=0, size=span):
        return pl.ds(pl.multiple_of(block * span + start, LANES), size)

    def chunk_rows(chunk):
        return pl.ds(STARTS[chunk], WIDTHS[chunk])

    item_load = load(item_hbm, item0, 0)
    user_load = load(user_hbm, user0, 4)
    rate_loads = []
    rate_late_loads = []
    mask_loads = []
    splits = (WIDTHS[0], WIDTHS[0], early, early)
    for slot, block in enumerate(order):
        rate_loads.append(load(ratings_hbm.at[block_rows(block, 0, early)], rate.at[slot, pl.ds(0, early)], 4 + slot // 2))
        rate_late_loads.append(load(ratings_hbm.at[block_rows(block, early, late)], rate.at[slot, pl.ds(early, late)], 2 + min(slot, 1)))
        pieces = []
        for half, (start, size) in enumerate(((0, splits[slot]), (splits[slot], span - splits[slot]))):
            src = mask_hbm.at[block_rows(block, start, size)]
            pieces.append(load(src, mask32.at[slot, pl.ds(start, size)], (4, 5, 5)[min(slot, 2)] if half == 0 else (1, 3)[slot // 2]))
        mask_loads.append(pieces)

    def convert(slot, start, size):
        rows = pl.ds(start, size)
        seen = mask32[slot, rows].astype(F32).astype(BF16)
        mask16[slot, rows] = seen
        if start + size == span:
            late_seen[row * COLS + order[slot]] = seen[early - start:]

    item_load.start()
    for pieces in mask_loads[:2]:
        for copy in pieces:
            copy.start()
    for slot in range(COLS):
        if slot >= 2:
            mask_loads[slot][1].start()
        rate_late_loads[slot].start()

    item_load.wait()
    item16[...] = item0[...].astype(BF16)
    pl.semaphore_wait(barrier, 4)
    item_copies = []
    for lane, (device, _, _) in enumerate(peers[:2]):
        item_copies.append(copy_to(item16, item16_peer.at[lane], item_sem.at[lane], device))
        item_copies[-1].start()
    first = pl.ds(0, DIRECT)

    def send_late(slot):
        rows = pl.ds(early, late)
        late_send[order[slot]] = jnp.where(mask32[slot, rows] > 0, rate[slot, rows], jnp.inf).astype(BF16)
        copy_to(late_send.at[order[slot]], late_recv.at[order[slot]], late_sem.at[min(slot, 1)], cross).start()

    def mask_copy(half):
        rows = pl.ds(*((splits[0], span - splits[0]) if half else (DIRECT, splits[0] - DIRECT)))
        return copy_to(mask16.at[0, rows], mask16_peer.at[0, rows], mask_sem.at[half], pair)

    mask_copies = [mask_copy(half) for half in range(2)]
    mask_loads[0][0].wait()
    convert(0, 0, splits[0])
    mask_copies[0].start()
    copy_to(mask16.at[0, first], mask16_direct.at[1], own_sem.at[0], diag).start()
    mask_loads[1][0].wait()
    convert(1, 0, splits[1])
    copy_to(mask16.at[1, first], mask16_direct.at[0], own_sem.at[0], far).start()
    rest = pl.ds(splits[0], span - splits[0])
    wait_for(mask32.at[pl.ds(0, 2), rest], in_sem.at[1])
    convert(0, splits[0], span - splits[0])
    mask_copies[1].start()
    user_load.start()
    for pieces in mask_loads[2:]:
        pieces[0].start()
    for copy in rate_loads:
        copy.start()
    rate_late_loads[0].wait()
    send_late(0)
    convert(1, splits[1], span - splits[1])
    wait_all([rate.at[pl.ds(1, COLS - 1), pl.ds(early, late)], mask32.at[pl.ds(2, 2), pl.ds(early, late)]], in_sem.at[3])
    send_late(1)
    for slot in (2, 3):
        convert(slot, early, late)
        send_late(slot)

    def put_products(index, factors):
        high, low = pair_products(factors.astype(F32))
        ffs[index, :, :items] = high
        ffs[index, :, items:] = low

    put_products(0, item16[...])
    item_copies[0].wait_recv()
    put_products(1, item16_peer[0])

    def gram_of(index, seen):
        return dot_nt(ffs[index], side_by_side([seen, seen]))

    def gram_part(slot, rows):
        return gram_of(0, mask16[slot, rows, :]) + gram_of(1, mask16_peer[slot // 2, rows, :])

    def pack(gram, chunk):
        tiles = gram.shape[1] // LANES
        base = sum(PACKED[:chunk])
        for d in range(HALF):
            for t in range(tiles):
                piece = gram[d * RANK:(d + 1) * RANK, t * LANES:(t + 1) * LANES]
                gram_send[base + d * tiles + t] = piece.astype(BF16)
        half = gram[HALF * RANK:HALF * RANK + HALF]
        for t in range(0, tiles, 2):
            both = [half[:, min(u, tiles - 1) * LANES:][:, :LANES] for u in (t, t + 1)]
            gram_send[base + HALF * tiles + t // 2] = stacked(both).astype(BF16)

    def unpack(chunk):
        gap = far_span(chunk)[1]
        tiles = gap // LANES
        base = sum(PACKED[:chunk])
        diags = [side_by_side(gram_recv[base + d * tiles + t].astype(F32) for t in range(tiles)) for d in range(HALF)]
        pieces = []
        for t in range(0, tiles, 2):
            both = gram_recv[base + HALF * tiles + t // 2].astype(F32)
            for half in (both[:HALF], both[HALF:])[:tiles - t]:
                pieces.append(stacked([half, half]))
        diags.append(side_by_side(pieces))
        pad = WIDTHS[chunk] - gap
        return [side_by_side([jnp.zeros((RANK, pad), F32), d]) if pad else d for d in diags]

    gram_copies = []
    for chunk in range(CHUNKS):
        part_of = pl.ds(sum(PACKED[:chunk]), PACKED[chunk])
        gram_copies.append(copy_to(gram_send.at[part_of], gram_recv.at[part_of], gram_sem.at[max(chunk - 1, 0)], far))

    def far_gram(chunk):
        if chunk < 2:
            mask_copies[chunk].wait_recv()
        pack(gram_part(1, pl.ds(*far_span(chunk))), chunk)

    for chunk in range(2):
        far_gram(chunk)
        gram_copies[chunk].start()

    def user_residual(slot, block):
        start = user0[:, block_rows(block)]
        scores = dot_nn(start.T.astype(BF16), item16[...])
        resid = jnp.where(mask32[slot] > 0, rate[slot] - scores, 0.0).astype(BF16)
        return dot_nt(item16[...], resid)

    wait_all([user0, rate.at[pl.ds(0, 2), pl.ds(0, early)]], in_sem.at[4])
    res_pair[0] = user_residual(0, diag_col)
    pair_copies = [copy_to(res_pair.at[slot], res_pair_recv.at[slot], (own_sem if slot else pair_sem).at[0], pair) for slot in range(2)]
    pair_copies[0].start()
    far_part = user_residual(1, far_col)
    far_gram(2)
    pair_copies[0].wait_recv()
    total = (far_part + res_pair_recv[0]).astype(BF16)
    for t in range(span // LANES):
        res_far[t] = total[:, t * LANES:(t + 1) * LANES]
    far_copies = []
    res_groups = pl.ds(0, early // LANES), pl.ds(early // LANES, late // LANES)
    for half, tiles in enumerate(res_groups):
        far_copies.append(copy_to(res_far.at[tiles], res_far_recv.at[tiles], gram_sem.at[half * 2], far))
    for copy in (far_copies[0], gram_copies[2], far_copies[1]):
        copy.start()
    for chunk in range(LATE, CHUNKS):
        far_gram(chunk)
        if chunk < CHUNKS - 1:
            gram_copies[chunk].start()
    pl.when(core == 0)(gram_copies[-1].start)
    item_copies[1].wait_recv()
    copy_to(item16_peer.at[1], item16_peer.at[2], own_sem.at[0], pair).start()
    wait_all([mask32.at[pl.ds(2, 2), pl.ds(0, early)], rate.at[pl.ds(2, 2), pl.ds(0, early)]], in_sem.at[5])
    convert(2, 0, early)
    own_mask_copy = copy_to(mask16.at[2], mask16_peer.at[1], own_sem.at[0], pair)
    own_mask_copy.start()
    convert(3, 0, early)
    res_pair[1] = user_residual(2, pair_col)
    pair_copies[1].start()
    own_part = user_residual(3, col)
    wait_all([mask16_peer.at[1], item16_peer.at[2], mask16_direct, res_pair_recv.at[1]], own_sem.at[0])
    for chunk in range(CHUNKS):
        gram_own[:, chunk_rows(chunk)] = gram_part(3, chunk_rows(chunk))
    for lane in range(2):
        put_products(2 + lane, item16_peer[1 + lane])
        gram_own[:, :DIRECT] += gram_of(2 + lane, mask16_direct[lane])
    res_own[...] = own_part + res_pair_recv[1] - user_ridge * user0[:, block_rows(col)]

    wait_for(late_recv.at[0], late_sem.at[0])
    for slot in range(COLS):
        seen_rate = jnp.where(mask32[slot] > 0, rate[slot], 0.0)
        zrate[slot] = three_terms(seen_rate[:early])
        late_rated[row * COLS + order[slot]] = seen_rate[early:].astype(BF16)

    def item_sums(factors, seen, rated):
        pairs = stacked(pair_products(factors.astype(F32)))
        return dot_nn(pairs, seen), dot_nn(factors, rated)

    def item_part(entries):
        factors = side_by_side(fac[source, t] for source, _, chunk in entries for t in chunk_tiles(chunk))
        seen = stacked(mask16[slot, chunk_rows(chunk), :] for _, slot, chunk in entries)
        rated = stacked(zrate[slot, chunk_rows(chunk), :] for _, slot, chunk in entries)
        gram, rated_sum = item_sums(factors, seen, rated)
        return gram[:terms] + gram[terms:], sum((rated_sum[:, i * items:(i + 1) * items] for i in (1, 2)), rated_sum[:, :items])

    def add_part(entries, index):
        @pl.when(col < COLS)
        def _():
            early_sums[index, :terms], early_sums[index, terms:] = item_part(entries)

    def late_part(of_row, chunk):
        tiles = [t - early // LANES for t in chunk_tiles(chunk)]
        rows = pl.ds(STARTS[chunk] - early, WIDTHS[chunk])
        factors = side_by_side(late_fac[of_row * COLS + block, t] for block in range(COLS) for t in tiles)
        seen = stacked(late_seen[of_row * COLS + block, rows, :] for block in range(COLS))
        rated = stacked(late_rated[of_row * COLS + block, rows, :] for block in range(COLS))
        gram, rated_sum = item_sums(factors, seen, rated)
        index = chunk - LATE, lax.rem(of_row + row, 2)
        late_sums[index + (pl.ds(0, terms),)] = gram[:terms] + gram[terms:]
        late_sums[index + (pl.ds(terms, RANK),)] = rated_sum

    def split_late(slot):
        value = late_recv[order[slot]].astype(F32)
        seen = value < jnp.inf
        late_seen[(1 - row) * COLS + order[slot]] = seen.astype(F32).astype(BF16)
        late_rated[(1 - row) * COLS + order[slot]] = jnp.where(seen, value, 0.0).astype(BF16)

    groups = (range(0, early // LANES), range(early // LANES, span // LANES))

    def send_users(group):
        mine = user1.at[col, pl.ds(groups[group][0], len(groups[group]))]
        for lane, (device, _, _) in enumerate(peers[:2 + group]):
            sem = user_sem.at[1 if (group, lane) == (0, 1) else 0]
            copy_to(mine, mine, sem, device).start()

    def forward_users():
        theirs = user1.at[far_col, pl.ds(groups[0][0], len(groups[0]))]
        wait_for(theirs, user_sem.at[1])
        copy_to(theirs, theirs, user_sem.at[0], pair).start()

    def solve(chunk):
        lanes = chunk_rows(chunk)
        if chunk != 1:
            together = [gram_recv.at[pl.ds(sum(PACKED[:c]), PACKED[c])] for c in ((0, 1) if chunk == 0 else (chunk,))]
            if chunk in (0, LATE):
                together.append(res_far_recv.at[res_groups[chunk // LATE]])
            wait_all(together, gram_sem.at[max(chunk - 1, 0)])
        far_diags = unpack(chunk)
        diags = [gram_own[d * RANK:(d + 1) * RANK, lanes] + far_diags[d] for d in range(DIAGS)]
        start = user0[:, block_rows(col, STARTS[chunk], WIDTHS[chunk])]
        residual = res_own[:, lanes] + side_by_side(res_far_recv[t].astype(F32) for t in chunk_tiles(chunk))
        solved = cg_solve(diags, residual, start, user_ridge)
        return [solved[:, i * LANES:(i + 1) * LANES] for i in range(WIDTHS[chunk] // LANES)]

    fac_groups = pl.ds(0, STARTS[2] // LANES), pl.ds(STARTS[2] // LANES, WIDTHS[2] // LANES)

    def hand_on(group):
        theirs = fac.at[far_col, fac_groups[group]]
        copy = pltpu.make_async_remote_copy(
            src_ref=theirs, dst_ref=theirs, send_sem=send_sem.at[0], recv_sem=fac_sem.at[1 + group],
            device_id=pair, device_id_type=MESH,
        )
        pl.when(core == 0)(copy.start)

    def entries_of(lanes, chunks):
        return [(peers[lane][1], peers[lane][2], chunk) for chunk in chunks for lane in lanes]

    for chunk in range(LATE):
        pieces = solve(chunk)
        tiles = chunk_tiles(chunk)
        for t, piece in zip(tiles, pieces):
            fac[col, t] = piece.astype(BF16)
            user1[col, t] = piece
        if chunk:
            mine = fac.at[col, fac_groups[chunk - 1]]
            copy_to(mine, mine, fac_sem.at[chunk], far_chip[0]).start()
            copy = copy_to(mine, mine, fac_sem.at[chunk], far_chip[1])
            pl.when(core == 1)(copy.start)
            copy_to(mine, mine, fac_sem.at[0], pair).start()
            if chunk == 1:
                pl.when(core == 1)(gram_copies[-1].start)
    send_users(0)
    add_part([(col, 3, chunk) for chunk in range(LATE)], 0)
    wait_for(fac.at[0], fac_sem.at[0])
    add_part(entries_of((0,), range(LATE)), 1)
    for chunk in range(LATE, CHUNKS):
        pieces = solve(chunk)
        tiles = chunk_tiles(chunk)
        for t, piece in zip(tiles, pieces):
            late_fac[row * COLS + col, t - early // LANES] = piece.astype(BF16)
            user1[col, t] = piece
        mine = late_fac.at[row * COLS + col, pl.ds(tiles[0] - early // LANES, len(tiles))]
        for device, other_row in [(far_chip[0], 0), (diag_chip[0], 1), (cross_chip[0], 1), (diag_chip[1], 1), (cross_chip[1], 1), (far_chip[1], 0), (pair, 0)]:
            copy_to(mine, mine, late_fac_sem.at[(chunk - LATE) * 2 + other_row], device).start()
    send_users(1)
    wait_for(fac.at[pl.ds(0, 2), fac_groups[0]], fac_sem.at[1])
    hand_on(0)
    add_part(entries_of((1, 2), range(LATE - 1)), 2)
    wait_for(fac.at[pl.ds(0, 2), fac_groups[1]], fac_sem.at[2])
    hand_on(1)
    gram, residual = item_part(entries_of((1, 2), (LATE - 1,)))
    before = early_sums[0] + early_sums[1] + early_sums[2]
    gram = gram + before[:terms]
    start = item16[...].astype(F32)
    residual = residual + before[terms:] - apply_gram(diagonals(gram), start)
    high = residual.astype(BF16)
    item_send[:terms] = gram.astype(BF16)
    item_send[terms:terms + RANK] = high
    item_send[terms + RANK:] = (residual - high.astype(F32)).astype(BF16)
    cross_copy = copy_to(item_send, item_recv, cross_sem.at[0], cross)
    cross_copy.start()
    wait_for(late_recv.at[pl.ds(1, COLS - 1)], late_sem.at[1])
    for slot in range(COLS):
        split_late(slot)
    forward_users()

    def late_arrived(chunk, which):
        tiles = chunk_tiles(chunk)
        view = late_fac.at[pl.ds(0, COLS - 1 + which), pl.ds(tiles[0] - early // LANES, len(tiles))]
        wait_for(view, late_fac_sem.at[(chunk - LATE) * 2 + which])

    for which, of_row in enumerate((row, 1 - row)):
        for chunk in range(LATE, CHUNKS):
            late_arrived(chunk, which)
            pl.when(col < COLS)(functools.partial(late_part, of_row, chunk))
    late_total = sum((late_sums[chunk, 0] for chunk in range(1, CHUNKS - LATE)), late_sums[0, 0])
    late_total = late_total + sum((late_sums[chunk, 1] for chunk in range(1, CHUNKS - LATE)), late_sums[0, 1])
    late_gram = late_total[:terms]
    late_residual = late_total[terms:] - apply_gram(diagonals(late_gram), start)

    wait_all([user1.at[0, pl.ds(0, early // LANES)]] * 2 + [user1.at[0, pl.ds(0, late // LANES)]] * 3, user_sem.at[0])
    for source in range(COLS):
        for t in range(span // LANES):
            user_out[:, pl.ds(source * span + t * LANES, LANES)] = user1[source, t]

    cross_copy.wait_recv()
    full = item_send[...].astype(F32) + item_recv[...].astype(F32)
    residual = full[terms:terms + RANK] + full[terms + RANK:] + late_residual - item_ridge * item0[...]
    item_out[...] = cg_solve(diagonals(full[:terms] + late_gram), residual, item0[...], item_ridge)

    wait_all(sent, send_sem.at[0])


def write_kernel(user_ref, item_ref, user_out, item_out, sems):
    pltpu.make_async_copy(item_ref, item_out, sems.at[1]).start()
    for half in range(2):
        for piece in range(4):
            lanes = user_ref.shape[1] // 4
            part = pl.ds(half * RANK // 2, RANK // 2), pl.ds(piece * lanes, lanes)
            pltpu.make_async_copy(user_ref.at[part], user_out.at[part], sems.at[0]).start()
    pltpu.make_async_copy(user_ref, user_out, sems.at[0]).wait()
    pltpu.make_async_copy(item_ref, item_out, sems.at[1]).wait()


def solution(mesh):
    row_size = mesh.shape["row"]
    col_size = mesh.shape["col"]
    grid_spec = P(("part", "row"), "col")
    user_spec = P(("part", "row"), None)
    item_spec = P(("part", "col"), None)

    def local_step(ratings_blk, mask_blk, user_blk, item_blk):
        users, items = ratings_blk.shape
        span = users // COLS
        early = STARTS[LATE]
        late = span - early
        tiles = span // LANES
        hbm_spec = pl.BlockSpec(memory_space=pltpu.HBM)
        vmem = pltpu.VMEM
        dma = pltpu.SemaphoreType.DMA
        terms = DIAGS * RANK
        user_new, item_new = pl.pallas_call(
            functools.partial(sweep_kernel, RIDGE_WEIGHT * items * col_size, RIDGE_WEIGHT * users * row_size),
            out_shape=(
                pltpu.VMEM((RANK, users), F32),
                pltpu.VMEM((RANK, items), F32),
            ),
            in_specs=[hbm_spec] * 4,
            out_specs=(pl.BlockSpec(memory_space=pltpu.VMEM),) * 2,
            scratch_shapes=[
                vmem((COLS, span, items), F32),
                vmem((COLS, span, items), jnp.int32),
                vmem((RANK, users), F32),
                vmem((RANK, items), F32),
                vmem((COLS, span, items), BF16),
                vmem((2, span, items), BF16),
                vmem((2, DIRECT, items), BF16),
                vmem((RANK, items), BF16),
                vmem((3, RANK, items), BF16),
                vmem((COLS, terms, 2 * items), BF16),
                vmem((COLS, early, 3 * items), BF16),
                vmem((sum(PACKED), RANK, LANES), BF16),
                vmem((sum(PACKED), RANK, LANES), BF16),
                vmem((terms, span), F32),
                vmem((2, RANK, span), F32),
                vmem((2, RANK, span), F32),
                vmem((tiles, RANK, LANES), BF16),
                vmem((tiles, RANK, LANES), BF16),
                vmem((RANK, span), F32),
                vmem((COLS, early // LANES, RANK, LANES), BF16),
                vmem((COLS, tiles, RANK, LANES), F32),
                vmem((terms + 2 * RANK, items), BF16),
                vmem((terms + 2 * RANK, items), BF16),
                vmem((COLS, late, items), BF16),
                vmem((COLS, late, items), BF16),
                vmem((2 * COLS, late, items), BF16),
                vmem((2 * COLS, late, items), BF16),
                vmem((2 * COLS, late // LANES, RANK, LANES), BF16),
                vmem((CHUNKS - LATE, 2, terms + RANK, items), F32),
                vmem((3, terms + RANK, items), F32),
                dma((6,)),
                dma((1,)),
                dma((2,)),
                dma((1,)),
                dma((2,)),
                dma((1,)),
                dma((CHUNKS - 1,)),
                dma((3,)),
                dma((2,)),
                dma((1,)),
                dma((2,)),
                dma((2 * (CHUNKS - LATE),)),
            ],
            compiler_params=pltpu.CompilerParams(collective_id=0, has_side_effects=True, vmem_limit_bytes=60000 * 1024),
        )(ratings_blk, mask_blk, user_blk.T, item_blk.T)
        user_new, item_new = pl.pallas_call(
            write_kernel,
            out_shape=(
                jax.ShapeDtypeStruct((RANK, users), F32),
                jax.ShapeDtypeStruct((RANK, items), F32),
            ),
            in_specs=[pl.BlockSpec(memory_space=pltpu.VMEM)] * 2,
            out_specs=(hbm_spec, hbm_spec),
            scratch_shapes=[dma((2,))],
            compiler_params=pltpu.CompilerParams(vmem_limit_bytes=2**20),
        )(user_new, item_new)
        return user_new.T, item_new.T

    return jax.shard_map(local_step, mesh=mesh, in_specs=(grid_spec, grid_spec, user_spec, item_spec), out_specs=(user_spec, item_spec), check_vma=False)
```

```python
import functools
import math

import jax
import jax.numpy as jnp
from jax import lax
from jax.experimental import pallas as pl
from jax.experimental.pallas import tpu as pltpu
from jax.sharding import PartitionSpec as P

CG_STEPS = 4
RIDGE_WEIGHT = 0.0005
RANK = 16
DIAGS = RANK // 2 + 1
MESH = pl.DeviceIdType.MESH
F32 = jnp.float32
BF16 = jnp.bfloat16
COLS = 4
LANES = 128
HALF = RANK // 2
WIDTHS = (256, 256, 128, 256, 128)
STARTS = tuple(sum(WIDTHS[:i]) for i in range(len(WIDTHS)))
CHUNKS = len(WIDTHS)
LATE = 3
DIRECT = 128


def dot_nt(a, b):
    return lax.dot_general(a, b, (((1,), (1,)), ((), ())), preferred_element_type=F32)


def dot_nn(a, b):
    return lax.dot_general(a, b, (((1,), (0,)), ((), ())), preferred_element_type=F32)


def turn(x, shift):
    return x if shift % RANK == 0 else pltpu.roll(x, shift % RANK, 0)


def pair_products(fac):
    prods = jnp.concatenate([fac * turn(fac, -d) for d in range(DIAGS)], axis=0)
    high = prods.astype(BF16)
    low = (prods - high.astype(F32)).astype(BF16)
    return high, low


def apply_gram(diags, vec):
    parts = [diags[d] * turn(vec, -d) for d in range(DIAGS)]
    parts += [turn(diags[d] * vec, d) for d in range(1, RANK // 2)]
    while len(parts) > 1:
        parts = [sum(parts[i:i + 2][1:], parts[i]) for i in range(0, len(parts), 2)]
    return parts[0]


def cg_solve(diags, residual, start, ridge):
    direction = residual
    estimate = start
    res_sq = jnp.sum(residual * residual, axis=0, keepdims=True)
    for cg_step in range(CG_STEPS):
        gram_dir = apply_gram(diags, direction) + ridge * direction
        step_size = res_sq / jnp.sum(direction * gram_dir, axis=0, keepdims=True)
        estimate = estimate + step_size * direction
        if cg_step + 1 < CG_STEPS:
            residual = residual - step_size * gram_dir
            new_sq = jnp.sum(residual * residual, axis=0, keepdims=True)
            direction = residual + (new_sq / res_sq) * direction
            res_sq = new_sq
    return estimate


def far_span(chunk):
    skip = DIRECT if chunk == 0 else 0
    return STARTS[chunk] + skip, WIDTHS[chunk] - skip


def packed_tiles(chunk):
    tiles = far_span(chunk)[1] // LANES
    return HALF * tiles + (tiles + 1) // 2


PACKED = tuple(packed_tiles(chunk) for chunk in range(CHUNKS))


def chunk_tiles(chunk):
    return range(STARTS[chunk] // LANES, (STARTS[chunk] + WIDTHS[chunk]) // LANES)


def side_by_side(blocks):
    return jnp.concatenate(list(blocks), axis=1)


def stacked(blocks):
    return jnp.concatenate(list(blocks), axis=0)


def three_terms(values):
    high = values.astype(BF16)
    rest = values - high.astype(F32)
    middle = rest.astype(BF16)
    return side_by_side([high, middle, (rest - middle.astype(F32)).astype(BF16)])


def diagonals(full):
    return [full[d * RANK:(d + 1) * RANK] for d in range(DIAGS)]


def sweep_kernel(
    user_ridge, item_ridge,
    ratings_hbm, mask_hbm, user_hbm, item_hbm,
    user_out, item_out,
    rate, mask32, user0, item0,
    mask16, mask16_peer, mask16_direct, item16, item16_peer, ffs, zrate,
    gram_send, gram_recv, gram_own,
    res_pair, res_pair_recv, res_far, res_far_recv, res_own,
    fac, user1, item_send, item_recv,
    late_send, late_recv, late_seen, late_rated, late_fac, late_sums, early_sums,
    in_sem, send_sem, item_sem, own_sem, mask_sem, pair_sem, gram_sem, fac_sem, user_sem, cross_sem, late_sem, late_fac_sem,
):
    part = lax.axis_index("part")
    row = lax.axis_index("row")
    col = lax.axis_index("col")
    chip = col // 2
    core = col % 2
    pair_col = chip * 2 + (1 - core)
    far_col = (1 - chip) * 2 + core
    diag_col = (1 - chip) * 2 + (1 - core)
    pair = (part, row, pair_col)
    far = (part, row, far_col)
    diag = (part, row, diag_col)
    cross = (part, 1 - row, col)
    peers = ((pair, pair_col, 2), (far, far_col, 1), (diag, diag_col, 0))
    far_chip = [(part, row, (1 - chip) * 2 + k) for k in range(2)]
    cross_chip = [(part, 1 - row, chip * 2 + k) for k in range(2)]
    diag_chip = [(part, 1 - row, (1 - chip) * 2 + k) for k in range(2)]

    span = mask16.shape[1]
    items = item0.shape[1]
    terms = DIAGS * RANK
    early = STARTS[LATE]
    late = span - early

    sent = []

    def copy_to(src, dst, recv_sem, device):
        sent.append(src)
        return pltpu.make_async_remote_copy(
            src_ref=src, dst_ref=dst, send_sem=send_sem.at[0], recv_sem=recv_sem,
            device_id=device, device_id_type=MESH,
        )

    def wait_for(ref, sem):
        pltpu.make_async_copy(ref, ref, sem).wait()

    def wait_all(refs, sem):
        count = sum(math.prod(ref.shape) * ref.dtype.itemsize for ref in refs) // (items * rate.dtype.itemsize)
        parts = next(parts for parts in (1, 2, COLS) if count <= parts * span and count % parts == 0)
        wait_for(rate.at[pl.ds(0, parts), pl.ds(0, count // parts)], sem)

    barrier = pltpu.get_barrier_semaphore()
    for device in (pair, far, diag, cross):
        pl.semaphore_signal(barrier, inc=1, device_id=device, device_id_type=MESH)

    order = (diag_col, far_col, pair_col, col)

    def load(src, dst, slot):
        return pltpu.make_async_copy(src, dst, in_sem.at[slot])

    def block_rows(block, start=0, size=span):
        return pl.ds(pl.multiple_of(block * span + start, LANES), size)

    def chunk_rows(chunk):
        return pl.ds(STARTS[chunk], WIDTHS[chunk])

    item_load = load(item_hbm, item0, 0)
    user_load = load(user_hbm, user0, 4)
    rate_loads = []
    rate_late_loads = []
    mask_loads = []
    splits = (WIDTHS[0], WIDTHS[0], early, early)
    for slot, block in enumerate(order):
        rate_loads.append(load(ratings_hbm.at[block_rows(block, 0, early)], rate.at[slot, pl.ds(0, early)], 4 + slot // 2))
        rate_late_loads.append(load(ratings_hbm.at[block_rows(block, early, late)], rate.at[slot, pl.ds(early, late)], 2 + min(slot, 1)))
        pieces = []
        for half, (start, size) in enumerate(((0, splits[slot]), (splits[slot], span - splits[slot]))):
            src = mask_hbm.at[block_rows(block, start, size)]
            pieces.append(load(src, mask32.at[slot, pl.ds(start, size)], (4, 5, 5)[min(slot, 2)] if half == 0 else (1, 3)[slot // 2]))
        mask_loads.append(pieces)

    def convert(slot, start, size):
        rows = pl.ds(start, size)
        seen = mask32[slot, rows].astype(F32).astype(BF16)
        mask16[slot, rows] = seen
        if start + size == span:
            late_seen[row * COLS + order[slot]] = seen[early - start:]

    item_load.start()
    for pieces in mask_loads[:2]:
        for copy in pieces:
            copy.start()
    for slot in range(COLS):
        if slot >= 2:
            mask_loads[slot][1].start()
        rate_late_loads[slot].start()

    item_load.wait()
    item16[...] = item0[...].astype(BF16)
    pl.semaphore_wait(barrier, 4)
    item_copies = []
    for lane, (device, _, _) in enumerate(peers[:2]):
        item_copies.append(copy_to(item16, item16_peer.at[lane], item_sem.at[lane], device))
        item_copies[-1].start()
    first = pl.ds(0, DIRECT)

    def send_late(slot):
        rows = pl.ds(early, late)
        late_send[order[slot]] = jnp.where(mask32[slot, rows] > 0, rate[slot, rows], jnp.inf).astype(BF16)
        copy_to(late_send.at[order[slot]], late_recv.at[order[slot]], late_sem.at[min(slot, 1)], cross).start()

    def mask_copy(half):
        rows = pl.ds(*((splits[0], span - splits[0]) if half else (DIRECT, splits[0] - DIRECT)))
        return copy_to(mask16.at[0, rows], mask16_peer.at[0, rows], mask_sem.at[half], pair)

    mask_copies = [mask_copy(half) for half in range(2)]
    mask_loads[0][0].wait()
    convert(0, 0, splits[0])
    mask_copies[0].start()
    copy_to(mask16.at[0, first], mask16_direct.at[1], own_sem.at[0], diag).start()
    mask_loads[1][0].wait()
    convert(1, 0, splits[1])
    copy_to(mask16.at[1, first], mask16_direct.at[0], own_sem.at[0], far).start()
    rest = pl.ds(splits[0], span - splits[0])
    wait_for(mask32.at[pl.ds(0, 2), rest], in_sem.at[1])
    convert(0, splits[0], span - splits[0])
    mask_copies[1].start()
    user_load.start()
    for pieces in mask_loads[2:]:
        pieces[0].start()
    for copy in rate_loads:
        copy.start()
    rate_late_loads[0].wait()
    send_late(0)
    convert(1, splits[1], span - splits[1])
    wait_all([rate.at[pl.ds(1, COLS - 1), pl.ds(early, late)], mask32.at[pl.ds(2, 2), pl.ds(early, late)]], in_sem.at[3])
    send_late(1)
    for slot in (2, 3):
        convert(slot, early, late)
        send_late(slot)

    def put_products(index, factors):
        high, low = pair_products(factors.astype(F32))
        ffs[index, :, :items] = high
        ffs[index, :, items:] = low

    put_products(0, item16[...])
    item_copies[0].wait_recv()
    put_products(1, item16_peer[0])

    def gram_of(index, seen):
        return dot_nt(ffs[index], side_by_side([seen, seen]))

    def gram_part(slot, rows):
        return gram_of(0, mask16[slot, rows, :]) + gram_of(1, mask16_peer[slot // 2, rows, :])

    def pack(gram, chunk):
        tiles = gram.shape[1] // LANES
        base = sum(PACKED[:chunk])
        for d in range(HALF):
            for t in range(tiles):
                piece = gram[d * RANK:(d + 1) * RANK, t * LANES:(t + 1) * LANES]
                gram_send[base + d * tiles + t] = piece.astype(BF16)
        half = gram[HALF * RANK:HALF * RANK + HALF]
        for t in range(0, tiles, 2):
            both = [half[:, min(u, tiles - 1) * LANES:][:, :LANES] for u in (t, t + 1)]
            gram_send[base + HALF * tiles + t // 2] = stacked(both).astype(BF16)

    def unpack(chunk):
        gap = far_span(chunk)[1]
        tiles = gap // LANES
        base = sum(PACKED[:chunk])
        diags = [side_by_side(gram_recv[base + d * tiles + t].astype(F32) for t in range(tiles)) for d in range(HALF)]
        pieces = []
        for t in range(0, tiles, 2):
            both = gram_recv[base + HALF * tiles + t // 2].astype(F32)
            for half in (both[:HALF], both[HALF:])[:tiles - t]:
                pieces.append(stacked([half, half]))
        diags.append(side_by_side(pieces))
        pad = WIDTHS[chunk] - gap
        return [side_by_side([jnp.zeros((RANK, pad), F32), d]) if pad else d for d in diags]

    gram_copies = []
    for chunk in range(CHUNKS):
        part_of = pl.ds(sum(PACKED[:chunk]), PACKED[chunk])
        gram_copies.append(copy_to(gram_send.at[part_of], gram_recv.at[part_of], gram_sem.at[max(chunk - 1, 0)], far))

    def far_gram(chunk):
        if chunk < 2:
            mask_copies[chunk].wait_recv()
        pack(gram_part(1, pl.ds(*far_span(chunk))), chunk)

    for chunk in range(2):
        far_gram(chunk)
        gram_copies[chunk].start()

    def user_residual(slot, block):
        start = user0[:, block_rows(block)]
        scores = dot_nn(start.T.astype(BF16), item16[...])
        resid = jnp.where(mask32[slot] > 0, rate[slot] - scores, 0.0).astype(BF16)
        return dot_nt(item16[...], resid)

    wait_all([user0, rate.at[pl.ds(0, 2), pl.ds(0, early)]], in_sem.at[4])
    res_pair[0] = user_residual(0, diag_col)
    pair_copies = [copy_to(res_pair.at[slot], res_pair_recv.at[slot], (own_sem if slot else pair_sem).at[0], pair) for slot in range(2)]
    pair_copies[0].start()
    far_part = user_residual(1, far_col)
    far_gram(2)
    pair_copies[0].wait_recv()
    total = (far_part + res_pair_recv[0]).astype(BF16)
    for t in range(span // LANES):
        res_far[t] = total[:, t * LANES:(t + 1) * LANES]
    far_copies = []
    res_groups = pl.ds(0, early // LANES), pl.ds(early // LANES, late // LANES)
    for half, tiles in enumerate(res_groups):
        far_copies.append(copy_to(res_far.at[tiles], res_far_recv.at[tiles], gram_sem.at[half * 2], far))
    for copy in (far_copies[0], gram_copies[2], far_copies[1]):
        copy.start()
    for chunk in range(LATE, CHUNKS):
        far_gram(chunk)
        if chunk < CHUNKS - 1:
            gram_copies[chunk].start()
    pl.when(core == 0)(gram_copies[-1].start)
    item_copies[1].wait_recv()
    copy_to(item16_peer.at[1], item16_peer.at[2], own_sem.at[0], pair).start()
    wait_all([mask32.at[pl.ds(2, 2), pl.ds(0, early)], rate.at[pl.ds(2, 2), pl.ds(0, early)]], in_sem.at[5])
    convert(2, 0, early)
    own_mask_copy = copy_to(mask16.at[2], mask16_peer.at[1], own_sem.at[0], pair)
    own_mask_copy.start()
    convert(3, 0, early)
    res_pair[1] = user_residual(2, pair_col)
    pair_copies[1].start()
    own_part = user_residual(3, col)
    wait_all([mask16_peer.at[1], item16_peer.at[2], mask16_direct, res_pair_recv.at[1]], own_sem.at[0])
    for chunk in range(CHUNKS):
        gram_own[:, chunk_rows(chunk)] = gram_part(3, chunk_rows(chunk))
    for lane in range(2):
        put_products(2 + lane, item16_peer[1 + lane])
        gram_own[:, :DIRECT] += gram_of(2 + lane, mask16_direct[lane])
    res_own[...] = own_part + res_pair_recv[1] - user_ridge * user0[:, block_rows(col)]

    wait_for(late_recv.at[0], late_sem.at[0])
    for slot in range(COLS):
        seen_rate = jnp.where(mask32[slot] > 0, rate[slot], 0.0)
        zrate[slot] = three_terms(seen_rate[:early])
        late_rated[row * COLS + order[slot]] = seen_rate[early:].astype(BF16)

    def item_sums(factors, seen, rated):
        pairs = stacked(pair_products(factors.astype(F32)))
        return dot_nn(pairs, seen), dot_nn(factors, rated)

    def item_part(entries):
        factors = side_by_side(fac[source, t] for source, _, chunk in entries for t in chunk_tiles(chunk))
        seen = stacked(mask16[slot, chunk_rows(chunk), :] for _, slot, chunk in entries)
        rated = stacked(zrate[slot, chunk_rows(chunk), :] for _, slot, chunk in entries)
        gram, rated_sum = item_sums(factors, seen, rated)
        return gram[:terms] + gram[terms:], sum((rated_sum[:, i * items:(i + 1) * items] for i in (1, 2)), rated_sum[:, :items])

    def add_part(entries, index):
        @pl.when(col < COLS)
        def _():
            early_sums[index, :terms], early_sums[index, terms:] = item_part(entries)

    def late_part(of_row, chunk):
        tiles = [t - early // LANES for t in chunk_tiles(chunk)]
        rows = pl.ds(STARTS[chunk] - early, WIDTHS[chunk])
        factors = side_by_side(late_fac[of_row * COLS + block, t] for block in range(COLS) for t in tiles)
        seen = stacked(late_seen[of_row * COLS + block, rows, :] for block in range(COLS))
        rated = stacked(late_rated[of_row * COLS + block, rows, :] for block in range(COLS))
        gram, rated_sum = item_sums(factors, seen, rated)
        index = chunk - LATE, lax.rem(of_row + row, 2)
        late_sums[index + (pl.ds(0, terms),)] = gram[:terms] + gram[terms:]
        late_sums[index + (pl.ds(terms, RANK),)] = rated_sum

    def split_late(slot):
        value = late_recv[order[slot]].astype(F32)
        seen = value < jnp.inf
        late_seen[(1 - row) * COLS + order[slot]] = seen.astype(F32).astype(BF16)
        late_rated[(1 - row) * COLS + order[slot]] = jnp.where(seen, value, 0.0).astype(BF16)

    groups = (range(0, early // LANES), range(early // LANES, span // LANES))

    def send_users(group):
        mine = user1.at[col, pl.ds(groups[group][0], len(groups[group]))]
        for lane, (device, _, _) in enumerate(peers[:2 + group]):
            sem = user_sem.at[1 if (group, lane) == (0, 1) else 0]
            copy_to(mine, mine, sem, device).start()

    def forward_users():
        theirs = user1.at[far_col, pl.ds(groups[0][0], len(groups[0]))]
        wait_for(theirs, user_sem.at[1])
        copy_to(theirs, theirs, user_sem.at[0], pair).start()

    def solve(chunk):
        lanes = chunk_rows(chunk)
        if chunk != 1:
            together = [gram_recv.at[pl.ds(sum(PACKED[:c]), PACKED[c])] for c in ((0, 1) if chunk == 0 else (chunk,))]
            if chunk in (0, LATE):
                together.append(res_far_recv.at[res_groups[chunk // LATE]])
            wait_all(together, gram_sem.at[max(chunk - 1, 0)])
        far_diags = unpack(chunk)
        diags = [gram_own[d * RANK:(d + 1) * RANK, lanes] + far_diags[d] for d in range(DIAGS)]
        start = user0[:, block_rows(col, STARTS[chunk], WIDTHS[chunk])]
        residual = res_own[:, lanes] + side_by_side(res_far_recv[t].astype(F32) for t in chunk_tiles(chunk))
        solved = cg_solve(diags, residual, start, user_ridge)
        return [solved[:, i * LANES:(i + 1) * LANES] for i in range(WIDTHS[chunk] // LANES)]

    fac_groups = pl.ds(0, STARTS[2] // LANES), pl.ds(STARTS[2] // LANES, WIDTHS[2] // LANES)

    def hand_on(group):
        theirs = fac.at[far_col, fac_groups[group]]
        copy = pltpu.make_async_remote_copy(
            src_ref=theirs, dst_ref=theirs, send_sem=send_sem.at[0], recv_sem=fac_sem.at[1 + group],
            device_id=pair, device_id_type=MESH,
        )
        pl.when(core == 0)(copy.start)

    def entries_of(lanes, chunks):
        return [(peers[lane][1], peers[lane][2], chunk) for chunk in chunks for lane in lanes]

    for chunk in range(LATE):
        pieces = solve(chunk)
        tiles = chunk_tiles(chunk)
        for t, piece in zip(tiles, pieces):
            fac[col, t] = piece.astype(BF16)
            user1[col, t] = piece
        if chunk:
            mine = fac.at[col, fac_groups[chunk - 1]]
            copy_to(mine, mine, fac_sem.at[chunk], far_chip[0]).start()
            copy = copy_to(mine, mine, fac_sem.at[chunk], far_chip[1])
            pl.when(core == 1)(copy.start)
            copy_to(mine, mine, fac_sem.at[0], pair).start()
            if chunk == 1:
                pl.when(core == 1)(gram_copies[-1].start)
    send_users(0)
    add_part([(col, 3, chunk) for chunk in range(LATE)], 0)
    wait_for(fac.at[0], fac_sem.at[0])
    add_part(entries_of((0,), range(LATE)), 1)
    for chunk in range(LATE, CHUNKS):
        pieces = solve(chunk)
        tiles = chunk_tiles(chunk)
        for t, piece in zip(tiles, pieces):
            late_fac[row * COLS + col, t - early // LANES] = piece.astype(BF16)
            user1[col, t] = piece
        mine = late_fac.at[row * COLS + col, pl.ds(tiles[0] - early // LANES, len(tiles))]
        for device, other_row in [(far_chip[0], 0), (diag_chip[0], 1), (cross_chip[0], 1), (diag_chip[1], 1), (cross_chip[1], 1), (far_chip[1], 0), (pair, 0)]:
            copy_to(mine, mine, late_fac_sem.at[(chunk - LATE) * 2 + other_row], device).start()
    send_users(1)
    wait_for(fac.at[pl.ds(0, 2), fac_groups[0]], fac_sem.at[1])
    hand_on(0)
    add_part(entries_of((1, 2), range(LATE - 1)), 2)
    wait_for(fac.at[pl.ds(0, 2), fac_groups[1]], fac_sem.at[2])
    hand_on(1)
    gram, residual = item_part(entries_of((1, 2), (LATE - 1,)))
    before = early_sums[0] + early_sums[1] + early_sums[2]
    gram = gram + before[:terms]
    start = item16[...].astype(F32)
    item_send[:terms] = gram.astype(BF16)
    first_rows = pl.ds(0, terms)
    copy_to(item_send.at[first_rows], item_recv.at[first_rows], cross_sem.at[0], cross).start()
    residual = residual + before[terms:] - apply_gram(diagonals(gram), start)
    high = residual.astype(BF16)
    item_send[terms:terms + RANK] = high
    item_send[terms + RANK:] = (residual - high.astype(F32)).astype(BF16)
    last_rows = pl.ds(terms, 2 * RANK)
    cross_copy = copy_to(item_send.at[last_rows], item_recv.at[last_rows], cross_sem.at[0], cross)
    cross_copy.start()
    wait_for(late_recv.at[pl.ds(1, COLS - 1)], late_sem.at[1])
    for slot in range(COLS):
        split_late(slot)
    forward_users()

    def late_arrived(chunk, which):
        tiles = chunk_tiles(chunk)
        view = late_fac.at[pl.ds(0, COLS - 1 + which), pl.ds(tiles[0] - early // LANES, len(tiles))]
        wait_for(view, late_fac_sem.at[(chunk - LATE) * 2 + which])

    for which, of_row in enumerate((row, 1 - row)):
        for chunk in range(LATE, CHUNKS):
            late_arrived(chunk, which)
            pl.when(col < COLS)(functools.partial(late_part, of_row, chunk))
    late_total = sum((late_sums[chunk, 0] for chunk in range(1, CHUNKS - LATE)), late_sums[0, 0])
    late_total = late_total + sum((late_sums[chunk, 1] for chunk in range(1, CHUNKS - LATE)), late_sums[0, 1])
    late_gram = late_total[:terms]
    late_residual = late_total[terms:] - apply_gram(diagonals(late_gram), start)

    wait_all([user1.at[0, pl.ds(0, early // LANES)]] * 2 + [user1.at[0, pl.ds(0, late // LANES)]] * 3, user_sem.at[0])
    for source in range(COLS):
        for t in range(span // LANES):
            user_out[:, pl.ds(source * span + t * LANES, LANES)] = user1[source, t]

    wait_for(item_recv, cross_sem.at[0])
    full = item_send[...].astype(F32) + item_recv[...].astype(F32)
    residual = full[terms:terms + RANK] + full[terms + RANK:] + late_residual - item_ridge * item0[...]
    item_out[...] = cg_solve(diagonals(full[:terms] + late_gram), residual, item0[...], item_ridge)

    wait_all(sent, send_sem.at[0])


def write_kernel(user_ref, item_ref, user_out, item_out, sems):
    pltpu.make_async_copy(item_ref, item_out, sems.at[1]).start()
    for half in range(2):
        for piece in range(4):
            lanes = user_ref.shape[1] // 4
            part = pl.ds(half * RANK // 2, RANK // 2), pl.ds(piece * lanes, lanes)
            pltpu.make_async_copy(user_ref.at[part], user_out.at[part], sems.at[0]).start()
    pltpu.make_async_copy(user_ref, user_out, sems.at[0]).wait()
    pltpu.make_async_copy(item_ref, item_out, sems.at[1]).wait()


def solution(mesh):
    row_size = mesh.shape["row"]
    col_size = mesh.shape["col"]
    grid_spec = P(("part", "row"), "col")
    user_spec = P(("part", "row"), None)
    item_spec = P(("part", "col"), None)

    def local_step(ratings_blk, mask_blk, user_blk, item_blk):
        users, items = ratings_blk.shape
        span = users // COLS
        early = STARTS[LATE]
        late = span - early
        tiles = span // LANES
        hbm_spec = pl.BlockSpec(memory_space=pltpu.HBM)
        vmem = pltpu.VMEM
        dma = pltpu.SemaphoreType.DMA
        terms = DIAGS * RANK
        user_new, item_new = pl.pallas_call(
            functools.partial(sweep_kernel, RIDGE_WEIGHT * items * col_size, RIDGE_WEIGHT * users * row_size),
            out_shape=(
                pltpu.VMEM((RANK, users), F32),
                pltpu.VMEM((RANK, items), F32),
            ),
            in_specs=[hbm_spec] * 4,
            out_specs=(pl.BlockSpec(memory_space=pltpu.VMEM),) * 2,
            scratch_shapes=[
                vmem((COLS, span, items), F32),
                vmem((COLS, span, items), jnp.int32),
                vmem((RANK, users), F32),
                vmem((RANK, items), F32),
                vmem((COLS, span, items), BF16),
                vmem((2, span, items), BF16),
                vmem((2, DIRECT, items), BF16),
                vmem((RANK, items), BF16),
                vmem((3, RANK, items), BF16),
                vmem((COLS, terms, 2 * items), BF16),
                vmem((COLS, early, 3 * items), BF16),
                vmem((sum(PACKED), RANK, LANES), BF16),
                vmem((sum(PACKED), RANK, LANES), BF16),
                vmem((terms, span), F32),
                vmem((2, RANK, span), F32),
                vmem((2, RANK, span), F32),
                vmem((tiles, RANK, LANES), BF16),
                vmem((tiles, RANK, LANES), BF16),
                vmem((RANK, span), F32),
                vmem((COLS, early // LANES, RANK, LANES), BF16),
                vmem((COLS, tiles, RANK, LANES), F32),
                vmem((terms + 2 * RANK, items), BF16),
                vmem((terms + 2 * RANK, items), BF16),
                vmem((COLS, late, items), BF16),
                vmem((COLS, late, items), BF16),
                vmem((2 * COLS, late, items), BF16),
                vmem((2 * COLS, late, items), BF16),
                vmem((2 * COLS, late // LANES, RANK, LANES), BF16),
                vmem((CHUNKS - LATE, 2, terms + RANK, items), F32),
                vmem((3, terms + RANK, items), F32),
                dma((6,)),
                dma((1,)),
                dma((2,)),
                dma((1,)),
                dma((2,)),
                dma((1,)),
                dma((CHUNKS - 1,)),
                dma((3,)),
                dma((2,)),
                dma((1,)),
                dma((2,)),
                dma((2 * (CHUNKS - LATE),)),
            ],
            compiler_params=pltpu.CompilerParams(collective_id=0, has_side_effects=True, vmem_limit_bytes=60000 * 1024),
        )(ratings_blk, mask_blk, user_blk.T, item_blk.T)
        user_new, item_new = pl.pallas_call(
            write_kernel,
            out_shape=(
                jax.ShapeDtypeStruct((RANK, users), F32),
                jax.ShapeDtypeStruct((RANK, items), F32),
            ),
            in_specs=[pl.BlockSpec(memory_space=pltpu.VMEM)] * 2,
            out_specs=(hbm_spec, hbm_spec),
            scratch_shapes=[dma((2,))],
            compiler_params=pltpu.CompilerParams(vmem_limit_bytes=2**20),
        )(user_new, item_new)
        return user_new.T, item_new.T

    return jax.shard_map(local_step, mesh=mesh, in_specs=(grid_spec, grid_spec, user_spec, item_spec), out_specs=(user_spec, item_spec), check_vma=False)
```
